16 devices in a mesh: data: 16 (over z, y, x, core).
Axes of the slice: x: 2, y: 2, z: 2, core: 2. Of those that a mesh axis runs over, the one named last changes fastest.
Arguments:
- x_in: bfloat16 [16, 1024, 768], P('data')
- grad_y: bfloat16 [16, 1024, 768], P('data')
- gain_one: float32 [2, 768], replicated
- gain_two: float32 [2, 768], replicated
- w_qkv: bfloat16 [2, 768, 2304], replicated
- w_out: bfloat16 [2, 768, 768], replicated
- w_up: bfloat16 [2, 768, 3072], replicated
- w_down: bfloat16 [2, 3072, 768], replicated
Outputs:
- output 1: bfloat16 [16, 1024, 768], P('data')
- output 2: float32 [2, 768], replicated
- output 3: float32 [2, 768], replicated
- output 4: float32 [2, 768, 2304], replicated
- output 5: float32 [2, 768, 768], replicated
- output 6: float32 [2, 768, 3072], replicated
- output 7: float32 [2, 3072, 768], replicated
All inputs are finite; a program needn't handle non-finite values.
Results may differ from the reference program's by a relative error of at most 0.0198561.
Values are sent between devices in bfloat16 or wider.
A program may use at most 1 GiB of HBM per device.

```python
import jax
import jax.numpy as jnp
from jax import lax

D = 768
FF = 3072
HEADS = 12
LAYERS = 2
SEQ = 1024
BATCH = 16
GROUP = 16
HEAD_DIM = D // HEADS
NORM_EPS = 1e-6


def setup_inputs(seed: int = 0) -> dict:
    root_key = jax.random.key(seed)
    sub_keys = jax.random.split(root_key, 8)
    x_in = jax.random.normal(sub_keys[0], (BATCH, SEQ, D), jnp.float32)
    grad_y = jax.random.normal(sub_keys[1], (BATCH, SEQ, D), jnp.float32)
    gain_one = 1.0 + 0.3 * jax.random.normal(sub_keys[2], (LAYERS, D), jnp.float32)
    gain_two = 1.0 + 0.3 * jax.random.normal(sub_keys[3], (LAYERS, D), jnp.float32)
    w_qkv = jax.random.normal(sub_keys[4], (LAYERS, D, 3 * D), jnp.float32) * D ** -0.5
    w_out = jax.random.normal(sub_keys[5], (LAYERS, D, D), jnp.float32) * D ** -0.5
    w_up = jax.random.normal(sub_keys[6], (LAYERS, D, FF), jnp.float32) * D ** -0.5
    w_down = jax.random.normal(sub_keys[7], (LAYERS, FF, D), jnp.float32) * FF ** -0.5
    return {'x_in': x_in.astype(jnp.bfloat16), 'grad_y': grad_y.astype(jnp.bfloat16), 'gain_one': gain_one, 'gain_two': gain_two, 'w_qkv': w_qkv.astype(jnp.bfloat16), 'w_out': w_out.astype(jnp.bfloat16), 'w_up': w_up.astype(jnp.bfloat16), 'w_down': w_down.astype(jnp.bfloat16)}


def rms_gain(rows_f, gain_vec):
    return rows_f * lax.rsqrt(jnp.mean(rows_f * rows_f, axis=-1, keepdims=True) + NORM_EPS) * gain_vec


def gelu_tanh(pre_act):
    return jax.nn.gelu(pre_act, approximate=True)


def mat_lo(lhs_mat, rhs_mat):
    return jnp.dot(lhs_mat, rhs_mat, preferred_element_type=jnp.float32).astype(jnp.bfloat16)


def mat_nt(lhs_mat, rhs_mat):
    return lax.dot_general(lhs_mat, rhs_mat, (((1,), (1,)), ((), ())), preferred_element_type=jnp.float32).astype(jnp.bfloat16)


def mat_tn(lhs_mat, rhs_mat):
    return lax.dot_general(lhs_mat, rhs_mat, (((0,), (0,)), ((), ())), preferred_element_type=jnp.float32)


def head_mix(einsum_spec, lhs_arr, rhs_arr):
    return jnp.einsum(einsum_spec, lhs_arr.astype(jnp.float32), rhs_arr.astype(jnp.float32))


def seq_forward(seq_rows, gain_a, gain_b, w_qkv, w_out, w_up):
    norm_a, norm_a_back = jax.vjp(rms_gain, seq_rows.astype(jnp.float32), gain_a)
    u_one = norm_a.astype(jnp.bfloat16)
    qkv_lo = mat_lo(u_one, w_qkv)
    q_all = qkv_lo[:, :D].reshape(SEQ, HEADS, HEAD_DIM)
    k_all = qkv_lo[:, D:2 * D].reshape(SEQ, HEADS, HEAD_DIM)
    v_all = qkv_lo[:, 2 * D:].reshape(SEQ, HEADS, HEAD_DIM)
    scores = head_mix('qhe,khe->hqk', q_all, k_all) * HEAD_DIM ** -0.5
    causal = jnp.arange(SEQ)[:, None] >= jnp.arange(SEQ)[None, :]
    prob_full = jax.nn.softmax(jnp.where(causal, scores, -1e30), axis=-1)
    prob_lo = prob_full.astype(jnp.bfloat16)
    attn_out = head_mix('hqk,khe->qhe', prob_lo, v_all).astype(jnp.bfloat16).reshape(SEQ, D)
    hidden = seq_rows + mat_lo(attn_out, w_out)
    norm_b, norm_b_back = jax.vjp(rms_gain, hidden.astype(jnp.float32), gain_b)
    u_two = norm_b.astype(jnp.bfloat16)
    pre_lo = mat_lo(u_two, w_up)
    act_f, gelu_back = jax.vjp(gelu_tanh, pre_lo.astype(jnp.float32))
    act_lo = act_f.astype(jnp.bfloat16)
    saved_vals = (norm_a_back, u_one, q_all, k_all, v_all, prob_full, prob_lo, attn_out, norm_b_back, u_two, gelu_back, act_lo)
    return hidden, act_lo, saved_vals


def seq_backward(grad_blk, saved_vals, w_qkv, w_out, w_up, w_down):
    (norm_a_back, u_one, q_all, k_all, v_all, prob_full, prob_lo, attn_out, norm_b_back, u_two, gelu_back, act_lo) = saved_vals
    grad_down_w = mat_tn(act_lo, grad_blk)
    grad_act = mat_nt(grad_blk, w_down)
    (grad_pre_f,) = gelu_back(grad_act.astype(jnp.float32))
    grad_pre = grad_pre_f.astype(jnp.bfloat16)
    grad_up_w = mat_tn(u_two, grad_pre)
    grad_u_two = mat_nt(grad_pre, w_up)
    grad_h_norm, grad_gain_b = norm_b_back(grad_u_two.astype(jnp.float32))
    grad_hidden = (grad_blk.astype(jnp.float32) + grad_h_norm).astype(jnp.bfloat16)
    grad_out_w = mat_tn(attn_out, grad_hidden)
    grad_attn = mat_nt(grad_hidden, w_out).reshape(SEQ, HEADS, HEAD_DIM)
    grad_probs = head_mix('qhe,khe->hqk', grad_attn, v_all)
    grad_scores = (prob_full * (grad_probs - jnp.sum(prob_full * grad_probs, axis=-1, keepdims=True)) * HEAD_DIM ** -0.5).astype(jnp.bfloat16)
    grad_v = head_mix('hqk,qhe->khe', prob_lo, grad_attn).astype(jnp.bfloat16)
    grad_q = head_mix('hqk,khe->qhe', grad_scores, k_all).astype(jnp.bfloat16)
    grad_k = head_mix('hqk,qhe->khe', grad_scores, q_all).astype(jnp.bfloat16)
    grad_qkv = jnp.concatenate([grad_q.reshape(SEQ, D), grad_k.reshape(SEQ, D), grad_v.reshape(SEQ, D)], axis=-1)
    grad_qkv_w = mat_tn(u_one, grad_qkv)
    grad_u_one = mat_nt(grad_qkv, w_qkv)
    grad_x_norm, grad_gain_a = norm_a_back(grad_u_one.astype(jnp.float32))
    grad_x_blk = (grad_hidden.astype(jnp.float32) + grad_x_norm).astype(jnp.bfloat16)
    return grad_x_blk, (grad_gain_a, grad_gain_b, grad_qkv_w, grad_out_w, grad_up_w, grad_down_w)


def reference(x_in, grad_y, gain_one, gain_two, w_qkv, w_out, w_up, w_down):
    def one_seq(grad_acc, seq_pair):
        seq_rows, seq_grad = seq_pair
        hidden_x = seq_rows
        saved_all = []
        for layer_idx in range(LAYERS):
            hidden, act_lo, saved_vals = seq_forward(hidden_x, gain_one[layer_idx], gain_two[layer_idx], w_qkv[layer_idx], w_out[layer_idx], w_up[layer_idx])
            saved_all.append(saved_vals)
            if layer_idx + 1 < LAYERS:
                hidden_x = hidden + mat_lo(act_lo, w_down[layer_idx])
        grad_cur = seq_grad
        grads_rev = []
        for layer_idx in reversed(range(LAYERS)):
            grad_cur, layer_grads = seq_backward(grad_cur, saved_all[layer_idx], w_qkv[layer_idx], w_out[layer_idx], w_up[layer_idx], w_down[layer_idx])
            grads_rev.append(layer_grads)
        grads_fwd = grads_rev[::-1]
        new_acc = tuple(grad_acc[grad_idx] + jnp.stack([layer_set[grad_idx] for layer_set in grads_fwd]) for grad_idx in range(6))
        return new_acc, grad_cur

    init_acc = (jnp.zeros((LAYERS, D), jnp.float32), jnp.zeros((LAYERS, D), jnp.float32), jnp.zeros((LAYERS, D, 3 * D), jnp.float32), jnp.zeros((LAYERS, D, D), jnp.float32), jnp.zeros((LAYERS, D, FF), jnp.float32), jnp.zeros((LAYERS, FF, D), jnp.float32))
    grad_sums, grad_x = lax.scan(one_seq, init_acc, (x_in, grad_y))
    return (grad_x, grad_sums[0] / GROUP, grad_sums[1] / GROUP, grad_sums[2] / GROUP, grad_sums[3] / GROUP, grad_sums[4] / GROUP, grad_sums[5] / GROUP)
```

```python
import functools

import jax
import jax.numpy as jnp
from jax import lax
from jax.experimental import pallas as pl
from jax.experimental.pallas import tpu as pltpu
from jax.sharding import PartitionSpec as P

NORM_EPS = 1e-6
HEAD_DIM = 64
LANES = 128
Q_BLK = 256
EXP_SCALE = HEAD_DIM ** -0.5 * 1.4426950408889634
NEG = -1e30


def rms_gain(rows_f, gain_vec):
    return rows_f * lax.rsqrt(jnp.mean(rows_f * rows_f, axis=-1, keepdims=True) + NORM_EPS) * gain_vec


def gelu_tanh(pre_act):
    return jax.nn.gelu(pre_act, approximate=True)


def dot_lo(lhs, rhs):
    return jnp.dot(lhs, rhs, preferred_element_type=jnp.float32).astype(jnp.bfloat16)


def dot_nt(lhs, rhs):
    return lax.dot_general(lhs, rhs, (((1,), (1,)), ((), ())), preferred_element_type=jnp.float32)


def dot_tn(lhs, rhs):
    return lax.dot_general(lhs, rhs, (((0,), (0,)), ((), ())), preferred_element_type=jnp.float32)


def dot_nn(lhs, rhs):
    return jnp.dot(lhs, rhs, preferred_element_type=jnp.float32)


def head_mask(ref_rows, head):
    lane = lax.broadcasted_iota(jnp.int32, ref_rows.shape, 1)
    return jnp.where(lane // HEAD_DIM == head, ref_rows, jnp.zeros_like(ref_rows))


def scores_t(k_ref, q_m, q_start):
    diag = dot_nt(k_ref[q_start:q_start + Q_BLK, :], q_m)
    key_i = lax.broadcasted_iota(jnp.int32, diag.shape, 0)
    query_i = lax.broadcasted_iota(jnp.int32, diag.shape, 1)
    diag = jnp.where(key_i <= query_i, diag, NEG)
    if q_start == 0:
        return diag
    return jnp.concatenate([dot_nt(k_ref[:q_start, :], q_m), diag], axis=0)


def attn_fwd_kernel(q_ref, k_ref, v_ref, o_ref, lse_ref, vt_ref, ot_ref):
    head = pl.program_id(1)
    seq = q_ref.shape[0]

    @pl.when(head == 0)
    def _():
        vt_ref[...] = v_ref[...].T

    rows = pl.ds(pl.multiple_of(head * HEAD_DIM, HEAD_DIM), HEAD_DIM)
    for q_start in range(0, seq, Q_BLK):
        q_end = q_start + Q_BLK
        q_m = head_mask(q_ref[q_start:q_end, :], head)
        s_t = scores_t(k_ref, q_m, q_start)
        top = jnp.max(s_t, axis=0, keepdims=True)
        p_t = jnp.exp2((s_t - top) * EXP_SCALE)
        total = jnp.sum(p_t, axis=0, keepdims=True)
        p_lo = (p_t * (1.0 / total)).astype(jnp.bfloat16)
        ot_ref[rows, q_start:q_end] = dot_nn(vt_ref[rows, :q_end], p_lo)
        lse_ref[0, pl.ds(head, 1), q_start:q_end] = top * EXP_SCALE + jnp.log2(total)

    @pl.when(head == 1)
    def _():
        o_ref[...] = ot_ref[...].T.astype(jnp.bfloat16)


def attn_bwd_kernel(q_ref, k_ref, v_ref, do_ref, lse_ref, dq_ref, dk_ref, dv_ref, kt_ref, dqt_ref, dk_acc, dv_acc):
    head = pl.program_id(1)
    seq = q_ref.shape[0]

    @pl.when(head == 0)
    def _():
        kt_ref[...] = k_ref[...].T
        dk_acc[...] = jnp.zeros_like(dk_acc)
        dv_acc[...] = jnp.zeros_like(dv_acc)

    rows = pl.ds(pl.multiple_of(head * HEAD_DIM, HEAD_DIM), HEAD_DIM)
    for q_start in range(0, seq, Q_BLK):
        q_end = q_start + Q_BLK
        q_m = head_mask(q_ref[q_start:q_end, :], head)
        do_m = head_mask(do_ref[q_start:q_end, :], head)
        s_t = scores_t(k_ref, q_m, q_start)
        p_t = jnp.exp2(s_t * EXP_SCALE - lse_ref[0, pl.ds(head, 1), q_start:q_end])
        dp_t = dot_nt(v_ref[:q_end, :], do_m)
        delta = jnp.sum(p_t * dp_t, axis=0, keepdims=True)
        ds_t = (p_t * (dp_t - delta) * HEAD_DIM ** -0.5).astype(jnp.bfloat16)
        dv_acc[:q_end, :] += dot_nn(p_t.astype(jnp.bfloat16), do_m)
        dk_acc[:q_end, :] += dot_nn(ds_t, q_m)
        dqt_ref[rows, q_start:q_end] = dot_nn(kt_ref[rows, :q_end], ds_t)

    @pl.when(head == 1)
    def _():
        dq_ref[...] = dqt_ref[...].T.astype(jnp.bfloat16)
        dk_ref[...] = dk_acc[...].astype(jnp.bfloat16)
        dv_ref[...] = dv_acc[...].astype(jnp.bfloat16)


def attn_specs(seq, n_pairs):
    def col(shift):
        return pl.BlockSpec((seq, LANES), lambda pair, head: (0, pair + shift))
    lse = pl.BlockSpec((1, 8, seq), lambda pair, head: (pair, 0, 0))
    return col, lse


def attn_forward(qkv):
    seq, width = qkv.shape[0], qkv.shape[1] // 3
    n_pairs = width // LANES
    col, lse = attn_specs(seq, n_pairs)
    return pl.pallas_call(
        attn_fwd_kernel,
        grid=(n_pairs, 2),
        in_specs=[col(0), col(n_pairs), col(2 * n_pairs)],
        out_specs=[col(0), lse],
        out_shape=[jax.ShapeDtypeStruct((seq, width), jnp.bfloat16), jax.ShapeDtypeStruct((n_pairs, 8, seq), jnp.float32)],
        scratch_shapes=[pltpu.VMEM((LANES, seq), jnp.bfloat16), pltpu.VMEM((LANES, seq), jnp.float32)],
        compiler_params=pltpu.CompilerParams(dimension_semantics=("arbitrary", "arbitrary"), vmem_limit_bytes=48 * 2 ** 20),
        cost_estimate=pl.CostEstimate(flops=16 * 10 ** 9, bytes_accessed=8 * 2 ** 20, transcendentals=8 * 10 ** 6),
        name="attn_fwd",
    )(qkv, qkv, qkv)


def attn_backward(qkv, d_out, lse_vals):
    seq, width = qkv.shape[0], qkv.shape[1] // 3
    n_pairs = width // LANES
    col, lse = attn_specs(seq, n_pairs)
    shape = jax.ShapeDtypeStruct((seq, width), jnp.bfloat16)
    return pl.pallas_call(
        attn_bwd_kernel,
        grid=(n_pairs, 2),
        in_specs=[col(0), col(n_pairs), col(2 * n_pairs), col(0), lse],
        out_specs=[col(0), col(0), col(0)],
        out_shape=[shape, shape, shape],
        scratch_shapes=[pltpu.VMEM((LANES, seq), jnp.bfloat16), pltpu.VMEM((LANES, seq), jnp.float32), pltpu.VMEM((seq, LANES), jnp.float32), pltpu.VMEM((seq, LANES), jnp.float32)],
        compiler_params=pltpu.CompilerParams(dimension_semantics=("arbitrary", "arbitrary"), vmem_limit_bytes=56 * 2 ** 20),
        cost_estimate=pl.CostEstimate(flops=40 * 10 ** 9, bytes_accessed=14 * 2 ** 20, transcendentals=8 * 10 ** 6),
        name="attn_bwd",
    )(qkv, qkv, qkv, d_out, lse_vals)


def block_forward(x_blk, gain_a, gain_b, w_qkv, w_out, w_up):
    norm_a, norm_a_back = jax.vjp(rms_gain, x_blk.astype(jnp.float32), gain_a)
    u_one = norm_a.astype(jnp.bfloat16)
    qkv = dot_lo(u_one, w_qkv)
    attn_out, lse_vals = attn_forward(qkv)
    hidden = x_blk + dot_lo(attn_out, w_out)
    norm_b, norm_b_back = jax.vjp(rms_gain, hidden.astype(jnp.float32), gain_b)
    u_two = norm_b.astype(jnp.bfloat16)
    pre_lo = dot_lo(u_two, w_up)
    act_f, gelu_back = jax.vjp(gelu_tanh, pre_lo.astype(jnp.float32))
    act_lo = act_f.astype(jnp.bfloat16)
    return hidden, act_lo, (norm_a_back, u_one, qkv, lse_vals, attn_out, norm_b_back, u_two, gelu_back, act_lo)


def block_backward(grad_blk, saved_vals, w_qkv, w_out, w_up, w_down, reduce_fn):
    (norm_a_back, u_one, qkv, lse_vals, attn_out, norm_b_back, u_two, gelu_back, act_lo) = saved_vals
    width = grad_blk.shape[1]
    red_down = reduce_fn(dot_tn(act_lo, grad_blk))
    grad_act = dot_nt(grad_blk, w_down).astype(jnp.bfloat16)
    (grad_pre_f,) = gelu_back(grad_act.astype(jnp.float32))
    grad_pre = grad_pre_f.astype(jnp.bfloat16)
    red_up = reduce_fn(dot_tn(u_two, grad_pre))
    grad_u_two = dot_nt(grad_pre, w_up).astype(jnp.bfloat16)
    grad_h_norm, grad_gain_b = norm_b_back(grad_u_two.astype(jnp.float32))
    grad_hidden = (grad_blk.astype(jnp.float32) + grad_h_norm).astype(jnp.bfloat16)
    red_out = reduce_fn(dot_tn(attn_out, grad_hidden))
    grad_attn = dot_nt(grad_hidden, w_out).astype(jnp.bfloat16)
    grad_qkv = jnp.concatenate(attn_backward(qkv, grad_attn, lse_vals), axis=1)
    red_qkv = reduce_fn(dot_tn(u_one, grad_qkv))
    grad_u_one = dot_nt(grad_qkv, w_qkv).astype(jnp.bfloat16)
    grad_x_norm, grad_gain_a = norm_a_back(grad_u_one.astype(jnp.float32))
    grad_x_blk = (grad_hidden.astype(jnp.float32) + grad_x_norm).astype(jnp.bfloat16)
    return grad_x_blk, grad_gain_a, grad_gain_b, red_qkv, red_out, red_up, red_down


def swap_perm(n_dev, bit):
    return [(dev, dev ^ (1 << bit)) for dev in range(n_dev)]


def pick(arr, axis, index):
    return lax.squeeze(lax.dynamic_slice_in_dim(arr, index, 1, axis), (axis,))


def reduce_gather(grad_w, n_dev):
    n_bits = n_dev.bit_length() - 1
    me = lax.axis_index('data')
    bits = [(me >> bit) & 1 for bit in range(n_bits)]
    n_rows, n_cols = grad_w.shape
    shard_rows = n_rows // n_dev
    n_color = n_bits - 1
    view = grad_w.reshape((2,) * n_bits + (shard_rows, n_cols))
    core_axis = n_bits - 1
    sent = pick(view, core_axis, 1 - bits[0]).astype(jnp.bfloat16)
    got = lax.ppermute(sent, 'data', swap_perm(n_dev, 0))
    mine = pick(view, core_axis, bits[0])
    shards = []
    width = n_cols // n_color
    for color in range(n_color):
        cols = slice(color * width, (color + 1) * width)
        terms = [mine[..., cols], got[..., cols]]
        left = list(range(n_bits - 1, 0, -1))
        for step in range(n_color):
            bit = 1 + (color + step) % n_color
            axis = left.index(bit)
            out_terms = [pick(term, axis, 1 - bits[bit]) for term in terms]
            terms = [pick(term, axis, bits[bit]) for term in terms]
            out = functools.reduce(lambda acc, term: acc + term.astype(jnp.float32), out_terms[1:], out_terms[0])
            terms.append(lax.ppermute(out.astype(jnp.bfloat16), 'data', swap_perm(n_dev, bit)))
            left.remove(bit)
        total = functools.reduce(lambda acc, term: acc + term.astype(jnp.float32), terms[1:], terms[0])
        shards.append(total.astype(jnp.bfloat16))
    shard = jnp.concatenate(shards, axis=1)
    return lax.all_gather(shard, 'data', axis=0, tiled=True)


def solution(mesh):
    n_dev = mesh.shape['data']

    def local_step(x_loc, grad_y_loc, gain_one, gain_two, w_qkv, w_out, w_up, w_down):
        n_layers = w_qkv.shape[0]
        reduce_fn = functools.partial(reduce_gather, n_dev=n_dev)
        hidden_x = x_loc[0]
        saved_all = []
        for layer_idx in range(n_layers):
            hidden, act_lo, saved_vals = block_forward(hidden_x, gain_one[layer_idx], gain_two[layer_idx], w_qkv[layer_idx], w_out[layer_idx], w_up[layer_idx])
            saved_all.append(saved_vals)
            if layer_idx + 1 < n_layers:
                hidden_x = hidden + dot_lo(act_lo, w_down[layer_idx])
        grad_cur = grad_y_loc[0]
        layers_rev = []
        for layer_idx in reversed(range(n_layers)):
            out = block_backward(grad_cur, saved_all[layer_idx], w_qkv[layer_idx], w_out[layer_idx], w_up[layer_idx], w_down[layer_idx], reduce_fn)
            grad_cur = out[0]
            layers_rev.append(out[1:])
        layers = layers_rev[::-1]
        gains = jnp.stack([layer[0] for layer in layers] + [layer[1] for layer in layers])
        gains = lax.psum(gains, 'data') / n_dev
        weights = tuple(jnp.stack([layer[idx] for layer in layers]).astype(jnp.float32) / n_dev for idx in range(2, 6))
        return (grad_cur[None], gains[:n_layers], gains[n_layers:]) + weights

    batch_spec = P('data')
    full_spec = P()
    return jax.shard_map(local_step, mesh=mesh, in_specs=(batch_spec, batch_spec) + (full_spec,) * 6, out_specs=(batch_spec,) + (full_spec,) * 6, check_vma=False)
```

```python
import functools

import jax
import jax.numpy as jnp
from jax import lax
from jax.experimental import pallas as pl
from jax.experimental.pallas import tpu as pltpu
from jax.sharding import PartitionSpec as P

NORM_EPS = 1e-6
HEAD_DIM = 64
LANES = 128
Q_BLK = 256
EXP_SCALE = HEAD_DIM ** -0.5 * 1.4426950408889634
NEG = -1e30


def rms_gain(rows_f, gain_vec):
    return rows_f * lax.rsqrt(jnp.mean(rows_f * rows_f, axis=-1, keepdims=True) + NORM_EPS) * gain_vec


def gelu_tanh(pre_act):
    return jax.nn.gelu(pre_act, approximate=True)


def dot_lo(lhs, rhs):
    return jnp.dot(lhs, rhs, preferred_element_type=jnp.float32).astype(jnp.bfloat16)


def dot_nt(lhs, rhs):
    return lax.dot_general(lhs, rhs, (((1,), (1,)), ((), ())), preferred_element_type=jnp.float32)


def dot_tn(lhs, rhs):
    return lax.dot_general(lhs, rhs, (((0,), (0,)), ((), ())), preferred_element_type=jnp.float32)


def dot_nn(lhs, rhs):
    return jnp.dot(lhs, rhs, preferred_element_type=jnp.float32)


def head_mask(ref_rows, head):
    lane = lax.broadcasted_iota(jnp.int32, ref_rows.shape, 1)
    return jnp.where(lane // HEAD_DIM == head, ref_rows, jnp.zeros_like(ref_rows))


def scores_t(k_ref, q_m, q_start):
    diag = dot_nt(k_ref[q_start:q_start + Q_BLK, :], q_m)
    key_i = lax.broadcasted_iota(jnp.int32, diag.shape, 0)
    query_i = lax.broadcasted_iota(jnp.int32, diag.shape, 1)
    diag = jnp.where(key_i <= query_i, diag, NEG)
    if q_start == 0:
        return diag
    return jnp.concatenate([dot_nt(k_ref[:q_start, :], q_m), diag], axis=0)


def attn_fwd_kernel(q_ref, k_ref, v_ref, o_ref, lse_ref, vt_ref, ot_ref):
    head = pl.program_id(1)
    seq = q_ref.shape[0]

    @pl.when(head == 0)
    def _():
        vt_ref[...] = v_ref[...].T

    rows = pl.ds(pl.multiple_of(head * HEAD_DIM, HEAD_DIM), HEAD_DIM)
    for q_start in range(0, seq, Q_BLK):
        q_end = q_start + Q_BLK
        q_m = head_mask(q_ref[q_start:q_end, :], head)
        s_t = scores_t(k_ref, q_m, q_start)
        top = jnp.max(s_t, axis=0, keepdims=True)
        p_t = jnp.exp2((s_t - top) * EXP_SCALE)
        total = jnp.sum(p_t, axis=0, keepdims=True)
        p_lo = (p_t * (1.0 / total)).astype(jnp.bfloat16)
        ot_ref[rows, q_start:q_end] = dot_nn(vt_ref[rows, :q_end], p_lo)
        lse_ref[0, pl.ds(head, 1), q_start:q_end] = top * EXP_SCALE + jnp.log2(total)

    @pl.when(head == 1)
    def _():
        o_ref[...] = ot_ref[...].T.astype(jnp.bfloat16)


N_COLOR = 3
SUB_ROWS = 48
UNIT_COLS = 768
AXIS_BITS = (3, 2, 1)
MESH = pl.DeviceIdType.MESH


class Reducer:
    def __init__(self, grad_refs, units, refs):
        (self.own, self.send0, self.recv0, self.send1, self.recv1, self.send2, self.recv2, self.send3, self.recv3, self.load_sem, self.send_sem, self.recv_sem) = refs
        self.grad_refs, self.units = grad_refs, units
        self.n_chunks = len(units) // N_COLOR
        me = lax.axis_index('data')
        self.me = me
        self.bit = [lax.rem(lax.div(me, 1 << b), 2) for b in range(4)]
        self.partner = [me + (1 - 2 * self.bit[b]) * (1 << b) for b in range(4)]

    def barrier(self):
        sem = pltpu.get_barrier_semaphore()
        for dev in self.partner:
            pl.semaphore_signal(sem, inc=1, device_id=(dev,), device_id_type=MESH)
        pl.semaphore_wait(sem, 4)

    def load(self, chunk, half):
        for color in range(N_COLOR):
            array, row, col = self.units[chunk * N_COLOR + color]
            src = self.grad_refs[array].at[:, half, pl.ds(row, SUB_ROWS), pl.ds(col, UNIT_COLS)]
            pltpu.make_async_copy(src, self.own.at[chunk, color], self.load_sem.at[chunk, color]).start()

    def wait_load(self, chunk):
        for color in range(N_COLOR):
            ref = self.own.at[chunk, color]
            pltpu.make_async_copy(ref, ref, self.load_sem.at[chunk, color]).wait()

    def copy(self, stage, chunk, color):
        send = (self.send0, self.send1, self.send2, self.send3)[stage].at[chunk, color]
        recv = (self.recv0, self.recv1, self.recv2, self.recv3)[stage].at[chunk, color]
        dev = self.partner[0] if stage == 0 else self.partner[self.order(color)[stage - 1]]
        return pltpu.make_async_remote_copy(src_ref=send, dst_ref=recv, send_sem=self.send_sem.at[stage, chunk, color], recv_sem=self.recv_sem.at[stage, chunk, color], device_id=(dev,), device_id_type=MESH)

    def order(self, color):
        return [1 + (color + step) % N_COLOR for step in range(N_COLOR)]

    def block(self, values):
        return values[3] * 4 + values[2] * 2 + values[1]

    def convert(self, chunk):
        self.wait_load(chunk)
        for color in range(N_COLOR):
            def body(i, carry):
                self.send0[chunk, color, i] = self.own[chunk, color, i].astype(jnp.bfloat16)
                return carry
            lax.fori_loop(0, 8, body, 0)
            self.copy(0, chunk, color).start()

    def total(self, chunk, color, values, n_recv):
        order = self.order(color)
        index = self.block(values)
        acc = self.own[chunk, color, index] + self.recv0[chunk, color, index].astype(jnp.float32)
        if n_recv >= 2:
            acc = acc + self.recv1[chunk, color, values[order[1]] * 2 + values[order[2]]].astype(jnp.float32)
        if n_recv >= 3:
            acc = acc + self.recv2[chunk, color, values[order[2]]].astype(jnp.float32)
        if n_recv >= 4:
            acc = acc + self.recv3[chunk, color, 0].astype(jnp.float32)
        return acc

    def stage(self, step, chunk):
        if step == 1:
            self.wait_load(chunk)
        send = (None, self.send1, self.send2, self.send3)[step]
        n_free = N_COLOR - step
        for color in range(N_COLOR):
            self.copy(step - 1, chunk, color).wait_recv()
            order = self.order(color)

            def body(i, carry):
                values = [0, 0, 0, 0]
                for done in range(step - 1):
                    values[order[done]] = self.bit[order[done]]
                values[order[step - 1]] = 1 - self.bit[order[step - 1]]
                if n_free == 2:
                    values[order[1]], values[order[2]] = lax.div(i, 2), lax.rem(i, 2)
                elif n_free == 1:
                    values[order[2]] = i
                send[chunk, color, i] = self.total(chunk, color, values, step).astype(jnp.bfloat16)
                return carry
            if n_free:
                lax.fori_loop(0, 1 << n_free, body, 0)
            else:
                body(0, 0)
            self.copy(step, chunk, color).start()

    def finish(self, chunk, out_ref):
        for color in range(N_COLOR):
            self.copy(3, chunk, color).wait_recv()
            out_ref[chunk * N_COLOR + color] = self.total(chunk, color, self.bit, 4).astype(jnp.bfloat16)
        for stage in range(4):
            for color in range(N_COLOR):
                self.copy(stage, chunk, color).wait_send()


def reducer_scratch(n_chunks):
    def buf(blocks, dtype):
        return pltpu.VMEM((n_chunks, N_COLOR, blocks, SUB_ROWS, UNIT_COLS), dtype)
    lo = jnp.bfloat16
    return [buf(8, jnp.float32), buf(8, lo), buf(8, lo), buf(4, lo), buf(4, lo), buf(2, lo), buf(2, lo), buf(1, lo), buf(1, lo), pltpu.SemaphoreType.DMA((n_chunks, N_COLOR)), pltpu.SemaphoreType.DMA((4, n_chunks, N_COLOR)), pltpu.SemaphoreType.DMA((4, n_chunks, N_COLOR))]


N_REDUCER_REFS = 12


def grad_view(grad_w):
    rows, cols = grad_w.shape
    return grad_w.reshape(8, 2, rows // 16, cols)


def grad_units(grads):
    units = []
    for array, grad_w in enumerate(grads):
        rows, cols = grad_w.shape
        for row in range(0, rows // 16, SUB_ROWS):
            for col in range(0, cols, UNIT_COLS):
                units.append((array, row, col))
    return units


def attn_bwd_kernel(units, n_grads, *refs):
    q_ref, k_ref, v_ref, do_ref, lse_ref = refs[:5]
    grad_refs = refs[5:5 + n_grads]
    dq_ref, dk_ref, dv_ref, shard_ref, kt_ref, dqt_ref, dk_acc, dv_acc = refs[5 + n_grads:13 + n_grads]
    red = Reducer(grad_refs, units, refs[13 + n_grads:])
    n_chunks = red.n_chunks
    head = pl.program_id(1)
    step = pl.program_id(0) * 2 + head
    last = 2 * pl.num_programs(0) - 1
    seq = q_ref.shape[0]

    @pl.when(step == 0)
    def _():
        red.barrier()
        for chunk in range(n_chunks):
            red.load(chunk, 1 - red.bit[0])

    for chunk in range(n_chunks):
        @pl.when(step == max(chunk - 1, 0))
        def _():
            red.convert(chunk)
            red.load(chunk, red.bit[0])

    @pl.when((step >= 1) & (step <= n_chunks))
    def _():
        red.stage(1, step - 1)

    @pl.when((step >= 4) & (step < 4 + 2 * n_chunks) & (lax.rem(step, 2) == 0))
    def _():
        red.stage(2, lax.div(step - 4, 2))

    @pl.when((step >= 9) & (step < 9 + n_chunks))
    def _():
        red.stage(3, step - 9)

    @pl.when(head == 0)
    def _():
        kt_ref[...] = k_ref[...].T
        dk_acc[...] = jnp.zeros_like(dk_acc)
        dv_acc[...] = jnp.zeros_like(dv_acc)

    rows = pl.ds(pl.multiple_of(head * HEAD_DIM, HEAD_DIM), HEAD_DIM)
    for q_start in range(0, seq, Q_BLK):
        q_end = q_start + Q_BLK
        q_m = head_mask(q_ref[q_start:q_end, :], head)
        do_m = head_mask(do_ref[q_start:q_end, :], head)
        s_t = scores_t(k_ref, q_m, q_start)
        p_t = jnp.exp2(s_t * EXP_SCALE - lse_ref[0, pl.ds(head, 1), q_start:q_end])
        dp_t = dot_nt(v_ref[:q_end, :], do_m)
        delta = jnp.sum(p_t * dp_t, axis=0, keepdims=True)
        ds_t = (p_t * (dp_t - delta) * HEAD_DIM ** -0.5).astype(jnp.bfloat16)
        dv_acc[:q_end, :] += dot_nn(p_t.astype(jnp.bfloat16), do_m)
        dk_acc[:q_end, :] += dot_nn(ds_t, q_m)
        dqt_ref[rows, q_start:q_end] = dot_nn(kt_ref[rows, :q_end], ds_t)

    @pl.when(head == 1)
    def _():
        dq_ref[...] = dqt_ref[...].T.astype(jnp.bfloat16)
        dk_ref[...] = dk_acc[...].astype(jnp.bfloat16)
        dv_ref[...] = dv_acc[...].astype(jnp.bfloat16)

    @pl.when(step == last)
    def _():
        for chunk in range(n_chunks):
            if 9 + chunk > 11:
                red.stage(3, chunk)
        for chunk in range(n_chunks):
            red.finish(chunk, shard_ref)


def tail_kernel(units, n_grads, *refs):
    gains_ref = refs[0]
    grad_refs = refs[1:1 + n_grads]
    shard_ref, gsum_ref, gbuf, gsend_sem, grecv_sem = refs[1 + n_grads:6 + n_grads]
    red = Reducer(grad_refs, units, refs[6 + n_grads:])
    n_dev = gbuf.shape[0]
    for chunk in range(red.n_chunks):
        red.load(chunk, 1 - red.bit[0])
    sem = pltpu.get_barrier_semaphore()
    for shift in range(1, n_dev):
        pl.semaphore_signal(sem, inc=1, device_id=(lax.rem(red.me + shift, n_dev),), device_id_type=MESH)
    pl.semaphore_wait(sem, n_dev - 1)

    def gain_copy(shift):
        dev = lax.rem(red.me + shift, n_dev)
        return pltpu.make_async_remote_copy(src_ref=gains_ref, dst_ref=gbuf.at[shift], send_sem=gsend_sem.at[shift], recv_sem=grecv_sem.at[shift], device_id=(dev,), device_id_type=MESH)
    for shift in range(1, n_dev):
        gain_copy(shift).start()
    gbuf[0] = gains_ref[...]
    for chunk in range(red.n_chunks):
        red.convert(chunk)
        red.load(chunk, red.bit[0])
    for step in range(1, 4):
        for chunk in range(red.n_chunks):
            red.stage(step, chunk)
    for shift in range(1, n_dev):
        gain_copy(shift).wait()
    acc = jnp.zeros(gains_ref.shape, jnp.float32)
    for dev in range(n_dev):
        acc = acc + gbuf[lax.rem(red.me + n_dev - dev, n_dev)]
    gsum_ref[...] = acc
    for chunk in range(red.n_chunks):
        red.finish(chunk, shard_ref)


def attn_specs(seq, n_pairs):
    def col(shift):
        return pl.BlockSpec((seq, LANES), lambda pair, head: (0, pair + shift))
    lse = pl.BlockSpec((1, 8, seq), lambda pair, head: (pair, 0, 0))
    return col, lse


def attn_forward(qkv):
    seq, width = qkv.shape[0], qkv.shape[1] // 3
    n_pairs = width // LANES
    col, lse = attn_specs(seq, n_pairs)
    return pl.pallas_call(
        attn_fwd_kernel,
        grid=(n_pairs, 2),
        in_specs=[col(0), col(n_pairs), col(2 * n_pairs)],
        out_specs=[col(0), lse],
        out_shape=[jax.ShapeDtypeStruct((seq, width), jnp.bfloat16), jax.ShapeDtypeStruct((n_pairs, 8, seq), jnp.float32)],
        scratch_shapes=[pltpu.VMEM((LANES, seq), jnp.bfloat16), pltpu.VMEM((LANES, seq), jnp.float32)],
        compiler_params=pltpu.CompilerParams(dimension_semantics=("arbitrary", "arbitrary"), vmem_limit_bytes=48 * 2 ** 20),
        cost_estimate=pl.CostEstimate(flops=16 * 10 ** 9, bytes_accessed=8 * 2 ** 20, transcendentals=8 * 10 ** 6),
        name="attn_fwd",
    )(qkv, qkv, qkv)


def attn_backward(qkv, d_out, lse_vals, grads, call_id):
    seq, width = qkv.shape[0], qkv.shape[1] // 3
    n_pairs = width // LANES
    col, lse = attn_specs(seq, n_pairs)
    shape = jax.ShapeDtypeStruct((seq, width), jnp.bfloat16)
    units = grad_units(grads)
    shard_shape = (len(units), SUB_ROWS, UNIT_COLS)
    out = pl.pallas_call(
        functools.partial(attn_bwd_kernel, units, len(grads)),
        grid=(n_pairs, 2),
        in_specs=[col(0), col(n_pairs), col(2 * n_pairs), col(0), lse] + [pl.BlockSpec(memory_space=pl.ANY)] * len(grads),
        out_specs=[col(0), col(0), col(0), pl.BlockSpec(shard_shape, lambda pair, head: (0, 0, 0))],
        out_shape=[shape, shape, shape, jax.ShapeDtypeStruct(shard_shape, jnp.bfloat16)],
        scratch_shapes=[pltpu.VMEM((LANES, seq), jnp.bfloat16), pltpu.VMEM((LANES, seq), jnp.float32), pltpu.VMEM((seq, LANES), jnp.float32), pltpu.VMEM((seq, LANES), jnp.float32)] + reducer_scratch(len(units) // N_COLOR),
        compiler_params=pltpu.CompilerParams(dimension_semantics=("arbitrary", "arbitrary"), vmem_limit_bytes=67043328, collective_id=call_id, has_side_effects=True),
        cost_estimate=pl.CostEstimate(flops=40 * 10 ** 9, bytes_accessed=14 * 2 ** 20, transcendentals=8 * 10 ** 6),
        name="attn_bwd",
    )(qkv, qkv, qkv, d_out, lse_vals, *[grad_view(grad_w) for grad_w in grads])
    return out[:3], out[3]


def tail_reduce(gains, grads, call_id, n_dev):
    units = grad_units(grads)
    shard_shape = (len(units), SUB_ROWS, UNIT_COLS)
    return pl.pallas_call(
        functools.partial(tail_kernel, units, len(grads)),
        in_specs=[pl.BlockSpec(memory_space=pltpu.VMEM)] + [pl.BlockSpec(memory_space=pl.ANY)] * len(grads),
        out_specs=[pl.BlockSpec(memory_space=pltpu.VMEM)] * 2,
        out_shape=[jax.ShapeDtypeStruct(shard_shape, jnp.bfloat16), jax.ShapeDtypeStruct(gains.shape, jnp.float32)],
        scratch_shapes=[pltpu.VMEM((n_dev,) + gains.shape, jnp.float32), pltpu.SemaphoreType.DMA((n_dev,)), pltpu.SemaphoreType.DMA((n_dev,))] + reducer_scratch(len(units) // N_COLOR),
        compiler_params=pltpu.CompilerParams(vmem_limit_bytes=40 * 2 ** 20, collective_id=call_id, has_side_effects=True),
        cost_estimate=pl.CostEstimate(flops=20 * 10 ** 9, bytes_accessed=14 * 2 ** 20, transcendentals=0),
        name="tail_reduce",
    )(gains, *[grad_view(grad_w) for grad_w in grads])


def block_forward(x_blk, gain_a, gain_b, w_qkv, w_out, w_up):
    norm_a, norm_a_back = jax.vjp(rms_gain, x_blk.astype(jnp.float32), gain_a)
    u_one = norm_a.astype(jnp.bfloat16)
    qkv = dot_lo(u_one, w_qkv)
    attn_out, lse_vals = attn_forward(qkv)
    hidden = x_blk + dot_lo(attn_out, w_out)
    norm_b, norm_b_back = jax.vjp(rms_gain, hidden.astype(jnp.float32), gain_b)
    u_two = norm_b.astype(jnp.bfloat16)
    pre_lo = dot_lo(u_two, w_up)
    act_f, gelu_back = jax.vjp(gelu_tanh, pre_lo.astype(jnp.float32))
    act_lo = act_f.astype(jnp.bfloat16)
    return hidden, act_lo, (norm_a_back, u_one, qkv, lse_vals, attn_out, norm_b_back, u_two, gelu_back, act_lo)


def block_backward(grad_blk, saved_vals, w_qkv, w_out, w_up, w_down, ready, call_id):
    (norm_a_back, u_one, qkv, lse_vals, attn_out, norm_b_back, u_two, gelu_back, act_lo) = saved_vals
    grad_down_w = dot_tn(act_lo, grad_blk)
    grad_act = dot_nt(grad_blk, w_down).astype(jnp.bfloat16)
    (grad_pre_f,) = gelu_back(grad_act.astype(jnp.float32))
    grad_pre = grad_pre_f.astype(jnp.bfloat16)
    grad_up_w = dot_tn(u_two, grad_pre)
    grad_u_two = dot_nt(grad_pre, w_up).astype(jnp.bfloat16)
    grad_h_norm, grad_gain_b = norm_b_back(grad_u_two.astype(jnp.float32))
    grad_hidden = (grad_blk.astype(jnp.float32) + grad_h_norm).astype(jnp.bfloat16)
    grad_out_w = dot_tn(attn_out, grad_hidden)
    grad_attn = dot_nt(grad_hidden, w_out).astype(jnp.bfloat16)
    pieces, shard = attn_backward(qkv, grad_attn, lse_vals, ready + [grad_down_w, grad_up_w, grad_out_w], call_id)
    grad_qkv = jnp.concatenate(pieces, axis=1)
    grad_qkv_w = dot_tn(u_one, grad_qkv)
    grad_u_one = dot_nt(grad_qkv, w_qkv).astype(jnp.bfloat16)
    grad_x_norm, grad_gain_a = norm_a_back(grad_u_one.astype(jnp.float32))
    grad_x_blk = (grad_hidden.astype(jnp.float32) + grad_x_norm).astype(jnp.bfloat16)
    return grad_x_blk, grad_gain_a, grad_gain_b, grad_qkv_w, shard


def unit_gather(shard):
    n_units = shard.shape[0]
    flat = lax.all_gather(shard.reshape(n_units * SUB_ROWS, UNIT_COLS), 'data', axis=0, tiled=True)
    return flat.reshape(-1, n_units, SUB_ROWS, UNIT_COLS)


def rows_of(gathered, first):
    piece = gathered[:, first:first + 4]
    return piece.reshape(-1, UNIT_COLS)


def cols_of(gathered, first, count):
    piece = gathered[:, first:first + count]
    n_dev = piece.shape[0]
    return piece.transpose(0, 2, 1, 3).reshape(n_dev * SUB_ROWS, count * UNIT_COLS)


def solution(mesh):
    n_dev = mesh.shape['data']

    def local_step(x_loc, grad_y_loc, gain_one, gain_two, w_qkv, w_out, w_up, w_down):
        n_layers = w_qkv.shape[0]
        hidden_x = x_loc[0]
        saved_all = []
        for layer_idx in range(n_layers):
            hidden, act_lo, saved_vals = block_forward(hidden_x, gain_one[layer_idx], gain_two[layer_idx], w_qkv[layer_idx], w_out[layer_idx], w_up[layer_idx])
            saved_all.append(saved_vals)
            if layer_idx + 1 < n_layers:
                hidden_x = hidden + dot_lo(act_lo, w_down[layer_idx])
        grad_cur = grad_y_loc[0]
        gains = [None] * (2 * n_layers)
        ready = []
        gathered = []
        for layer_idx in reversed(range(n_layers)):
            out = block_backward(grad_cur, saved_all[layer_idx], w_qkv[layer_idx], w_out[layer_idx], w_up[layer_idx], w_down[layer_idx], ready, n_layers - 1 - layer_idx)
            grad_cur, gains[layer_idx], gains[n_layers + layer_idx], grad_qkv_w, shard = out
            ready = [grad_qkv_w]
            gathered.append(unit_gather(shard))
        gain_rows = jnp.concatenate([jnp.stack(gains), jnp.zeros((8 - 2 * n_layers, gains[0].shape[0]), jnp.float32)])
        shard, gain_sums = tail_reduce(gain_rows, ready, n_layers, n_dev)
        gathered.append(unit_gather(shard))
        gain_sums = gain_sums / n_dev
        top, low, last = gathered
        pairs = [(cols_of(last, 0, 3), cols_of(low, 0, 3)), (cols_of(low, 11, 1), cols_of(top, 8, 1)), (cols_of(low, 7, 4), cols_of(top, 4, 4)), (rows_of(low, 3), rows_of(top, 0))]
        weights = tuple(jnp.stack(pair).astype(jnp.float32) / n_dev for pair in pairs)
        return (grad_cur[None], gain_sums[:n_layers], gain_sums[n_layers:2 * n_layers]) + weights

    batch_spec = P('data')
    full_spec = P()
    return jax.shard_map(local_step, mesh=mesh, in_specs=(batch_spec, batch_spec) + (full_spec,) * 6, out_specs=(batch_spec,) + (full_spec,) * 6, check_vma=False)
```

```python
import functools

import jax
import jax.numpy as jnp
from jax import lax
from jax.experimental import pallas as pl
from jax.experimental.pallas import tpu as pltpu
from jax.sharding import PartitionSpec as P

NORM_EPS = 1e-6
HEAD_DIM = 64
LANES = 128
Q_BLK = 256
EXP_SCALE = HEAD_DIM ** -0.5 * 1.4426950408889634
NEG = -1e30


def rms_gain(rows_f, gain_vec):
    return rows_f * lax.rsqrt(jnp.mean(rows_f * rows_f, axis=-1, keepdims=True) + NORM_EPS) * gain_vec


def gelu_tanh(pre_act):
    return jax.nn.gelu(pre_act, approximate=True)


def dot_lo(lhs, rhs):
    return jnp.dot(lhs, rhs, preferred_element_type=jnp.float32).astype(jnp.bfloat16)


def dot_nt(lhs, rhs):
    return lax.dot_general(lhs, rhs, (((1,), (1,)), ((), ())), preferred_element_type=jnp.float32)


def dot_tn(lhs, rhs):
    return lax.dot_general(lhs, rhs, (((0,), (0,)), ((), ())), preferred_element_type=jnp.float32)


def dot_nn(lhs, rhs):
    return jnp.dot(lhs, rhs, preferred_element_type=jnp.float32)


def head_mask(ref_rows, head):
    lane = lax.broadcasted_iota(jnp.int32, ref_rows.shape, 1)
    return jnp.where(lane // HEAD_DIM == head, ref_rows, jnp.zeros_like(ref_rows))


def scores_t(k_ref, q_m, q_start):
    diag = dot_nt(k_ref[q_start:q_start + Q_BLK, :], q_m)
    key_i = lax.broadcasted_iota(jnp.int32, diag.shape, 0)
    query_i = lax.broadcasted_iota(jnp.int32, diag.shape, 1)
    diag = jnp.where(key_i <= query_i, diag, NEG)
    if q_start == 0:
        return diag
    return jnp.concatenate([dot_nt(k_ref[:q_start, :], q_m), diag], axis=0)


def attn_fwd_kernel(q_ref, k_ref, v_ref, o_ref, lse_ref, vt_ref, ot_ref):
    head = pl.program_id(1)
    seq = q_ref.shape[0]

    @pl.when(head == 0)
    def _():
        vt_ref[...] = v_ref[...].T

    rows = pl.ds(pl.multiple_of(head * HEAD_DIM, HEAD_DIM), HEAD_DIM)
    for q_start in range(0, seq, Q_BLK):
        q_end = q_start + Q_BLK
        q_m = head_mask(q_ref[q_start:q_end, :], head)
        s_t = scores_t(k_ref, q_m, q_start)
        top = jnp.max(s_t, axis=0, keepdims=True)
        p_t = jnp.exp2((s_t - top) * EXP_SCALE)
        total = jnp.sum(p_t, axis=0, keepdims=True)
        p_lo = (p_t * (1.0 / total)).astype(jnp.bfloat16)
        ot_ref[rows, q_start:q_end] = dot_nn(vt_ref[rows, :q_end], p_lo)
        lse_ref[0, pl.ds(head, 1), q_start:q_end] = top * EXP_SCALE + jnp.log2(total)

    @pl.when(head == 1)
    def _():
        o_ref[...] = ot_ref[...].T.astype(jnp.bfloat16)


N_COLOR = 3
SUB_ROWS = 48
UNIT_COLS = 768
AXIS_BITS = (3, 2, 1)
MESH = pl.DeviceIdType.MESH


class Reducer:
    def __init__(self, grad_refs, units, refs):
        (self.own, self.send0, self.recv0, self.send1, self.recv1, self.send2, self.recv2, self.send3, self.recv3, self.load_sem, self.send_sem, self.recv_sem) = refs
        self.grad_refs, self.units = grad_refs, units
        self.n_chunks = len(units) // N_COLOR
        me = lax.axis_index('data')
        self.me = me
        self.bit = [lax.rem(lax.div(me, 1 << b), 2) for b in range(4)]
        self.partner = [me + (1 - 2 * self.bit[b]) * (1 << b) for b in range(4)]

    def barrier(self):
        sem = pltpu.get_barrier_semaphore()
        for dev in self.partner:
            pl.semaphore_signal(sem, inc=1, device_id=(dev,), device_id_type=MESH)
        pl.semaphore_wait(sem, 4)

    def load(self, chunk, half):
        for color in range(N_COLOR):
            array, row, col = self.units[chunk * N_COLOR + color]
            src = self.grad_refs[array].at[:, half, pl.ds(row, SUB_ROWS), pl.ds(col, UNIT_COLS)]
            pltpu.make_async_copy(src, self.own.at[chunk, color], self.load_sem.at[chunk, color]).start()

    def wait_load(self, chunk):
        for color in range(N_COLOR):
            ref = self.own.at[chunk, color]
            pltpu.make_async_copy(ref, ref, self.load_sem.at[chunk, color]).wait()

    def copy(self, stage, chunk, color):
        send = (self.send0, self.send1, self.send2, self.send3)[stage].at[chunk, color]
        recv = (self.recv0, self.recv1, self.recv2, self.recv3)[stage].at[chunk, color]
        dev = self.partner[0] if stage == 0 else self.partner[self.order(color)[stage - 1]]
        return pltpu.make_async_remote_copy(src_ref=send, dst_ref=recv, send_sem=self.send_sem.at[stage, chunk, color], recv_sem=self.recv_sem.at[stage, chunk, color], device_id=(dev,), device_id_type=MESH)

    def order(self, color):
        return [1 + (color + step) % N_COLOR for step in range(N_COLOR)]

    def block(self, values):
        return values[3] * 4 + values[2] * 2 + values[1]

    def convert(self, chunk):
        self.wait_load(chunk)
        for color in range(N_COLOR):
            def body(i, carry):
                self.send0[chunk, color, i] = self.own[chunk, color, i].astype(jnp.bfloat16)
                return carry
            lax.fori_loop(0, 8, body, 0)
            self.copy(0, chunk, color).start()

    def total(self, chunk, color, values, n_recv):
        order = self.order(color)
        index = self.block(values)
        acc = self.own[chunk, color, index] + self.recv0[chunk, color, index].astype(jnp.float32)
        if n_recv >= 2:
            acc = acc + self.recv1[chunk, color, values[order[1]] * 2 + values[order[2]]].astype(jnp.float32)
        if n_recv >= 3:
            acc = acc + self.recv2[chunk, color, values[order[2]]].astype(jnp.float32)
        if n_recv >= 4:
            acc = acc + self.recv3[chunk, color, 0].astype(jnp.float32)
        return acc

    def stage(self, step, chunk):
        if step == 1:
            self.wait_load(chunk)
        send = (None, self.send1, self.send2, self.send3)[step]
        n_free = N_COLOR - step
        for color in range(N_COLOR):
            self.copy(step - 1, chunk, color).wait_recv()
            order = self.order(color)

            def body(i, carry):
                values = [0, 0, 0, 0]
                for done in range(step - 1):
                    values[order[done]] = self.bit[order[done]]
                values[order[step - 1]] = 1 - self.bit[order[step - 1]]
                if n_free == 2:
                    values[order[1]], values[order[2]] = lax.div(i, 2), lax.rem(i, 2)
                elif n_free == 1:
                    values[order[2]] = i
                send[chunk, color, i] = self.total(chunk, color, values, step).astype(jnp.bfloat16)
                return carry
            if n_free:
                lax.fori_loop(0, 1 << n_free, body, 0)
            else:
                body(0, 0)
            self.copy(step, chunk, color).start()

    def gather_copy(self, stage, chunk, color, full_ref, sems):
        order = self.order(color)
        have = [0, 0, 0, 0]
        index = []
        fixed = order[:3 - stage] if stage < 3 else []
        dev = self.partner[order[2 - stage]] if stage < 3 else self.partner[0]
        for bit in AXIS_BITS:
            index.append(pl.ds(self.bit[bit], 1) if bit in fixed else slice(None))
        ref = full_ref.at[chunk * N_COLOR + color].at[tuple(index) + (pl.ds(self.bit[0], 1),)]
        return pltpu.make_async_remote_copy(src_ref=ref, dst_ref=ref, send_sem=sems[0].at[stage, chunk, color], recv_sem=sems[1].at[stage, chunk, color], device_id=(dev,), device_id_type=MESH)

    def finish(self, chunk, out_ref):
        for color in range(N_COLOR):
            self.copy(3, chunk, color).wait_recv()
            out_ref[chunk * N_COLOR + color] = self.total(chunk, color, self.bit, 4).astype(jnp.bfloat16)
        for stage in range(4):
            for color in range(N_COLOR):
                self.copy(stage, chunk, color).wait_send()


def reducer_scratch(n_chunks):
    def buf(blocks, dtype):
        return pltpu.VMEM((n_chunks, N_COLOR, blocks, SUB_ROWS, UNIT_COLS), dtype)
    lo = jnp.bfloat16
    return [buf(8, jnp.float32), buf(8, lo), buf(8, lo), buf(4, lo), buf(4, lo), buf(2, lo), buf(2, lo), buf(1, lo), buf(1, lo), pltpu.SemaphoreType.DMA((n_chunks, N_COLOR)), pltpu.SemaphoreType.DMA((4, n_chunks, N_COLOR)), pltpu.SemaphoreType.DMA((4, n_chunks, N_COLOR))]


N_REDUCER_REFS = 12


def grad_view(grad_w):
    rows, cols = grad_w.shape
    return grad_w.reshape(8, 2, rows // 16, cols)


def grad_units(grads):
    units = []
    for array, grad_w in enumerate(grads):
        rows, cols = grad_w.shape
        for row in range(0, rows // 16, SUB_ROWS):
            for col in range(0, cols, UNIT_COLS):
                units.append((array, row, col))
    return units


def attn_bwd_kernel(units, n_grads, n_after, *refs):
    q_ref, k_ref, v_ref, do_ref, lse_ref = refs[:5]
    grad_refs = refs[5:5 + n_grads]
    refs = refs[:5 + n_grads] + refs[5 + n_grads + n_after:]
    dq_ref, dk_ref, dv_ref, shard_ref, kt_ref, dqt_ref, dk_acc, dv_acc = refs[5 + n_grads:13 + n_grads]
    red = Reducer(grad_refs, units, refs[13 + n_grads:])
    n_chunks = red.n_chunks
    head = pl.program_id(1)
    step = pl.program_id(0) * 2 + head
    last = 2 * pl.num_programs(0) - 1
    seq = q_ref.shape[0]

    @pl.when(step == 0)
    def _():
        red.barrier()
        for chunk in range(n_chunks):
            red.load(chunk, 1 - red.bit[0])

    for chunk in range(n_chunks):
        @pl.when(step == max(chunk - 1, 0))
        def _():
            red.convert(chunk)
            red.load(chunk, red.bit[0])

    @pl.when((step >= 1) & (step <= n_chunks))
    def _():
        red.stage(1, step - 1)

    @pl.when((step >= 4) & (step < 4 + 2 * n_chunks) & (lax.rem(step, 2) == 0))
    def _():
        red.stage(2, lax.div(step - 4, 2))

    @pl.when((step >= 9) & (step < 9 + n_chunks))
    def _():
        red.stage(3, step - 9)

    @pl.when(head == 0)
    def _():
        kt_ref[...] = k_ref[...].T
        dk_acc[...] = jnp.zeros_like(dk_acc)
        dv_acc[...] = jnp.zeros_like(dv_acc)

    rows = pl.ds(pl.multiple_of(head * HEAD_DIM, HEAD_DIM), HEAD_DIM)
    for q_start in range(0, seq, Q_BLK):
        q_end = q_start + Q_BLK
        q_m = head_mask(q_ref[q_start:q_end, :], head)
        do_m = head_mask(do_ref[q_start:q_end, :], head)
        s_t = scores_t(k_ref, q_m, q_start)
        p_t = jnp.exp2(s_t * EXP_SCALE - lse_ref[0, pl.ds(head, 1), q_start:q_end])
        dp_t = dot_nt(v_ref[:q_end, :], do_m)
        delta = jnp.sum(p_t * dp_t, axis=0, keepdims=True)
        ds_t = (p_t * (dp_t - delta) * HEAD_DIM ** -0.5).astype(jnp.bfloat16)
        dv_acc[:q_end, :] += dot_nn(p_t.astype(jnp.bfloat16), do_m)
        dk_acc[:q_end, :] += dot_nn(ds_t, q_m)
        dqt_ref[rows, q_start:q_end] = dot_nn(kt_ref[rows, :q_end], ds_t)

    @pl.when(head == 1)
    def _():
        dq_ref[...] = dqt_ref[...].T.astype(jnp.bfloat16)
        dk_ref[...] = dk_acc[...].astype(jnp.bfloat16)
        dv_ref[...] = dv_acc[...].astype(jnp.bfloat16)

    @pl.when(step == last)
    def _():
        for chunk in range(n_chunks):
            if 9 + chunk > 11:
                red.stage(3, chunk)
        for chunk in range(n_chunks):
            red.finish(chunk, shard_ref)


def tail_kernel(units, n_grads, *refs):
    gains_ref = refs[0]
    grad_refs = refs[1:1 + n_grads]
    full_ref, gsum_ref, gbuf, gsend_sem, grecv_sem = refs[1 + n_grads:6 + n_grads]
    ag_sems = refs[6 + n_grads:8 + n_grads]
    red = Reducer(grad_refs, units, refs[8 + n_grads:])
    n_dev = gbuf.shape[0]
    for chunk in range(red.n_chunks):
        red.load(chunk, 1 - red.bit[0])
    sem = pltpu.get_barrier_semaphore()
    for shift in range(1, n_dev):
        pl.semaphore_signal(sem, inc=1, device_id=(lax.rem(red.me + shift, n_dev),), device_id_type=MESH)
    pl.semaphore_wait(sem, n_dev - 1)

    def gain_copy(shift):
        dev = lax.rem(red.me + shift, n_dev)
        return pltpu.make_async_remote_copy(src_ref=gains_ref, dst_ref=gbuf.at[shift], send_sem=gsend_sem.at[shift], recv_sem=grecv_sem.at[shift], device_id=(dev,), device_id_type=MESH)
    for shift in range(1, n_dev):
        gain_copy(shift).start()
    gbuf[0] = gains_ref[...]
    for chunk in range(red.n_chunks):
        red.convert(chunk)
        red.load(chunk, red.bit[0])
    for step in range(1, 4):
        for chunk in range(red.n_chunks):
            red.stage(step, chunk)
    z, y, x, c = (red.bit[b] for b in (3, 2, 1, 0))
    for chunk in range(red.n_chunks):
        for color in range(N_COLOR):
            red.copy(3, chunk, color).wait_recv()
            full_ref[chunk * N_COLOR + color, z, y, x, c] = red.total(chunk, color, red.bit, 4).astype(jnp.bfloat16)
            red.gather_copy(0, chunk, color, full_ref, ag_sems).start()
    for stage in range(1, 4):
        for chunk in range(red.n_chunks):
            for color in range(N_COLOR):
                red.gather_copy(stage - 1, chunk, color, full_ref, ag_sems).wait_recv()
                red.gather_copy(stage, chunk, color, full_ref, ag_sems).start()
    for shift in range(1, n_dev):
        gain_copy(shift).wait()
    acc = jnp.zeros(gains_ref.shape, jnp.float32)
    for dev in range(n_dev):
        acc = acc + gbuf[lax.rem(red.me + n_dev - dev, n_dev)]
    gsum_ref[...] = acc
    for chunk in range(red.n_chunks):
        for color in range(N_COLOR):
            red.gather_copy(3, chunk, color, full_ref, ag_sems).wait_recv()
            for stage in range(4):
                red.gather_copy(stage, chunk, color, full_ref, ag_sems).wait_send()
                red.copy(stage, chunk, color).wait_send()


def attn_specs(seq, n_pairs):
    def col(shift):
        return pl.BlockSpec((seq, LANES), lambda pair, head: (0, pair + shift))
    lse = pl.BlockSpec((1, 8, seq), lambda pair, head: (pair, 0, 0))
    return col, lse


def attn_forward(qkv):
    seq, width = qkv.shape[0], qkv.shape[1] // 3
    n_pairs = width // LANES
    col, lse = attn_specs(seq, n_pairs)
    return pl.pallas_call(
        attn_fwd_kernel,
        grid=(n_pairs, 2),
        in_specs=[col(0), col(n_pairs), col(2 * n_pairs)],
        out_specs=[col(0), lse],
        out_shape=[jax.ShapeDtypeStruct((seq, width), jnp.bfloat16), jax.ShapeDtypeStruct((n_pairs, 8, seq), jnp.float32)],
        scratch_shapes=[pltpu.VMEM((LANES, seq), jnp.bfloat16), pltpu.VMEM((LANES, seq), jnp.float32)],
        compiler_params=pltpu.CompilerParams(dimension_semantics=("arbitrary", "arbitrary"), vmem_limit_bytes=48 * 2 ** 20),
        cost_estimate=pl.CostEstimate(flops=16 * 10 ** 9, bytes_accessed=8 * 2 ** 20, transcendentals=8 * 10 ** 6),
        name="attn_fwd",
    )(qkv, qkv, qkv)


def attn_backward(qkv, d_out, lse_vals, grads, after, call_id):
    seq, width = qkv.shape[0], qkv.shape[1] // 3
    n_pairs = width // LANES
    col, lse = attn_specs(seq, n_pairs)
    shape = jax.ShapeDtypeStruct((seq, width), jnp.bfloat16)
    units = grad_units(grads)
    shard_shape = (len(units), SUB_ROWS, UNIT_COLS)
    out = pl.pallas_call(
        functools.partial(attn_bwd_kernel, units, len(grads), len(after)),
        grid=(n_pairs, 2),
        in_specs=[col(0), col(n_pairs), col(2 * n_pairs), col(0), lse] + [pl.BlockSpec(memory_space=pl.ANY)] * (len(grads) + len(after)),
        out_specs=[col(0), col(0), col(0), pl.BlockSpec(shard_shape, lambda pair, head: (0, 0, 0))],
        out_shape=[shape, shape, shape, jax.ShapeDtypeStruct(shard_shape, jnp.bfloat16)],
        scratch_shapes=[pltpu.VMEM((LANES, seq), jnp.bfloat16), pltpu.VMEM((LANES, seq), jnp.float32), pltpu.VMEM((seq, LANES), jnp.float32), pltpu.VMEM((seq, LANES), jnp.float32)] + reducer_scratch(len(units) // N_COLOR),
        compiler_params=pltpu.CompilerParams(dimension_semantics=("arbitrary", "arbitrary"), vmem_limit_bytes=67043328, collective_id=call_id, has_side_effects=True),
        cost_estimate=pl.CostEstimate(flops=40 * 10 ** 9, bytes_accessed=14 * 2 ** 20, transcendentals=8 * 10 ** 6),
        name="attn_bwd",
    )(qkv, qkv, qkv, d_out, lse_vals, *[grad_view(grad_w) for grad_w in grads], *after)
    return out[:3], out[3]


def tail_reduce(gains, grads, call_id, n_dev):
    units = grad_units(grads)
    full_shape = (len(units), 2, 2, 2, 2, SUB_ROWS, UNIT_COLS)
    n_chunks = len(units) // N_COLOR
    return pl.pallas_call(
        functools.partial(tail_kernel, units, len(grads)),
        in_specs=[pl.BlockSpec(memory_space=pltpu.VMEM)] + [pl.BlockSpec(memory_space=pl.ANY)] * len(grads),
        out_specs=[pl.BlockSpec(memory_space=pltpu.VMEM)] * 2,
        out_shape=[jax.ShapeDtypeStruct(full_shape, jnp.bfloat16), jax.ShapeDtypeStruct(gains.shape, jnp.float32)],
        scratch_shapes=[pltpu.VMEM((n_dev,) + gains.shape, jnp.float32), pltpu.SemaphoreType.DMA((n_dev,)), pltpu.SemaphoreType.DMA((n_dev,)), pltpu.SemaphoreType.DMA((4, n_chunks, N_COLOR)), pltpu.SemaphoreType.DMA((4, n_chunks, N_COLOR))] + reducer_scratch(len(units) // N_COLOR),
        compiler_params=pltpu.CompilerParams(vmem_limit_bytes=40 * 2 ** 20, collective_id=call_id, has_side_effects=True),
        cost_estimate=pl.CostEstimate(flops=20 * 10 ** 9, bytes_accessed=14 * 2 ** 20, transcendentals=0),
        name="tail_reduce",
    )(gains, *[grad_view(grad_w) for grad_w in grads])


def block_forward(x_blk, gain_a, gain_b, w_qkv, w_out, w_up):
    norm_a, norm_a_back = jax.vjp(rms_gain, x_blk.astype(jnp.float32), gain_a)
    u_one = norm_a.astype(jnp.bfloat16)
    qkv = dot_lo(u_one, w_qkv)
    attn_out, lse_vals = attn_forward(qkv)
    hidden = x_blk + dot_lo(attn_out, w_out)
    norm_b, norm_b_back = jax.vjp(rms_gain, hidden.astype(jnp.float32), gain_b)
    u_two = norm_b.astype(jnp.bfloat16)
    pre_lo = dot_lo(u_two, w_up)
    act_f, gelu_back = jax.vjp(gelu_tanh, pre_lo.astype(jnp.float32))
    act_lo = act_f.astype(jnp.bfloat16)
    return hidden, act_lo, (norm_a_back, u_one, qkv, lse_vals, attn_out, norm_b_back, u_two, gelu_back, act_lo)


def block_backward(grad_blk, saved_vals, w_qkv, w_out, w_up, w_down, ready, after, call_id):
    (norm_a_back, u_one, qkv, lse_vals, attn_out, norm_b_back, u_two, gelu_back, act_lo) = saved_vals
    grad_down_w = dot_tn(act_lo, grad_blk)
    grad_act = dot_nt(grad_blk, w_down).astype(jnp.bfloat16)
    (grad_pre_f,) = gelu_back(grad_act.astype(jnp.float32))
    grad_pre = grad_pre_f.astype(jnp.bfloat16)
    grad_up_w = dot_tn(u_two, grad_pre)
    grad_u_two = dot_nt(grad_pre, w_up).astype(jnp.bfloat16)
    grad_h_norm, grad_gain_b = norm_b_back(grad_u_two.astype(jnp.float32))
    grad_hidden = (grad_blk.astype(jnp.float32) + grad_h_norm).astype(jnp.bfloat16)
    grad_out_w = dot_tn(attn_out, grad_hidden)
    grad_attn = dot_nt(grad_hidden, w_out).astype(jnp.bfloat16)
    pieces, shard = attn_backward(qkv, grad_attn, lse_vals, ready + [grad_down_w, grad_up_w, grad_out_w], after, call_id)
    grad_qkv = jnp.concatenate(pieces, axis=1)
    grad_qkv_w = dot_tn(u_one, grad_qkv)
    grad_u_one = dot_nt(grad_qkv, w_qkv).astype(jnp.bfloat16)
    grad_x_norm, grad_gain_a = norm_a_back(grad_u_one.astype(jnp.float32))
    grad_x_blk = (grad_hidden.astype(jnp.float32) + grad_x_norm).astype(jnp.bfloat16)
    return grad_x_blk, grad_gain_a, grad_gain_b, grad_qkv_w, shard


def unit_gather(shard):
    n_units = shard.shape[0]
    flat = lax.all_gather(shard.reshape(n_units * SUB_ROWS, UNIT_COLS), 'data', axis=0, tiled=True)
    return flat.reshape(-1, n_units, SUB_ROWS, UNIT_COLS)


def place(block, out_ref, n_dev):
    n_rows, n_cols = out_ref.shape
    per_row = n_cols // UNIT_COLS
    for unit in range(block.shape[0]):
        row, col = (unit // per_row) * SUB_ROWS, (unit % per_row) * UNIT_COLS
        out_ref[row:row + SUB_ROWS, col:col + UNIT_COLS] = block[unit].astype(jnp.float32) * (1.0 / n_dev)


def unpack_kernel(n_in, layout, n_dev, *refs):
    ins, outs = refs[:n_in], refs[-len(layout):]
    for (pieces, out_ref) in zip(layout, outs):
        for layer, (src, first, count) in enumerate(pieces):
            place(ins[src][0, first:first + count], out_ref.at[layer], n_dev)


def unpack(gathered, layout, shapes, layer, into, n_dev):
    def in_spec(arr):
        return pl.BlockSpec((1,) + arr.shape[1:], lambda dev: (dev, 0, 0, 0))
    out_specs = []
    for pieces, (rows, cols) in zip(layout, shapes):
        if len(pieces) == 1:
            out_specs.append(pl.BlockSpec((1, rows // n_dev, cols), lambda dev: (layer, dev, 0)))
        else:
            out_specs.append(pl.BlockSpec((len(pieces), rows // n_dev, cols), lambda dev: (0, dev, 0)))
    n_in = len(gathered)
    return pl.pallas_call(
        functools.partial(unpack_kernel, n_in, layout, n_dev),
        grid=(n_dev,),
        in_specs=[in_spec(arr) for arr in gathered] + [pl.BlockSpec(memory_space=pl.ANY)] * len(into),
        out_specs=out_specs,
        out_shape=[jax.ShapeDtypeStruct((2, rows, cols), jnp.float32) for rows, cols in shapes],
        input_output_aliases={n_in + i: i for i in range(len(into))},
        compiler_params=pltpu.CompilerParams(dimension_semantics=("arbitrary",), vmem_limit_bytes=48 * 2 ** 20),
        cost_estimate=pl.CostEstimate(flops=10 ** 10, bytes_accessed=40 * 2 ** 20, transcendentals=0),
        name="unpack",
    )(*gathered, *into)


def unpack_qkv_kernel(n_dev, low_qkv_ref, full_ref, out_ref):
    place(full_ref[:, 0], out_ref.at[0], n_dev)
    place(low_qkv_ref[0], out_ref.at[1], n_dev)


def unpack_qkv(full, low, shape, n_dev):
    rows, cols = shape
    return pl.pallas_call(
        functools.partial(unpack_qkv_kernel, n_dev),
        grid=(n_dev,),
        in_specs=[pl.BlockSpec((1, 3, SUB_ROWS, UNIT_COLS), lambda dev: (dev, 0, 0, 0)), pl.BlockSpec((3, 1, SUB_ROWS, UNIT_COLS), lambda dev: (0, dev, 0, 0))],
        out_specs=pl.BlockSpec((2, rows // n_dev, cols), lambda dev: (0, dev, 0)),
        out_shape=jax.ShapeDtypeStruct((2, rows, cols), jnp.float32),
        compiler_params=pltpu.CompilerParams(dimension_semantics=("arbitrary",), vmem_limit_bytes=32 * 2 ** 20),
        cost_estimate=pl.CostEstimate(flops=4 * 10 ** 9, bytes_accessed=20 * 2 ** 20, transcendentals=0),
        name="unpack_qkv",
    )(low, full)


def solution(mesh):
    n_dev = mesh.shape['data']

    def local_step(x_loc, grad_y_loc, gain_one, gain_two, w_qkv, w_out, w_up, w_down):
        n_layers = w_qkv.shape[0]
        hidden_x = x_loc[0]
        saved_all = []
        for layer_idx in range(n_layers):
            hidden, act_lo, saved_vals = block_forward(hidden_x, gain_one[layer_idx], gain_two[layer_idx], w_qkv[layer_idx], w_out[layer_idx], w_up[layer_idx])
            saved_all.append(saved_vals)
            if layer_idx + 1 < n_layers:
                hidden_x = hidden + dot_lo(act_lo, w_down[layer_idx])
        grad_cur = grad_y_loc[0]
        gains = [None] * (2 * n_layers)
        ready, after, gathered = [], [], []
        for layer_idx in reversed(range(n_layers)):
            out = block_backward(grad_cur, saved_all[layer_idx], w_qkv[layer_idx], w_out[layer_idx], w_up[layer_idx], w_down[layer_idx], ready, after, n_layers - 1 - layer_idx)
            grad_cur, gains[layer_idx], gains[n_layers + layer_idx], grad_qkv_w, shard = out
            ready = [grad_qkv_w]
            gathered.append(unit_gather(shard))
            after = [gathered[-1]]
        gain_rows = jnp.concatenate([jnp.stack(gains), jnp.zeros((8 - 2 * n_layers, gains[0].shape[0]), jnp.float32)])
        full, gain_sums = tail_reduce(gain_rows, ready, n_layers, n_dev)
        gain_sums = gain_sums / n_dev
        full = full.reshape(3, n_dev, SUB_ROWS, UNIT_COLS)
        shapes = [(w_down.shape[1], w_down.shape[2]), (w_up.shape[1], w_up.shape[2]), (w_out.shape[1], w_out.shape[2])]
        top, low = gathered
        partial = unpack([top], [((0, 0, 4),), ((0, 4, 4),), ((0, 8, 1),)], shapes, 1, [], n_dev)
        w_d, w_u, w_o = unpack([low], [((0, 3, 4),), ((0, 7, 4),), ((0, 11, 1),)], shapes, 0, partial, n_dev)
        grad_qkv = unpack_qkv(full, low, w_qkv.shape[1:], n_dev)
        weights = (grad_qkv, w_o, w_u, w_d)
        return (grad_cur[None], gain_sums[:n_layers], gain_sums[n_layers:2 * n_layers]) + weights

    batch_spec = P('data')
    full_spec = P()
    return jax.shard_map(local_step, mesh=mesh, in_specs=(batch_spec, batch_spec) + (full_spec,) * 6, out_specs=(batch_spec,) + (full_spec,) * 6, check_vma=False)
```

```python
import functools

import jax
import jax.numpy as jnp
from jax import lax
from jax.experimental import pallas as pl
from jax.experimental.pallas import tpu as pltpu
from jax.sharding import PartitionSpec as P

NORM_EPS = 1e-6
HEAD_DIM = 64
LANES = 128
Q_BLK = 256
EXP_SCALE = HEAD_DIM ** -0.5 * 1.4426950408889634
NEG = -1e30
MIB = 2 ** 20
VMEM_ALL = 67043328
MESH = pl.DeviceIdType.MESH


def cost(gflops, mbytes):
    return pl.CostEstimate(flops=gflops * 10 ** 9, bytes_accessed=mbytes * MIB, transcendentals=0)


def rms_gain(rows_f, gain_vec):
    return rows_f * lax.rsqrt(jnp.mean(rows_f * rows_f, axis=-1, keepdims=True) + NORM_EPS) * gain_vec


def gelu_tanh(pre_act):
    return jax.nn.gelu(pre_act, approximate=True)


def dot_lo(lhs, rhs):
    return jnp.dot(lhs, rhs, preferred_element_type=jnp.float32).astype(jnp.bfloat16)


def dot_nt(lhs, rhs):
    return lax.dot_general(lhs, rhs, (((1,), (1,)), ((), ())), preferred_element_type=jnp.float32)


def dot_tn(lhs, rhs):
    return lax.dot_general(lhs, rhs, (((0,), (0,)), ((), ())), preferred_element_type=jnp.float32)


def dot_nn(lhs, rhs):
    return jnp.dot(lhs, rhs, preferred_element_type=jnp.float32)


def head_mask(ref_rows, head):
    lane = lax.broadcasted_iota(jnp.int32, ref_rows.shape, 1)
    return jnp.where(lane // HEAD_DIM == head, ref_rows, jnp.zeros_like(ref_rows))


def scores_t(k_ref, q_m, q_start):
    diag = dot_nt(k_ref[q_start:q_start + Q_BLK, :], q_m)
    key_i = lax.broadcasted_iota(jnp.int32, diag.shape, 0)
    query_i = lax.broadcasted_iota(jnp.int32, diag.shape, 1)
    diag = jnp.where(key_i <= query_i, diag, NEG)
    if q_start == 0:
        return diag
    return jnp.concatenate([dot_nt(k_ref[:q_start, :], q_m), diag], axis=0)


def attn_fwd_kernel(q_ref, k_ref, v_ref, o_ref, lse_ref, vt_ref, ot_ref):
    seq = q_ref.shape[0]
    vt_ref[...] = v_ref[...].T
    for head in range(LANES // HEAD_DIM):
        rows = slice(head * HEAD_DIM, (head + 1) * HEAD_DIM)
        for q_start in range(0, seq, Q_BLK):
            q_end = q_start + Q_BLK
            q_m = head_mask(q_ref[q_start:q_end, :], head)
            s_t = scores_t(k_ref, q_m, q_start)
            top = jnp.max(s_t, axis=0, keepdims=True)
            p_t = jnp.exp2((s_t - top) * EXP_SCALE)
            total = jnp.sum(p_t, axis=0, keepdims=True)
            p_lo = (p_t * (1.0 / total)).astype(jnp.bfloat16)
            ot_ref[rows, q_start:q_end] = dot_nn(vt_ref[rows, :q_end], p_lo)
            lse_ref[0, head:head + 1, q_start:q_end] = top * EXP_SCALE + jnp.log2(total)
    o_ref[...] = ot_ref[...].T.astype(jnp.bfloat16)


N_COLOR = 3
UNIT_COLS = 256
FF_BLK = 256
MLP_ROWS = 96
ATTN_ROWS = 144
MLP_CHUNKS = 3
GELU_C = 0.7978845608028654
AXIS_BITS = (3, 2, 1)


class Reducer:
    def __init__(self, n_chunks, refs, grad_refs=(), parts=()):
        (self.own, self.send0, self.recv0, self.send1, self.recv1, self.send2, self.recv2, self.send3, self.recv3, self.load_sem, self.send_sem, self.recv_sem) = refs
        self.grad_refs, self.parts = grad_refs, parts
        self.n_chunks = n_chunks
        me = lax.axis_index('data')
        self.me = me
        self.bit = [lax.rem(lax.div(me, 1 << b), 2) for b in range(4)]
        self.partner = [me + (1 - 2 * self.bit[b]) * (1 << b) for b in range(4)]

    def barrier(self):
        sem = pltpu.get_barrier_semaphore()
        for dev in self.partner:
            pl.semaphore_signal(sem, inc=1, device_id=(dev,), device_id_type=MESH)
        pl.semaphore_wait(sem, 4)

    def load(self, chunk, half):
        for color in range(N_COLOR):
            for part, (array, kind, col, row, n_rows) in enumerate(self.parts[chunk][color]):
                if kind == 'block':
                    src = self.grad_refs[array].at[col, :, half]
                else:
                    src = self.grad_refs[array].at[:, half, :, pl.ds(col, UNIT_COLS)]
                dst = self.own.at[chunk, color, :, pl.ds(row, n_rows)]
                pltpu.make_async_copy(src, dst, self.load_sem.at[chunk, color, part]).start()

    def wait_load(self, chunk):
        for color in range(N_COLOR):
            for part, (_, _, _, row, n_rows) in enumerate(self.parts[chunk][color]):
                ref = self.own.at[chunk, color, :, pl.ds(row, n_rows)]
                pltpu.make_async_copy(ref, ref, self.load_sem.at[chunk, color, part]).wait()

    def copy(self, stage, chunk, color):
        send = (self.send0, self.send1, self.send2, self.send3)[stage].at[chunk, color]
        recv = (self.recv0, self.recv1, self.recv2, self.recv3)[stage].at[chunk, color]
        dev = self.partner[0] if stage == 0 else self.partner[self.order(color)[stage - 1]]
        return pltpu.make_async_remote_copy(src_ref=send, dst_ref=recv, send_sem=self.send_sem.at[stage, chunk, color], recv_sem=self.recv_sem.at[stage, chunk, color], device_id=(dev,), device_id_type=MESH)

    def order(self, color):
        return [1 + (color + step) % N_COLOR for step in range(N_COLOR)]

    def block(self, values):
        return values[3] * 4 + values[2] * 2 + values[1]

    def convert(self, chunk):
        self.wait_load(chunk)
        for color in range(N_COLOR):
            def body(i, carry):
                self.send0[chunk, color, i] = self.own[chunk, color, i].astype(jnp.bfloat16)
                return carry
            lax.fori_loop(0, 8, body, 0)
            self.copy(0, chunk, color).start()

    def total(self, chunk, color, values, n_recv):
        order = self.order(color)
        index = self.block(values)
        acc = self.own[chunk, color, index] + self.recv0[chunk, color, index].astype(jnp.float32)
        if n_recv >= 2:
            acc = acc + self.recv1[chunk, color, values[order[1]] * 2 + values[order[2]]].astype(jnp.float32)
        if n_recv >= 3:
            acc = acc + self.recv2[chunk, color, values[order[2]]].astype(jnp.float32)
        if n_recv >= 4:
            acc = acc + self.recv3[chunk, color, 0].astype(jnp.float32)
        return acc

    def stage(self, step, chunk):
        send = (None, self.send1, self.send2, self.send3)[step]
        n_free = N_COLOR - step
        for color in range(N_COLOR):
            self.copy(step - 1, chunk, color).wait_recv()
            order = self.order(color)

            def body(i, carry):
                values = [0, 0, 0, 0]
                for done in range(step - 1):
                    values[order[done]] = self.bit[order[done]]
                values[order[step - 1]] = 1 - self.bit[order[step - 1]]
                if n_free == 2:
                    values[order[1]], values[order[2]] = lax.div(i, 2), lax.rem(i, 2)
                elif n_free == 1:
                    values[order[2]] = i
                send[chunk, color, i] = self.total(chunk, color, values, step).astype(jnp.bfloat16)
                return carry
            if n_free:
                lax.fori_loop(0, 1 << n_free, body, 0)
            else:
                body(0, 0)
            self.copy(step, chunk, color).start()

    def finish(self, chunk, out_ref):
        for color in range(N_COLOR):
            self.copy(3, chunk, color).wait_recv()
            out_ref[chunk * N_COLOR + color] = self.total(chunk, color, self.bit, 4).astype(jnp.bfloat16)
        for stage in range(4):
            for color in range(N_COLOR):
                self.copy(stage, chunk, color).wait_send()


def reducer_scratch(n_chunks, rows):
    def buf(blocks, dtype):
        return pltpu.VMEM((n_chunks, N_COLOR, blocks, rows, UNIT_COLS), dtype)
    lo = jnp.bfloat16
    return [buf(8, jnp.float32), buf(8, lo), buf(8, lo), buf(4, lo), buf(4, lo), buf(2, lo), buf(2, lo), buf(1, lo), buf(1, lo), pltpu.SemaphoreType.DMA((n_chunks, N_COLOR, N_COLOR)), pltpu.SemaphoreType.DMA((4, n_chunks, N_COLOR)), pltpu.SemaphoreType.DMA((4, n_chunks, N_COLOR))]


def grad_view(grad_w):
    rows, cols = grad_w.shape
    return grad_w.reshape(8, 2, rows // 16, cols)


def qkv_parts(array):
    return [[(array, 'cols', (color * 3 + part) * UNIT_COLS, part * 48, 48) for part in range(3)] for color in range(N_COLOR)]


def rest_parts(block_array, out_array):
    return [[(block_array, 'block', color, 0, MLP_ROWS), (out_array, 'cols', color * UNIT_COLS, MLP_ROWS, 48)] for color in range(N_COLOR)]


def mlp_bwd_kernel(n_after, *refs):
    dy_ref, u_ref, z_ref, w1_ref, w2_ref = refs[:5]
    du_ref, block_ref, shard_ref, ut_ref, a_ref, dz_ref = refs[5 + n_after:11 + n_after]
    red = Reducer(MLP_CHUNKS, refs[11 + n_after:])
    step = pl.program_id(0)
    n_blk = dz_ref.shape[1] // FF_BLK
    core = red.bit[0]
    seq = dy_ref.shape[0]

    @pl.when(step == 0)
    def _():
        red.barrier()
        ut_ref[...] = u_ref[...].T

    for stage, first, count in ((1, 4, MLP_CHUNKS), (2, 7, MLP_CHUNKS), (3, 9, MLP_CHUNKS - 1)):
        @pl.when((step >= first) & (step < first + N_COLOR * count) & (lax.rem(step + 2 * first, N_COLOR) == 0))
        def _():
            red.stage(stage, lax.div(step - first, N_COLOR))

    @pl.when(step < n_blk)
    def _():
        cols = pl.ds(pl.multiple_of(step * FF_BLK, FF_BLK), FF_BLK)
        for row in range(0, seq, 256):
            rows = slice(row, row + 256)
            da = dot_nt(dy_ref[rows, :], w2_ref[0]).astype(jnp.bfloat16).astype(jnp.float32)
            z = z_ref[rows, :].astype(jnp.float32)
            z_sq = z * z
            th = jnp.tanh(z * (GELU_C + (GELU_C * 0.044715) * z_sq))
            cdf = 0.5 + 0.5 * th
            a_ref[rows, :] = (z * cdf).astype(jnp.bfloat16)
            slope = cdf + (0.5 * z) * (1.0 - th * th) * (GELU_C + (3.0 * GELU_C * 0.044715) * z_sq)
            dz_ref[rows, cols] = (slope * da).astype(jnp.bfloat16)
        dw1 = dot_nn(ut_ref[...], dz_ref[:, cols])
        block_ref[0, :, :, 0:48, :] = dw1.reshape(8, 2, 48, UNIT_COLS)
        dw2 = dot_nn(a_ref[...].T, dy_ref[...])
        for part in range(3):
            block_ref[0, :, :, 48 + 16 * part:64 + 16 * part, :] = dw2[:, part * UNIT_COLS:(part + 1) * UNIT_COLS].reshape(8, 2, 16, UNIT_COLS)

    @pl.when(step < N_COLOR * MLP_CHUNKS)
    def _():
        chunk, color = lax.div(step, N_COLOR), lax.rem(step, N_COLOR)

        def body(i, carry):
            red.own[chunk, color, i] = block_ref[0, i, core]
            red.send0[chunk, color, i] = block_ref[0, i, 1 - core].astype(jnp.bfloat16)
            return carry
        lax.fori_loop(0, 8, body, 0)
        red.copy(0, chunk, color).start()

    @pl.when(step >= n_blk)
    def _():
        du_ref[...] = dot_nt(dz_ref[...], w1_ref[0]).astype(jnp.bfloat16)

    @pl.when(step == pl.num_programs(0) - 1)
    def _():
        red.stage(3, MLP_CHUNKS - 1)
        for chunk in range(MLP_CHUNKS):
            red.finish(chunk, shard_ref)


def mlp_backward(dy, u_two, z_lo, w_up, w_down, layer, after, call_id):
    seq, width = dy.shape
    n_blk = w_up.shape[2] // FF_BLK
    n_last = width // 256
    last = n_blk - N_COLOR
    whole = pl.BlockSpec((seq, width), lambda step: (0, 0))
    shard_shape = (N_COLOR * MLP_CHUNKS, MLP_ROWS, UNIT_COLS)
    return pl.pallas_call(
        functools.partial(mlp_bwd_kernel, len(after)),
        grid=(n_blk + n_last,),
        in_specs=[
            whole, whole,
            pl.BlockSpec((seq, FF_BLK), lambda step: (0, jnp.minimum(step, n_blk - 1))),
            pl.BlockSpec((1, 256, w_up.shape[2]), lambda step: (layer, jnp.maximum(step - n_blk, 0), 0)),
            pl.BlockSpec((1, FF_BLK, width), lambda step: (layer, jnp.minimum(step, n_blk - 1), 0)),
        ] + [pl.BlockSpec(memory_space=pl.ANY)] * len(after),
        out_specs=[
            pl.BlockSpec((seq, 256), lambda step: (0, jnp.maximum(step - n_blk, 0))),
            pl.BlockSpec((1, 8, 2, MLP_ROWS, UNIT_COLS), lambda step: (jnp.clip(step - last, 0, N_COLOR - 1), 0, 0, 0, 0)),
            pl.BlockSpec(shard_shape, lambda step: (0, 0, 0)),
        ],
        out_shape=[jax.ShapeDtypeStruct((seq, width), jnp.bfloat16), jax.ShapeDtypeStruct((N_COLOR, 8, 2, MLP_ROWS, UNIT_COLS), jnp.float32), jax.ShapeDtypeStruct(shard_shape, jnp.bfloat16)],
        scratch_shapes=[pltpu.VMEM((width, seq), jnp.bfloat16), pltpu.VMEM((seq, FF_BLK), jnp.bfloat16), pltpu.VMEM((seq, w_up.shape[2]), jnp.bfloat16)] + reducer_scratch(MLP_CHUNKS, MLP_ROWS),
        compiler_params=pltpu.CompilerParams(dimension_semantics=("arbitrary",), vmem_limit_bytes=VMEM_ALL, collective_id=call_id),
        cost_estimate=cost(30, 30),
        name="mlp_bwd",
    )(dy, u_two, z_lo, w_up, w_down, *after)


def attn_bwd_kernel(parts, n_grads, n_after, *refs):
    q_ref, k_ref, v_ref, do_ref, lse_ref = refs[:5]
    grad_refs = refs[5:5 + n_grads]
    refs = refs[:5 + n_grads] + refs[5 + n_grads + n_after:]
    dq_ref, dk_ref, dv_ref, shard_ref, kt_ref, dqt_ref, dk_acc, dv_acc = refs[5 + n_grads:13 + n_grads]
    red = Reducer(len(parts), refs[13 + n_grads:], grad_refs, parts)
    n_chunks = red.n_chunks
    pair = pl.program_id(0)
    seq = q_ref.shape[0]
    events = {}
    for chunk in range(n_chunks):
        events.setdefault(1 + chunk, []).append((1, chunk))
        events.setdefault(4 + 2 * chunk, []).append((2, chunk))
        events.setdefault(7 + 2 * chunk, []).append((3, chunk))

    @pl.when(pair == 0)
    def _():
        red.barrier()
        for chunk in range(n_chunks):
            red.load(chunk, 1 - red.bit[0])
        for chunk in range(n_chunks):
            red.convert(chunk)
            red.load(chunk, red.bit[0])

    kt_ref[...] = k_ref[...].T
    for head in range(LANES // HEAD_DIM):
        for when, todo in events.items():
            if when % 2 == head:
                @pl.when(pair == when // 2)
                def _():
                    for stage, chunk in todo:
                        if stage == 1:
                            red.wait_load(chunk)
                        red.stage(stage, chunk)
        rows = slice(head * HEAD_DIM, (head + 1) * HEAD_DIM)
        for q_start in range(0, seq, Q_BLK):
            q_end = q_start + Q_BLK
            q_m = head_mask(q_ref[q_start:q_end, :], head)
            do_m = head_mask(do_ref[q_start:q_end, :], head)
            s_t = scores_t(k_ref, q_m, q_start)
            p_t = jnp.exp2(s_t * EXP_SCALE - lse_ref[0, head:head + 1, q_start:q_end])
            dp_t = dot_nt(v_ref[:q_end, :], do_m)
            delta = jnp.sum(p_t * dp_t, axis=0, keepdims=True)
            ds_t = (p_t * (dp_t - delta) * HEAD_DIM ** -0.5).astype(jnp.bfloat16)
            dv_part = dot_nn(p_t.astype(jnp.bfloat16), do_m)
            dk_part = dot_nn(ds_t, q_m)
            if head == 0 and q_start == 0:
                dv_acc[...] = jnp.zeros_like(dv_acc)
                dk_acc[...] = jnp.zeros_like(dk_acc)
            dv_acc[:q_end, :] += dv_part
            dk_acc[:q_end, :] += dk_part
            dqt_ref[rows, q_start:q_end] = dot_nn(kt_ref[rows, :q_end], ds_t)
    dq_ref[...] = dqt_ref[...].T.astype(jnp.bfloat16)
    dk_ref[...] = dk_acc[...].astype(jnp.bfloat16)
    dv_ref[...] = dv_acc[...].astype(jnp.bfloat16)

    @pl.when(pair == pl.num_programs(0) - 1)
    def _():
        for chunk in range(n_chunks):
            red.finish(chunk, shard_ref)


def tail_kernel(parts, n_grads, n_after, *refs):
    gains_ref = refs[0]
    grad_refs = refs[1:1 + n_grads]
    refs = refs[:1 + n_grads] + refs[1 + n_grads + n_after:]
    shard_ref, gsum_ref, gbuf, gsend_sem, grecv_sem = refs[1 + n_grads:6 + n_grads]
    red = Reducer(len(parts), refs[6 + n_grads:], grad_refs, parts)
    n_dev = gbuf.shape[0]
    for chunk in range(red.n_chunks):
        red.load(chunk, 1 - red.bit[0])
    sem = pltpu.get_barrier_semaphore()
    for shift in range(1, n_dev):
        pl.semaphore_signal(sem, inc=1, device_id=(lax.rem(red.me + shift, n_dev),), device_id_type=MESH)
    pl.semaphore_wait(sem, n_dev - 1)

    def gain_copy(shift):
        dev = lax.rem(red.me + shift, n_dev)
        return pltpu.make_async_remote_copy(src_ref=gains_ref, dst_ref=gbuf.at[shift], send_sem=gsend_sem.at[shift], recv_sem=grecv_sem.at[shift], device_id=(dev,), device_id_type=MESH)
    for shift in range(1, n_dev):
        gain_copy(shift).start()
    gbuf[0] = gains_ref[...]
    for chunk in range(red.n_chunks):
        red.convert(chunk)
        red.load(chunk, red.bit[0])
    for step in range(1, 4):
        for chunk in range(red.n_chunks):
            if step == 1:
                red.wait_load(chunk)
            red.stage(step, chunk)
    for shift in range(1, n_dev):
        gain_copy(shift).wait()
    acc = jnp.zeros(gains_ref.shape, jnp.float32)
    for dev in range(n_dev):
        acc = acc + gbuf[lax.rem(red.me + n_dev - dev, n_dev)]
    gsum_ref[...] = acc
    for chunk in range(red.n_chunks):
        red.finish(chunk, shard_ref)


def attn_specs(seq, n_pairs):
    def col(shift):
        return pl.BlockSpec((seq, LANES), lambda pair: (0, pair + shift))
    lse = pl.BlockSpec((1, 8, seq), lambda pair: (pair, 0, 0))
    return col, lse


def attn_forward(qkv):
    seq, width = qkv.shape[0], qkv.shape[1] // 3
    n_pairs = width // LANES
    col, lse = attn_specs(seq, n_pairs)
    return pl.pallas_call(
        attn_fwd_kernel,
        grid=(n_pairs,),
        in_specs=[col(0), col(n_pairs), col(2 * n_pairs)],
        out_specs=[col(0), lse],
        out_shape=[jax.ShapeDtypeStruct((seq, width), jnp.bfloat16), jax.ShapeDtypeStruct((n_pairs, 8, seq), jnp.float32)],
        scratch_shapes=[pltpu.VMEM((LANES, seq), jnp.bfloat16), pltpu.VMEM((LANES, seq), jnp.float32)],
        compiler_params=pltpu.CompilerParams(dimension_semantics=("arbitrary",), vmem_limit_bytes=48 * MIB),
        cost_estimate=cost(16, 8),
        name="attn_fwd",
    )(qkv, qkv, qkv)


def attn_backward(qkv, d_out, lse_vals, grads, parts, after, call_id):
    seq, width = qkv.shape[0], qkv.shape[1] // 3
    n_pairs = width // LANES
    col, lse = attn_specs(seq, n_pairs)
    shape = jax.ShapeDtypeStruct((seq, width), jnp.bfloat16)
    shard_shape = (len(parts) * N_COLOR, ATTN_ROWS, UNIT_COLS)
    out = pl.pallas_call(
        functools.partial(attn_bwd_kernel, parts, len(grads), len(after)),
        grid=(n_pairs,),
        in_specs=[col(0), col(n_pairs), col(2 * n_pairs), col(0), lse] + [pl.BlockSpec(memory_space=pl.ANY)] * (len(grads) + len(after)),
        out_specs=[col(0), col(0), col(0), pl.BlockSpec(shard_shape, lambda pair: (0, 0, 0))],
        out_shape=[shape, shape, shape, jax.ShapeDtypeStruct(shard_shape, jnp.bfloat16)],
        scratch_shapes=[pltpu.VMEM((LANES, seq), jnp.bfloat16), pltpu.VMEM((LANES, seq), jnp.float32), pltpu.VMEM((seq, LANES), jnp.float32), pltpu.VMEM((seq, LANES), jnp.float32)] + reducer_scratch(len(parts), ATTN_ROWS),
        compiler_params=pltpu.CompilerParams(dimension_semantics=("arbitrary",), vmem_limit_bytes=60 * MIB, collective_id=call_id),
        cost_estimate=cost(40, 14),
        name="attn_bwd",
    )(qkv, qkv, qkv, d_out, lse_vals, *grads, *after)
    return out[:3], out[3]


def tail_reduce(gains, grads, parts, after, call_id, n_dev):
    n_chunks = len(parts)
    shard_shape = (n_chunks * N_COLOR, ATTN_ROWS, UNIT_COLS)
    return pl.pallas_call(
        functools.partial(tail_kernel, parts, len(grads), len(after)),
        in_specs=[pl.BlockSpec(memory_space=pltpu.VMEM)] + [pl.BlockSpec(memory_space=pl.ANY)] * (len(grads) + len(after)),
        out_specs=[pl.BlockSpec(memory_space=pltpu.VMEM)] * 2,
        out_shape=[jax.ShapeDtypeStruct(shard_shape, jnp.bfloat16), jax.ShapeDtypeStruct(gains.shape, jnp.float32)],
        scratch_shapes=[pltpu.VMEM((n_dev,) + gains.shape, jnp.float32), pltpu.SemaphoreType.DMA((n_dev,)), pltpu.SemaphoreType.DMA((n_dev,))] + reducer_scratch(n_chunks, ATTN_ROWS),
        compiler_params=pltpu.CompilerParams(vmem_limit_bytes=40 * MIB, collective_id=call_id),
        cost_estimate=cost(20, 14),
        name="tail_reduce",
    )(gains, *grads, *after)


def block_forward(x_blk, gain_a, gain_b, w_qkv, w_out, w_up):
    norm_a, norm_a_back = jax.vjp(rms_gain, x_blk.astype(jnp.float32), gain_a)
    u_one = norm_a.astype(jnp.bfloat16)
    qkv = dot_lo(u_one, w_qkv)
    attn_out, lse_vals = attn_forward(qkv)
    hidden = x_blk + dot_lo(attn_out, w_out)
    norm_b, norm_b_back = jax.vjp(rms_gain, hidden.astype(jnp.float32), gain_b)
    u_two = norm_b.astype(jnp.bfloat16)
    pre_lo = dot_lo(u_two, w_up)
    act_lo = gelu_tanh(pre_lo.astype(jnp.float32)).astype(jnp.bfloat16)
    return hidden, act_lo, (norm_a_back, u_one, qkv, lse_vals, attn_out, norm_b_back, u_two, pre_lo)


def block_backward(grad_blk, saved_vals, w_qkv, w_out, w_up, w_down, layer, ready, after):
    (norm_a_back, u_one, qkv, lse_vals, attn_out, norm_b_back, u_two, pre_lo) = saved_vals
    ids = 2 * len(ready)
    grad_u_two, block, shard_mlp = mlp_backward(grad_blk, u_two, pre_lo, w_up, w_down, layer, after[:1], ids)
    grad_h_norm, grad_gain_b = norm_b_back(grad_u_two.astype(jnp.float32))
    grad_hidden = (grad_blk.astype(jnp.float32) + grad_h_norm).astype(jnp.bfloat16)
    grad_out_w = dot_tn(attn_out, grad_hidden)
    grad_attn = dot_nt(grad_hidden, w_out).astype(jnp.bfloat16)
    grads = [grad_view(grad_w) for grad_w in ready] + [block, grad_view(grad_out_w)]
    parts = [qkv_parts(0)] * len(ready) + [rest_parts(len(ready), len(ready) + 1)]
    pieces, shard_attn = attn_backward(qkv, grad_attn, lse_vals, grads, parts, after[1:], ids + 1)
    grad_qkv = jnp.concatenate(pieces, axis=1)
    grad_qkv_w = dot_tn(u_one, grad_qkv)
    grad_u_one = dot_nt(grad_qkv, w_qkv).astype(jnp.bfloat16)
    grad_x_norm, grad_gain_a = norm_a_back(grad_u_one.astype(jnp.float32))
    grad_x_blk = (grad_hidden.astype(jnp.float32) + grad_x_norm).astype(jnp.bfloat16)
    return grad_x_blk, grad_gain_a, grad_gain_b, grad_qkv_w, unit_gather(shard_mlp), unit_gather(shard_attn)


def unit_gather(shard):
    n_units, rows, cols = shard.shape
    flat = lax.all_gather(shard.reshape(n_units * rows, cols), 'data', axis=0, tiled=True)
    return flat.reshape(-1, n_units, rows, cols)


def put_qkv(unit_ref, out_ref, scale):
    for color in range(N_COLOR):
        for part in range(3):
            cols = slice((color * 3 + part) * UNIT_COLS, (color * 3 + part + 1) * UNIT_COLS)
            out_ref[0, :, cols] = unit_ref[0, color, part * 48:part * 48 + 48].astype(jnp.float32) * scale


def unpack_kernel(first, n_dev, n_out, *refs):
    mlp_ref, attn_ref = refs[:2]
    up_ref, down_ref, out_ref = refs[-n_out:][:3]
    scale = 1.0 / n_dev

    def value(unit):
        return unit.astype(jnp.float32) * scale
    n_mlp = mlp_ref.shape[1]
    for blk in range(n_mlp + N_COLOR):
        unit = mlp_ref[0, blk] if blk < n_mlp else attn_ref[0, first + blk - n_mlp, 0:MLP_ROWS]
        up_ref[0, :, blk * FF_BLK:(blk + 1) * FF_BLK] = value(unit[0:48])
        for part in range(3):
            down_ref[0, blk, 0, :, part * UNIT_COLS:(part + 1) * UNIT_COLS] = value(unit[48 + 16 * part:64 + 16 * part])
    for color in range(N_COLOR):
        out_ref[0, :, color * UNIT_COLS:(color + 1) * UNIT_COLS] = value(attn_ref[0, first + color, MLP_ROWS:ATTN_ROWS])
    if first:
        put_qkv(attn_ref, refs[-1], scale)


def unpack(mlp_all, attn_all, first, layer, width, hidden, into, after):
    n_dev = mlp_all.shape[0]
    def in_spec(arr):
        return pl.BlockSpec((1,) + arr.shape[1:], lambda dev: (dev, 0, 0, 0))
    def rows(shape, at):
        return pl.BlockSpec((1, width // n_dev, shape[2]), lambda dev: (at, dev, 0))
    n_blk = hidden // FF_BLK
    shapes = [(2, width, hidden), (2, n_blk, n_dev, FF_BLK // n_dev, width), (2, width, width)]
    down = pl.BlockSpec((1, n_blk, 1, FF_BLK // n_dev, width), lambda dev: (layer, 0, dev, 0, 0))
    out_specs = [rows(shapes[0], layer), down, rows(shapes[2], layer)]
    if first:
        shapes.append((2, width, 3 * width))
        out_specs.append(rows(shapes[3], layer + 1))
    return pl.pallas_call(
        functools.partial(unpack_kernel, first, n_dev, len(shapes)),
        grid=(n_dev,),
        in_specs=[in_spec(mlp_all), in_spec(attn_all)] + [pl.BlockSpec(memory_space=pl.ANY)] * (len(into) + len(after)),
        out_specs=out_specs,
        out_shape=[jax.ShapeDtypeStruct(shape, jnp.float32) for shape in shapes],
        input_output_aliases={2 + i: i for i in range(len(into))},
        compiler_params=pltpu.CompilerParams(dimension_semantics=("arbitrary",), vmem_limit_bytes=48 * MIB),
        cost_estimate=cost(10, 40),
        name="unpack",
    )(mlp_all, attn_all, *into, *after)


def unpack_qkv_kernel(n_dev, last_ref, into_ref, out_ref):
    put_qkv(last_ref, out_ref, 1.0 / n_dev)


def unpack_qkv(last_all, into):
    n_dev = last_all.shape[0]
    rows, cols = into.shape[1:]
    return pl.pallas_call(
        functools.partial(unpack_qkv_kernel, n_dev),
        grid=(n_dev,),
        in_specs=[pl.BlockSpec((1,) + last_all.shape[1:], lambda dev: (dev, 0, 0, 0)), pl.BlockSpec(memory_space=pl.ANY)],
        out_specs=pl.BlockSpec((1, rows // n_dev, cols), lambda dev: (0, dev, 0)),
        out_shape=jax.ShapeDtypeStruct(into.shape, jnp.float32),
        input_output_aliases={1: 0},
        compiler_params=pltpu.CompilerParams(dimension_semantics=("arbitrary",), vmem_limit_bytes=32 * MIB),
        cost_estimate=cost(4, 20),
        name="unpack_qkv",
    )(last_all, into)


def solution(mesh):
    n_dev = mesh.shape['data']

    def local_step(x_loc, grad_y_loc, gain_one, gain_two, w_qkv, w_out, w_up, w_down):
        n_layers = w_qkv.shape[0]
        hidden_x = x_loc[0]
        saved_all = []
        for layer_idx in range(n_layers):
            hidden, act_lo, saved_vals = block_forward(hidden_x, gain_one[layer_idx], gain_two[layer_idx], w_qkv[layer_idx], w_out[layer_idx], w_up[layer_idx])
            saved_all.append(saved_vals)
            if layer_idx + 1 < n_layers:
                hidden_x = hidden + dot_lo(act_lo, w_down[layer_idx])
        grad_cur = grad_y_loc[0]
        width, hidden = w_up.shape[1:]
        gains = [None] * (2 * n_layers)
        ready, after, gathered = [], [], []
        for layer_idx in reversed(range(n_layers)):
            out = block_backward(grad_cur, saved_all[layer_idx], w_qkv[layer_idx], w_out[layer_idx], w_up, w_down, layer_idx, ready, after)
            grad_cur, gains[layer_idx], gains[n_layers + layer_idx], grad_qkv_w = out[:4]
            ready, after = [grad_qkv_w], list(out[4:])
            gathered.append(after)
        (top_mlp, top_attn), (low_mlp, low_attn) = gathered
        gain_rows = jnp.concatenate([jnp.stack(gains), jnp.zeros((8 - 2 * n_layers, width), jnp.float32)])
        shard, gain_sums = tail_reduce(gain_rows, [grad_view(ready[0])], [qkv_parts(0)], [low_mlp], 2 * n_layers, n_dev)
        last = unit_gather(shard)
        partial = unpack(top_mlp, top_attn, 0, 1, width, hidden, [], [gain_sums])
        w_u, w_d, w_o, grad_qkv = unpack(low_mlp, low_attn, N_COLOR, 0, width, hidden, partial, [])
        gain_sums = gain_sums / n_dev
        grad_qkv = unpack_qkv(last, grad_qkv)
        weights = (grad_qkv, w_o, w_u, w_d.reshape(n_layers, hidden, width))
        return (grad_cur[None], gain_sums[:n_layers], gain_sums[n_layers:2 * n_layers]) + weights

    batch_spec = P('data')
    full_spec = P()
    return jax.shard_map(local_step, mesh=mesh, in_specs=(batch_spec, batch_spec) + (full_spec,) * 6, out_specs=(batch_spec,) + (full_spec,) * 6, check_vma=False)
```

```python
import functools

import jax
import jax.numpy as jnp
from jax import lax
from jax.experimental import pallas as pl
from jax.experimental.pallas import tpu as pltpu
from jax.sharding import PartitionSpec as P

NORM_EPS = 1e-6
HEAD_DIM = 64
LANES = 128
Q_BLK = 256
EXP_SCALE = HEAD_DIM ** -0.5 * 1.4426950408889634
NEG = -1e30
MIB = 2 ** 20
VMEM_ALL = 67043328
MESH = pl.DeviceIdType.MESH


def cost(gflops, mbytes):
    return pl.CostEstimate(flops=gflops * 10 ** 9, bytes_accessed=mbytes * MIB, transcendentals=0)


def rms_gain(rows_f, gain_vec):
    return rows_f * lax.rsqrt(jnp.mean(rows_f * rows_f, axis=-1, keepdims=True) + NORM_EPS) * gain_vec


def gelu_tanh(pre_act):
    return jax.nn.gelu(pre_act, approximate=True)


def dot_lo(lhs, rhs):
    return jnp.dot(lhs, rhs, preferred_element_type=jnp.float32).astype(jnp.bfloat16)


def dot_nt(lhs, rhs):
    return lax.dot_general(lhs, rhs, (((1,), (1,)), ((), ())), preferred_element_type=jnp.float32)


def dot_tn(lhs, rhs):
    return lax.dot_general(lhs, rhs, (((0,), (0,)), ((), ())), preferred_element_type=jnp.float32)


def dot_nn(lhs, rhs):
    return jnp.dot(lhs, rhs, preferred_element_type=jnp.float32)


def head_mask(ref_rows, head):
    lane = lax.broadcasted_iota(jnp.int32, ref_rows.shape, 1)
    return jnp.where(lane // HEAD_DIM == head, ref_rows, jnp.zeros_like(ref_rows))


def scores_t(k_ref, q_m, q_start):
    diag = dot_nt(k_ref[q_start:q_start + Q_BLK, :], q_m)
    key_i = lax.broadcasted_iota(jnp.int32, diag.shape, 0)
    query_i = lax.broadcasted_iota(jnp.int32, diag.shape, 1)
    diag = jnp.where(key_i <= query_i, diag, NEG)
    if q_start == 0:
        return diag
    return jnp.concatenate([dot_nt(k_ref[:q_start, :], q_m), diag], axis=0)


def attn_fwd_kernel(q_ref, k_ref, v_ref, o_ref, lse_ref, vt_ref, ot_ref):
    seq = q_ref.shape[0]
    vt_ref[...] = v_ref[...].T
    for head in range(LANES // HEAD_DIM):
        rows = slice(head * HEAD_DIM, (head + 1) * HEAD_DIM)
        for q_start in range(0, seq, Q_BLK):
            q_end = q_start + Q_BLK
            q_m = head_mask(q_ref[q_start:q_end, :], head)
            s_t = scores_t(k_ref, q_m, q_start)
            top = jnp.max(s_t, axis=0, keepdims=True)
            p_t = jnp.exp2((s_t - top) * EXP_SCALE)
            total = jnp.sum(p_t, axis=0, keepdims=True)
            p_lo = (p_t * (1.0 / total)).astype(jnp.bfloat16)
            ot_ref[rows, q_start:q_end] = dot_nn(vt_ref[rows, :q_end], p_lo)
            lse_ref[0, head:head + 1, q_start:q_end] = top * EXP_SCALE + jnp.log2(total)
    o_ref[...] = ot_ref[...].T.astype(jnp.bfloat16)


N_COLOR = 3
UNIT_COLS = 256
FF_BLK = 256
MLP_ROWS = 96
ATTN_ROWS = 144
MLP_CHUNKS = 3
GELU_C = 0.7978845608028654
AXIS_BITS = (3, 2, 1)


class Reducer:
    def __init__(self, n_chunks, refs, grad_refs=(), parts=()):
        (self.own, self.send0, self.recv0, self.send1, self.recv1, self.send2, self.recv2, self.send3, self.recv3, self.load_sem, self.send_sem, self.recv_sem) = refs
        self.grad_refs, self.parts = grad_refs, parts
        self.n_chunks = n_chunks
        me = lax.axis_index('data')
        self.me = me
        self.bit = [lax.rem(lax.div(me, 1 << b), 2) for b in range(4)]
        self.partner = [me + (1 - 2 * self.bit[b]) * (1 << b) for b in range(4)]

    def barrier(self):
        sem = pltpu.get_barrier_semaphore()
        for dev in self.partner:
            pl.semaphore_signal(sem, inc=1, device_id=(dev,), device_id_type=MESH)
        pl.semaphore_wait(sem, 4)

    def load(self, chunk, half):
        for color in range(N_COLOR):
            for part, (array, kind, col, row, n_rows) in enumerate(self.parts[chunk][color]):
                if kind == 'block':
                    src = self.grad_refs[array].at[col, :, half]
                else:
                    src = self.grad_refs[array].at[:, half, :, pl.ds(col, UNIT_COLS)]
                dst = self.own.at[chunk, color, :, pl.ds(row, n_rows)]
                pltpu.make_async_copy(src, dst, self.load_sem.at[chunk, color, part]).start()

    def wait_load(self, chunk):
        for color in range(N_COLOR):
            for part, (_, _, _, row, n_rows) in enumerate(self.parts[chunk][color]):
                ref = self.own.at[chunk, color, :, pl.ds(row, n_rows)]
                pltpu.make_async_copy(ref, ref, self.load_sem.at[chunk, color, part]).wait()

    def copy(self, stage, chunk, color):
        send = (self.send0, self.send1, self.send2, self.send3)[stage].at[chunk, color]
        recv = (self.recv0, self.recv1, self.recv2, self.recv3)[stage].at[chunk, color]
        dev = self.partner[0] if stage == 0 else self.partner[self.order(color)[stage - 1]]
        return pltpu.make_async_remote_copy(src_ref=send, dst_ref=recv, send_sem=self.send_sem.at[stage, chunk, color], recv_sem=self.recv_sem.at[stage, chunk, color], device_id=(dev,), device_id_type=MESH)

    def order(self, color):
        return [1 + (color + step) % N_COLOR for step in range(N_COLOR)]

    def block(self, values):
        return values[3] * 4 + values[2] * 2 + values[1]

    def convert(self, chunk):
        self.wait_load(chunk)
        for color in range(N_COLOR):
            def body(i, carry):
                self.send0[chunk, color, i] = self.own[chunk, color, i].astype(jnp.bfloat16)
                return carry
            lax.fori_loop(0, 8, body, 0)
            self.copy(0, chunk, color).start()

    def total(self, chunk, color, values, n_recv):
        order = self.order(color)
        index = self.block(values)
        acc = self.own[chunk, color, index] + self.recv0[chunk, color, index].astype(jnp.float32)
        if n_recv >= 2:
            acc = acc + self.recv1[chunk, color, values[order[1]] * 2 + values[order[2]]].astype(jnp.float32)
        if n_recv >= 3:
            acc = acc + self.recv2[chunk, color, values[order[2]]].astype(jnp.float32)
        if n_recv >= 4:
            acc = acc + self.recv3[chunk, color, 0].astype(jnp.float32)
        return acc

    def stage(self, step, chunk):
        send = (None, self.send1, self.send2, self.send3)[step]
        n_free = N_COLOR - step
        for color in range(N_COLOR):
            self.copy(step - 1, chunk, color).wait_recv()
            order = self.order(color)

            def body(i, carry):
                values = [0, 0, 0, 0]
                for done in range(step - 1):
                    values[order[done]] = self.bit[order[done]]
                values[order[step - 1]] = 1 - self.bit[order[step - 1]]
                if n_free == 2:
                    values[order[1]], values[order[2]] = lax.div(i, 2), lax.rem(i, 2)
                elif n_free == 1:
                    values[order[2]] = i
                send[chunk, color, i] = self.total(chunk, color, values, step).astype(jnp.bfloat16)
                return carry
            if n_free:
                lax.fori_loop(0, 1 << n_free, body, 0)
            else:
                body(0, 0)
            self.copy(step, chunk, color).start()

    def finish(self, chunk, out_ref):
        for color in range(N_COLOR):
            self.copy(3, chunk, color).wait_recv()
            out_ref[chunk * N_COLOR + color] = self.total(chunk, color, self.bit, 4).astype(jnp.bfloat16)
        for stage in range(4):
            for color in range(N_COLOR):
                self.copy(stage, chunk, color).wait_send()


def reducer_scratch(n_chunks, rows):
    def buf(blocks, dtype):
        return pltpu.VMEM((n_chunks, N_COLOR, blocks, rows, UNIT_COLS), dtype)
    lo = jnp.bfloat16
    return [buf(8, jnp.float32), buf(8, lo), buf(8, lo), buf(4, lo), buf(4, lo), buf(2, lo), buf(2, lo), buf(1, lo), buf(1, lo), pltpu.SemaphoreType.DMA((n_chunks, N_COLOR, N_COLOR)), pltpu.SemaphoreType.DMA((4, n_chunks, N_COLOR)), pltpu.SemaphoreType.DMA((4, n_chunks, N_COLOR))]


def grad_view(grad_w):
    rows, cols = grad_w.shape
    return grad_w.reshape(8, 2, rows // 16, cols)


def qkv_parts(array):
    return [[(array + color, 'cols', part * UNIT_COLS, part * 48, 48) for part in range(3)] for color in range(N_COLOR)]


def rest_parts(block_array, out_array):
    return [[(block_array, 'block', color, 0, MLP_ROWS), (out_array, 'cols', color * UNIT_COLS, MLP_ROWS, 48)] for color in range(N_COLOR)]


def mlp_bwd_kernel(n_after, *refs):
    dy_ref, u_ref, z_ref, w1_ref, w2_ref = refs[:5]
    du_ref, block_ref, shard_ref, ut_ref, a_ref, dz_ref = refs[5 + n_after:11 + n_after]
    red = Reducer(MLP_CHUNKS, refs[11 + n_after:])
    step = pl.program_id(0)
    n_blk = dz_ref.shape[1] // FF_BLK
    core = red.bit[0]
    seq = dy_ref.shape[0]

    @pl.when(step == 0)
    def _():
        red.barrier()
        ut_ref[...] = u_ref[...].T

    for stage, first, count in ((3, 9, MLP_CHUNKS - 1), (2, 7, MLP_CHUNKS), (1, 4, MLP_CHUNKS)):
        @pl.when((step >= first) & (step < first + N_COLOR * count) & (lax.rem(step + 2 * first, N_COLOR) == 0))
        def _():
            red.stage(stage, lax.div(step - first, N_COLOR))

    @pl.when(step < n_blk)
    def _():
        cols = pl.ds(pl.multiple_of(step * FF_BLK, FF_BLK), FF_BLK)
        for row in range(0, seq, 256):
            rows = slice(row, row + 256)
            da = dot_nt(dy_ref[rows, :], w2_ref[0]).astype(jnp.bfloat16).astype(jnp.float32)
            z = z_ref[rows, :].astype(jnp.float32)
            z_sq = z * z
            th = jnp.tanh(z * (GELU_C + (GELU_C * 0.044715) * z_sq))
            cdf = 0.5 + 0.5 * th
            a_ref[rows, :] = (z * cdf).astype(jnp.bfloat16)
            slope = cdf + (0.5 * z) * (1.0 - th * th) * (GELU_C + (3.0 * GELU_C * 0.044715) * z_sq)
            dz_ref[rows, cols] = (slope * da).astype(jnp.bfloat16)
        dw1 = dot_nn(ut_ref[...], dz_ref[:, cols])
        block_ref[0, :, :, 0:48, :] = dw1.reshape(8, 2, 48, UNIT_COLS)
        dw2 = dot_nn(a_ref[...].T, dy_ref[...])
        for part in range(3):
            block_ref[0, :, :, 48 + 16 * part:64 + 16 * part, :] = dw2[:, part * UNIT_COLS:(part + 1) * UNIT_COLS].reshape(8, 2, 16, UNIT_COLS)

    @pl.when(step < N_COLOR * MLP_CHUNKS)
    def _():
        chunk, color = lax.div(step, N_COLOR), lax.rem(step, N_COLOR)

        def body(i, carry):
            red.own[chunk, color, i] = block_ref[0, i, core]
            red.send0[chunk, color, i] = block_ref[0, i, 1 - core].astype(jnp.bfloat16)
            return carry
        lax.fori_loop(0, 8, body, 0)
        red.copy(0, chunk, color).start()

    @pl.when(step >= n_blk)
    def _():
        du_ref[...] = dot_nt(dz_ref[...], w1_ref[0]).astype(jnp.bfloat16)

    @pl.when(step == pl.num_programs(0) - 1)
    def _():
        red.stage(3, MLP_CHUNKS - 1)
        for chunk in range(MLP_CHUNKS):
            red.finish(chunk, shard_ref)


def mlp_backward(dy, u_two, z_lo, w_up, w_down, layer, after, call_id):
    seq, width = dy.shape
    n_blk = w_up.shape[2] // FF_BLK
    n_last = width // 256
    last = n_blk - N_COLOR
    whole = pl.BlockSpec((seq, width), lambda step: (0, 0))
    shard_shape = (N_COLOR * MLP_CHUNKS, MLP_ROWS, UNIT_COLS)
    return pl.pallas_call(
        functools.partial(mlp_bwd_kernel, len(after)),
        grid=(n_blk + n_last,),
        in_specs=[
            whole, whole,
            pl.BlockSpec((seq, FF_BLK), lambda step: (0, jnp.minimum(step, n_blk - 1))),
            pl.BlockSpec((1, 256, w_up.shape[2]), lambda step: (layer, jnp.maximum(step - n_blk, 0), 0)),
            pl.BlockSpec((1, FF_BLK, width), lambda step: (layer, jnp.minimum(step, n_blk - 1), 0)),
        ] + [pl.BlockSpec(memory_space=pl.ANY)] * len(after),
        out_specs=[
            pl.BlockSpec((seq, 256), lambda step: (0, jnp.maximum(step - n_blk, 0))),
            pl.BlockSpec((1, 8, 2, MLP_ROWS, UNIT_COLS), lambda step: (jnp.clip(step - last, 0, N_COLOR - 1), 0, 0, 0, 0)),
            pl.BlockSpec(shard_shape, lambda step: (0, 0, 0)),
        ],
        out_shape=[jax.ShapeDtypeStruct((seq, width), jnp.bfloat16), jax.ShapeDtypeStruct((N_COLOR, 8, 2, MLP_ROWS, UNIT_COLS), jnp.float32), jax.ShapeDtypeStruct(shard_shape, jnp.bfloat16)],
        scratch_shapes=[pltpu.VMEM((width, seq), jnp.bfloat16), pltpu.VMEM((seq, FF_BLK), jnp.bfloat16), pltpu.VMEM((seq, w_up.shape[2]), jnp.bfloat16)] + reducer_scratch(MLP_CHUNKS, MLP_ROWS),
        compiler_params=pltpu.CompilerParams(dimension_semantics=("arbitrary",), vmem_limit_bytes=VMEM_ALL, collective_id=call_id),
        cost_estimate=cost(30, 30),
        name="mlp_bwd",
    )(dy, u_two, z_lo, w_up, w_down, *after)


def attn_bwd_kernel(parts, n_grads, n_after, *refs):
    q_ref, k_ref, v_ref, do_ref, lse_ref, u_ref = refs[:6]
    grad_refs = refs[6:6 + n_grads]
    refs = refs[6 + n_grads + n_after:]
    dq_ref, dk_ref, dv_ref, dwq_ref, dwk_ref, dwv_ref, shard_ref, ut_ref, kt_ref, dqt_ref, dk_acc, dv_acc = refs[:12]
    red = Reducer(len(parts), refs[12:], grad_refs, parts)
    n_chunks = red.n_chunks
    pair = pl.program_id(0)
    seq = q_ref.shape[0]
    events = {}
    for chunk in range(n_chunks):
        events.setdefault(1 + chunk, []).append((1, chunk))
        events.setdefault(4 + 2 * chunk, []).append((2, chunk))
        events.setdefault(7 + 2 * chunk, []).append((3, chunk))

    @pl.when(pair == 0)
    def _():
        red.barrier()
        for chunk in range(n_chunks):
            red.load(chunk, 1 - red.bit[0])
        for chunk in range(n_chunks):
            red.convert(chunk)
            red.load(chunk, red.bit[0])
        ut_ref[...] = u_ref[...].T

    kt_ref[...] = k_ref[...].T
    for head in range(LANES // HEAD_DIM):
        for when, todo in events.items():
            if when % 2 == head:
                @pl.when(pair == when // 2)
                def _():
                    for stage, chunk in todo:
                        if stage == 1:
                            red.wait_load(chunk)
                        red.stage(stage, chunk)
        rows = slice(head * HEAD_DIM, (head + 1) * HEAD_DIM)
        for q_start in range(0, seq, Q_BLK):
            q_end = q_start + Q_BLK
            q_m = head_mask(q_ref[q_start:q_end, :], head)
            do_m = head_mask(do_ref[q_start:q_end, :], head)
            s_t = scores_t(k_ref, q_m, q_start)
            p_t = jnp.exp2(s_t * EXP_SCALE - lse_ref[0, head:head + 1, q_start:q_end])
            dp_t = dot_nt(v_ref[:q_end, :], do_m)
            delta = jnp.sum(p_t * dp_t, axis=0, keepdims=True)
            ds_t = (p_t * (dp_t - delta) * HEAD_DIM ** -0.5).astype(jnp.bfloat16)
            dv_part = dot_nn(p_t.astype(jnp.bfloat16), do_m)
            dk_part = dot_nn(ds_t, q_m)
            if head == 0 and q_start == 0:
                dv_acc[...] = jnp.zeros_like(dv_acc)
                dk_acc[...] = jnp.zeros_like(dk_acc)
            dv_acc[:q_end, :] += dv_part
            dk_acc[:q_end, :] += dk_part
            dqt_ref[rows, q_start:q_end] = dot_nn(kt_ref[rows, :q_end], ds_t)
    dq_ref[...] = dqt_ref[...].T.astype(jnp.bfloat16)
    dk_ref[...] = dk_acc[...].astype(jnp.bfloat16)
    dv_ref[...] = dv_acc[...].astype(jnp.bfloat16)
    d_w = dot_nn(ut_ref[...], jnp.concatenate([dq_ref[...], dk_ref[...], dv_ref[...]], axis=1))
    for out_ref, at in ((dwq_ref, 0), (dwk_ref, LANES), (dwv_ref, 2 * LANES)):
        out_ref[...] = d_w[:, at:at + LANES].reshape(out_ref.shape)

    @pl.when(pair == pl.num_programs(0) - 1)
    def _():
        for chunk in range(n_chunks):
            red.finish(chunk, shard_ref)


def tail_kernel(parts, n_grads, n_after, *refs):
    gains_ref = refs[0]
    grad_refs = refs[1:1 + n_grads]
    refs = refs[:1 + n_grads] + refs[1 + n_grads + n_after:]
    shard_ref, gsum_ref, gbuf, gsend_sem, grecv_sem = refs[1 + n_grads:6 + n_grads]
    red = Reducer(len(parts), refs[6 + n_grads:], grad_refs, parts)
    n_dev = gbuf.shape[0]
    for chunk in range(red.n_chunks):
        red.load(chunk, 1 - red.bit[0])
    sem = pltpu.get_barrier_semaphore()
    for shift in range(1, n_dev):
        pl.semaphore_signal(sem, inc=1, device_id=(lax.rem(red.me + shift, n_dev),), device_id_type=MESH)
    pl.semaphore_wait(sem, n_dev - 1)

    def gain_copy(shift):
        dev = lax.rem(red.me + shift, n_dev)
        return pltpu.make_async_remote_copy(src_ref=gains_ref, dst_ref=gbuf.at[shift], send_sem=gsend_sem.at[shift], recv_sem=grecv_sem.at[shift], device_id=(dev,), device_id_type=MESH)
    for shift in range(1, n_dev):
        gain_copy(shift).start()
    gbuf[0] = gains_ref[...]
    for chunk in range(red.n_chunks):
        red.convert(chunk)
        red.load(chunk, red.bit[0])
    for step in range(1, 4):
        for chunk in range(red.n_chunks):
            if step == 1:
                red.wait_load(chunk)
            red.stage(step, chunk)
    for shift in range(1, n_dev):
        gain_copy(shift).wait()
    acc = jnp.zeros(gains_ref.shape, jnp.float32)
    for dev in range(n_dev):
        acc = acc + gbuf[lax.rem(red.me + n_dev - dev, n_dev)]
    gsum_ref[...] = acc
    for chunk in range(red.n_chunks):
        red.finish(chunk, shard_ref)


def attn_specs(seq, n_pairs):
    def col(shift):
        return pl.BlockSpec((seq, LANES), lambda pair: (0, pair + shift))
    lse = pl.BlockSpec((1, 8, seq), lambda pair: (pair, 0, 0))
    return col, lse


def attn_forward(qkv):
    seq, width = qkv.shape[0], qkv.shape[1] // 3
    n_pairs = width // LANES
    col, lse = attn_specs(seq, n_pairs)
    return pl.pallas_call(
        attn_fwd_kernel,
        grid=(n_pairs,),
        in_specs=[col(0), col(n_pairs), col(2 * n_pairs)],
        out_specs=[col(0), lse],
        out_shape=[jax.ShapeDtypeStruct((seq, width), jnp.bfloat16), jax.ShapeDtypeStruct((n_pairs, 8, seq), jnp.float32)],
        scratch_shapes=[pltpu.VMEM((LANES, seq), jnp.bfloat16), pltpu.VMEM((LANES, seq), jnp.float32)],
        compiler_params=pltpu.CompilerParams(dimension_semantics=("arbitrary",), vmem_limit_bytes=48 * MIB),
        cost_estimate=cost(16, 8),
        name="attn_fwd",
    )(qkv, qkv, qkv)


def attn_backward(qkv, d_out, lse_vals, u_one, grads, parts, after, call_id):
    seq, width = qkv.shape[0], qkv.shape[1] // 3
    n_pairs = width // LANES
    col, lse = attn_specs(seq, n_pairs)
    shape = jax.ShapeDtypeStruct((seq, width), jnp.bfloat16)
    shard_shape = (len(parts) * N_COLOR, ATTN_ROWS, UNIT_COLS)
    d_w = pl.BlockSpec((8, 2, width // 16, LANES), lambda pair: (0, 0, 0, pair))
    out = pl.pallas_call(
        functools.partial(attn_bwd_kernel, parts, len(grads), len(after)),
        grid=(n_pairs,),
        in_specs=[col(0), col(n_pairs), col(2 * n_pairs), col(0), lse, pl.BlockSpec((seq, width), lambda pair: (0, 0))] + [pl.BlockSpec(memory_space=pl.ANY)] * (len(grads) + len(after)),
        out_specs=[col(0), col(0), col(0), d_w, d_w, d_w, pl.BlockSpec(shard_shape, lambda pair: (0, 0, 0))],
        out_shape=[shape, shape, shape] + [jax.ShapeDtypeStruct((8, 2, width // 16, width), jnp.float32)] * 3 + [jax.ShapeDtypeStruct(shard_shape, jnp.bfloat16)],
        scratch_shapes=[pltpu.VMEM((width, seq), jnp.bfloat16), pltpu.VMEM((LANES, seq), jnp.bfloat16), pltpu.VMEM((LANES, seq), jnp.float32), pltpu.VMEM((seq, LANES), jnp.float32), pltpu.VMEM((seq, LANES), jnp.float32)] + reducer_scratch(len(parts), ATTN_ROWS),
        compiler_params=pltpu.CompilerParams(dimension_semantics=("arbitrary",), vmem_limit_bytes=VMEM_ALL, collective_id=call_id),
        cost_estimate=cost(40, 14),
        name="attn_bwd",
    )(qkv, qkv, qkv, d_out, lse_vals, u_one, *grads, *after)
    return out[:3], list(out[3:6]), out[6]


def tail_reduce(gains, grads, parts, after, call_id, n_dev):
    n_chunks = len(parts)
    shard_shape = (n_chunks * N_COLOR, ATTN_ROWS, UNIT_COLS)
    return pl.pallas_call(
        functools.partial(tail_kernel, parts, len(grads), len(after)),
        in_specs=[pl.BlockSpec(memory_space=pltpu.VMEM)] + [pl.BlockSpec(memory_space=pl.ANY)] * (len(grads) + len(after)),
        out_specs=[pl.BlockSpec(memory_space=pltpu.VMEM)] * 2,
        out_shape=[jax.ShapeDtypeStruct(shard_shape, jnp.bfloat16), jax.ShapeDtypeStruct(gains.shape, jnp.float32)],
        scratch_shapes=[pltpu.VMEM((n_dev,) + gains.shape, jnp.float32), pltpu.SemaphoreType.DMA((n_dev,)), pltpu.SemaphoreType.DMA((n_dev,))] + reducer_scratch(n_chunks, ATTN_ROWS),
        compiler_params=pltpu.CompilerParams(vmem_limit_bytes=40 * MIB, collective_id=call_id),
        cost_estimate=cost(20, 14),
        name="tail_reduce",
    )(gains, *grads, *after)


def block_forward(x_blk, gain_a, gain_b, w_qkv, w_out, w_up):
    norm_a, norm_a_back = jax.vjp(rms_gain, x_blk.astype(jnp.float32), gain_a)
    u_one = norm_a.astype(jnp.bfloat16)
    qkv = dot_lo(u_one, w_qkv)
    attn_out, lse_vals = attn_forward(qkv)
    hidden = x_blk + dot_lo(attn_out, w_out)
    norm_b, norm_b_back = jax.vjp(rms_gain, hidden.astype(jnp.float32), gain_b)
    u_two = norm_b.astype(jnp.bfloat16)
    pre_lo = dot_lo(u_two, w_up)
    act_lo = gelu_tanh(pre_lo.astype(jnp.float32)).astype(jnp.bfloat16)
    return hidden, act_lo, (norm_a_back, u_one, qkv, lse_vals, attn_out, norm_b_back, u_two, pre_lo)


def block_backward(grad_blk, saved_vals, w_qkv, w_out, w_up, w_down, layer, ready, after):
    (norm_a_back, u_one, qkv, lse_vals, attn_out, norm_b_back, u_two, pre_lo) = saved_vals
    ids = len(ready)
    grad_u_two, block, shard_mlp = mlp_backward(grad_blk, u_two, pre_lo, w_up, w_down, layer, after[:1], ids)
    grad_h_norm, grad_gain_b = norm_b_back(grad_u_two.astype(jnp.float32))
    grad_hidden = (grad_blk.astype(jnp.float32) + grad_h_norm).astype(jnp.bfloat16)
    grad_out_w = dot_tn(attn_out, grad_hidden)
    grad_attn = dot_nt(grad_hidden, w_out).astype(jnp.bfloat16)
    grads = ready + [block, grad_view(grad_out_w)]
    parts = [qkv_parts(0)] * (len(ready) // 3) + [rest_parts(len(ready), len(ready) + 1)]
    pieces, grad_qkv_w, shard_attn = attn_backward(qkv, grad_attn, lse_vals, u_one, grads, parts, after[1:], ids + 1)
    grad_qkv = jnp.concatenate(pieces, axis=1)
    grad_u_one = dot_nt(grad_qkv, w_qkv).astype(jnp.bfloat16)
    grad_x_norm, grad_gain_a = norm_a_back(grad_u_one.astype(jnp.float32))
    grad_x_blk = (grad_hidden.astype(jnp.float32) + grad_x_norm).astype(jnp.bfloat16)
    return grad_x_blk, grad_gain_a, grad_gain_b, grad_qkv_w, unit_gather(shard_mlp), unit_gather(shard_attn)


def unit_gather(shard):
    n_units, rows, cols = shard.shape
    flat = lax.all_gather(shard.reshape(n_units * rows, cols), 'data', axis=0, tiled=True)
    return flat.reshape(-1, n_units, rows, cols)


def put_qkv(unit_ref, out_ref, scale):
    for color in range(N_COLOR):
        for part in range(3):
            cols = slice((color * 3 + part) * UNIT_COLS, (color * 3 + part + 1) * UNIT_COLS)
            out_ref[0, :, cols] = unit_ref[0, color, part * 48:part * 48 + 48].astype(jnp.float32) * scale


def unpack_kernel(first, n_dev, n_out, *refs):
    mlp_ref, attn_ref = refs[:2]
    up_ref, down_ref, out_ref = refs[-n_out:][:3]
    scale = 1.0 / n_dev

    def value(unit):
        return unit.astype(jnp.float32) * scale
    n_mlp = mlp_ref.shape[1]
    for blk in range(n_mlp + N_COLOR):
        unit = mlp_ref[0, blk] if blk < n_mlp else attn_ref[0, first + blk - n_mlp, 0:MLP_ROWS]
        up_ref[0, :, blk * FF_BLK:(blk + 1) * FF_BLK] = value(unit[0:48])
        for part in range(3):
            down_ref[0, blk, 0, :, part * UNIT_COLS:(part + 1) * UNIT_COLS] = value(unit[48 + 16 * part:64 + 16 * part])
    for color in range(N_COLOR):
        out_ref[0, :, color * UNIT_COLS:(color + 1) * UNIT_COLS] = value(attn_ref[0, first + color, MLP_ROWS:ATTN_ROWS])
    if first:
        put_qkv(attn_ref, refs[-1], scale)


def unpack(mlp_all, attn_all, first, layer, width, hidden, into, after):
    n_dev = mlp_all.shape[0]
    def in_spec(arr):
        return pl.BlockSpec((1,) + arr.shape[1:], lambda dev: (dev, 0, 0, 0))
    def rows(shape, at):
        return pl.BlockSpec((1, width // n_dev, shape[2]), lambda dev: (at, dev, 0))
    n_blk = hidden // FF_BLK
    shapes = [(2, width, hidden), (2, n_blk, n_dev, FF_BLK // n_dev, width), (2, width, width)]
    down = pl.BlockSpec((1, n_blk, 1, FF_BLK // n_dev, width), lambda dev: (layer, 0, dev, 0, 0))
    out_specs = [rows(shapes[0], layer), down, rows(shapes[2], layer)]
    if first:
        shapes.append((2, width, 3 * width))
        out_specs.append(rows(shapes[3], layer + 1))
    return pl.pallas_call(
        functools.partial(unpack_kernel, first, n_dev, len(shapes)),
        grid=(n_dev,),
        in_specs=[in_spec(mlp_all), in_spec(attn_all)] + [pl.BlockSpec(memory_space=pl.ANY)] * (len(into) + len(after)),
        out_specs=out_specs,
        out_shape=[jax.ShapeDtypeStruct(shape, jnp.float32) for shape in shapes],
        input_output_aliases={2 + i: i for i in range(len(into))},
        compiler_params=pltpu.CompilerParams(dimension_semantics=("arbitrary",), vmem_limit_bytes=48 * MIB),
        cost_estimate=cost(10, 40),
        name="unpack",
    )(mlp_all, attn_all, *into, *after)


def unpack_qkv_kernel(n_dev, last_ref, into_ref, out_ref):
    put_qkv(last_ref, out_ref, 1.0 / n_dev)


def unpack_qkv(last_all, into):
    n_dev = last_all.shape[0]
    rows, cols = into.shape[1:]
    return pl.pallas_call(
        functools.partial(unpack_qkv_kernel, n_dev),
        grid=(n_dev,),
        in_specs=[pl.BlockSpec((1,) + last_all.shape[1:], lambda dev: (dev, 0, 0, 0)), pl.BlockSpec(memory_space=pl.ANY)],
        out_specs=pl.BlockSpec((1, rows // n_dev, cols), lambda dev: (0, dev, 0)),
        out_shape=jax.ShapeDtypeStruct(into.shape, jnp.float32),
        input_output_aliases={1: 0},
        compiler_params=pltpu.CompilerParams(dimension_semantics=("arbitrary",), vmem_limit_bytes=32 * MIB),
        cost_estimate=cost(4, 20),
        name="unpack_qkv",
    )(last_all, into)


def solution(mesh):
    n_dev = mesh.shape['data']

    def local_step(x_loc, grad_y_loc, gain_one, gain_two, w_qkv, w_out, w_up, w_down):
        n_layers = w_qkv.shape[0]
        hidden_x = x_loc[0]
        saved_all = []
        for layer_idx in range(n_layers):
            hidden, act_lo, saved_vals = block_forward(hidden_x, gain_one[layer_idx], gain_two[layer_idx], w_qkv[layer_idx], w_out[layer_idx], w_up[layer_idx])
            saved_all.append(saved_vals)
            if layer_idx + 1 < n_layers:
                hidden_x = hidden + dot_lo(act_lo, w_down[layer_idx])
        grad_cur = grad_y_loc[0]
        width, hidden = w_up.shape[1:]
        gains = [None] * (2 * n_layers)
        ready, after, gathered = [], [], []
        for layer_idx in reversed(range(n_layers)):
            out = block_backward(grad_cur, saved_all[layer_idx], w_qkv[layer_idx], w_out[layer_idx], w_up, w_down, layer_idx, ready, after)
            grad_cur, gains[layer_idx], gains[n_layers + layer_idx], grad_qkv_w = out[:4]
            ready, after = grad_qkv_w, list(out[4:])
            gathered.append(after)
        (top_mlp, top_attn), (low_mlp, low_attn) = gathered
        gain_rows = jnp.concatenate([jnp.stack(gains), jnp.zeros((8 - 2 * n_layers, width), jnp.float32)])
        shard, gain_sums = tail_reduce(gain_rows, ready, [qkv_parts(0)], [low_mlp], 3 * n_layers, n_dev)
        last = unit_gather(shard)
        partial = unpack(top_mlp, top_attn, 0, 1, width, hidden, [], [gain_sums])
        w_u, w_d, w_o, grad_qkv = unpack(low_mlp, low_attn, N_COLOR, 0, width, hidden, partial, [])
        gain_sums = gain_sums / n_dev
        grad_qkv = unpack_qkv(last, grad_qkv)
        weights = (grad_qkv, w_o, w_u, w_d.reshape(n_layers, hidden, width))
        return (grad_cur[None], gain_sums[:n_layers], gain_sums[n_layers:2 * n_layers]) + weights

    batch_spec = P('data')
    full_spec = P()
    return jax.shard_map(local_step, mesh=mesh, in_specs=(batch_spec, batch_spec) + (full_spec,) * 6, out_specs=(batch_spec,) + (full_spec,) * 6, check_vma=False)
```

```python
import functools

import jax
import jax.numpy as jnp
from jax import lax
from jax.experimental import pallas as pl
from jax.experimental.pallas import tpu as pltpu
from jax.sharding import PartitionSpec as P

NORM_EPS = 1e-6
HEAD_DIM = 64
LANES = 128
Q_BLK = 256
EXP_SCALE = HEAD_DIM ** -0.5 * 1.4426950408889634
NEG = -1e30
MIB = 2 ** 20
VMEM_ALL = 67043328
MESH = pl.DeviceIdType.MESH


def cost(gflops, mbytes):
    return pl.CostEstimate(flops=gflops * 10 ** 9, bytes_accessed=mbytes * MIB, transcendentals=0)


def rms_gain(rows_f, gain_vec):
    return rows_f * lax.rsqrt(jnp.mean(rows_f * rows_f, axis=-1, keepdims=True) + NORM_EPS) * gain_vec


def gelu_tanh(pre_act):
    return jax.nn.gelu(pre_act, approximate=True)


def dot_lo(lhs, rhs):
    return jnp.dot(lhs, rhs, preferred_element_type=jnp.float32).astype(jnp.bfloat16)


def dot_nt(lhs, rhs):
    return lax.dot_general(lhs, rhs, (((1,), (1,)), ((), ())), preferred_element_type=jnp.float32)


def dot_tn(lhs, rhs):
    return lax.dot_general(lhs, rhs, (((0,), (0,)), ((), ())), preferred_element_type=jnp.float32)


def dot_nn(lhs, rhs):
    return jnp.dot(lhs, rhs, preferred_element_type=jnp.float32)


def head_mask(ref_rows, head):
    lane = lax.broadcasted_iota(jnp.int32, ref_rows.shape, 1)
    return jnp.where(lane // HEAD_DIM == head, ref_rows, jnp.zeros_like(ref_rows))


def scores_t(k_ref, q_m, q_start):
    diag = dot_nt(k_ref[q_start:q_start + Q_BLK, :], q_m)
    key_i = lax.broadcasted_iota(jnp.int32, diag.shape, 0)
    query_i = lax.broadcasted_iota(jnp.int32, diag.shape, 1)
    diag = jnp.where(key_i <= query_i, diag, NEG)
    if q_start == 0:
        return diag
    return jnp.concatenate([dot_nt(k_ref[:q_start, :], q_m), diag], axis=0)


def attn_fwd_kernel(q_ref, k_ref, v_ref, o_ref, lse_ref, vt_ref, ot_ref):
    seq = q_ref.shape[0]
    vt_ref[...] = v_ref[...].T
    for head in range(LANES // HEAD_DIM):
        rows = slice(head * HEAD_DIM, (head + 1) * HEAD_DIM)
        for q_start in range(0, seq, Q_BLK):
            q_end = q_start + Q_BLK
            q_m = head_mask(q_ref[q_start:q_end, :], head)
            s_t = scores_t(k_ref, q_m, q_start)
            top = jnp.max(s_t, axis=0, keepdims=True)
            p_t = jnp.exp2((s_t - top) * EXP_SCALE)
            total = jnp.sum(p_t, axis=0, keepdims=True)
            p_lo = (p_t * (1.0 / total)).astype(jnp.bfloat16)
            ot_ref[rows, q_start:q_end] = dot_nn(vt_ref[rows, :q_end], p_lo)
            lse_ref[0, head:head + 1, q_start:q_end] = top * EXP_SCALE + jnp.log2(total)
    o_ref[...] = ot_ref[...].T.astype(jnp.bfloat16)


N_COLOR = 3
UNIT_COLS = 256
FF_BLK = 256
MLP_ROWS = 96
ATTN_ROWS = 144
MLP_CHUNKS = 3
GELU_C = 0.7978845608028654
AXIS_BITS = (3, 2, 1)


class Reducer:
    def __init__(self, n_chunks, refs, grad_refs=(), parts=()):
        (self.own, self.send0, self.recv0, self.send1, self.recv1, self.send2, self.recv2, self.send3, self.recv3, self.load_sem, self.send_sem, self.recv_sem) = refs
        self.grad_refs, self.parts = grad_refs, parts
        self.n_chunks = n_chunks
        me = lax.axis_index('data')
        self.me = me
        self.bit = [lax.rem(lax.div(me, 1 << b), 2) for b in range(4)]
        self.partner = [me + (1 - 2 * self.bit[b]) * (1 << b) for b in range(4)]

    def barrier(self):
        sem = pltpu.get_barrier_semaphore()
        for dev in self.partner:
            pl.semaphore_signal(sem, inc=1, device_id=(dev,), device_id_type=MESH)
        pl.semaphore_wait(sem, 4)

    def load(self, chunk, half):
        for color in range(N_COLOR):
            for part, (array, kind, col, row, n_rows) in enumerate(self.parts[chunk][color]):
                if kind == 'block':
                    src = self.grad_refs[array].at[col, :, half]
                else:
                    src = self.grad_refs[array].at[:, half, :, pl.ds(col, UNIT_COLS)]
                dst = self.own.at[chunk, color, :, pl.ds(row, n_rows)]
                pltpu.make_async_copy(src, dst, self.load_sem.at[chunk, color, part]).start()

    def wait_load(self, chunk):
        for color in range(N_COLOR):
            for part, (_, _, _, row, n_rows) in enumerate(self.parts[chunk][color]):
                ref = self.own.at[chunk, color, :, pl.ds(row, n_rows)]
                pltpu.make_async_copy(ref, ref, self.load_sem.at[chunk, color, part]).wait()

    def copy(self, stage, chunk, color):
        send = (self.send0, self.send1, self.send2, self.send3)[stage].at[chunk, color]
        recv = (self.recv0, self.recv1, self.recv2, self.recv3)[stage].at[chunk, color]
        dev = self.partner[0] if stage == 0 else self.partner[self.order(color)[stage - 1]]
        return pltpu.make_async_remote_copy(src_ref=send, dst_ref=recv, send_sem=self.send_sem.at[stage, chunk, color], recv_sem=self.recv_sem.at[stage, chunk, color], device_id=(dev,), device_id_type=MESH)

    def order(self, color):
        return [1 + (color + step) % N_COLOR for step in range(N_COLOR)]

    def block(self, values):
        return values[3] * 4 + values[2] * 2 + values[1]

    def convert(self, chunk):
        self.wait_load(chunk)
        for color in range(N_COLOR):
            def body(i, carry):
                self.send0[chunk, color, i] = self.own[chunk, color, i].astype(jnp.bfloat16)
                return carry
            lax.fori_loop(0, 8, body, 0)
            self.copy(0, chunk, color).start()

    def total(self, chunk, color, values, n_recv):
        order = self.order(color)
        index = self.block(values)
        acc = self.own[chunk, color, index] + self.recv0[chunk, color, index].astype(jnp.float32)
        if n_recv >= 2:
            acc = acc + self.recv1[chunk, color, values[order[1]] * 2 + values[order[2]]].astype(jnp.float32)
        if n_recv >= 3:
            acc = acc + self.recv2[chunk, color, values[order[2]]].astype(jnp.float32)
        if n_recv >= 4:
            acc = acc + self.recv3[chunk, color, 0].astype(jnp.float32)
        return acc

    def stage(self, step, chunk):
        send = (None, self.send1, self.send2, self.send3)[step]
        n_free = N_COLOR - step
        for color in range(N_COLOR):
            self.copy(step - 1, chunk, color).wait_recv()
            order = self.order(color)

            def body(i, carry):
                values = [0, 0, 0, 0]
                for done in range(step - 1):
                    values[order[done]] = self.bit[order[done]]
                values[order[step - 1]] = 1 - self.bit[order[step - 1]]
                if n_free == 2:
                    values[order[1]], values[order[2]] = lax.div(i, 2), lax.rem(i, 2)
                elif n_free == 1:
                    values[order[2]] = i
                send[chunk, color, i] = self.total(chunk, color, values, step).astype(jnp.bfloat16)
                return carry
            if n_free:
                lax.fori_loop(0, 1 << n_free, body, 0)
            else:
                body(0, 0)
            self.copy(step, chunk, color).start()

    def finish(self, chunk, out_ref, base=0):
        n_rows = self.own.shape[3]
        for color in range(N_COLOR):
            self.copy(3, chunk, color).wait_recv()
            row = base + (chunk * N_COLOR + color) * n_rows
            out_ref[row:row + n_rows, :] = self.total(chunk, color, self.bit, 4).astype(jnp.bfloat16)
        for stage in range(4):
            for color in range(N_COLOR):
                self.copy(stage, chunk, color).wait_send()


def reducer_scratch(n_chunks, rows):
    def buf(blocks, dtype):
        return pltpu.VMEM((n_chunks, N_COLOR, blocks, rows, UNIT_COLS), dtype)
    lo = jnp.bfloat16
    return [buf(8, jnp.float32), buf(8, lo), buf(8, lo), buf(4, lo), buf(4, lo), buf(2, lo), buf(2, lo), buf(1, lo), buf(1, lo), pltpu.SemaphoreType.DMA((n_chunks, N_COLOR, N_COLOR)), pltpu.SemaphoreType.DMA((4, n_chunks, N_COLOR)), pltpu.SemaphoreType.DMA((4, n_chunks, N_COLOR))]


def grad_view(grad_w):
    rows, cols = grad_w.shape
    return grad_w.reshape(8, 2, rows // 16, cols)


def qkv_parts(array):
    return [[(array + color, 'cols', part * UNIT_COLS, part * 48, 48) for part in range(3)] for color in range(N_COLOR)]


def rest_parts(block_array, out_array):
    return [[(block_array, 'block', color, 0, MLP_ROWS), (out_array, 'cols', color * UNIT_COLS, MLP_ROWS, 48)] for color in range(N_COLOR)]


def mlp_bwd_kernel(parts, n_grads, n_after, *refs):
    dy_ref, u_ref, z_ref, w1_ref, w2_ref = refs[:5]
    grad_refs = refs[5:5 + n_grads]
    refs = refs[5 + n_grads + n_after:]
    du_ref, block_ref, shard_ref, ut_ref, a_ref, dz_ref = refs[:6]
    n_red = (len(refs) - 6) // (2 if parts else 1)
    red = Reducer(MLP_CHUNKS, refs[6:6 + n_red])
    early = Reducer(len(parts), refs[6 + n_red:], grad_refs, parts) if parts else None
    step = pl.program_id(0)
    n_blk = dz_ref.shape[1] // FF_BLK
    core = red.bit[0]
    seq = dy_ref.shape[0]

    @pl.when(step == 0)
    def _():
        red.barrier()
        if early:
            early.load(0, 1 - core)
        ut_ref[...] = u_ref[...].T

    if early:
        @pl.when(step == 1)
        def _():
            early.convert(0)
            early.load(0, core)

        for stage, when in ((1, 2), (2, 5), (3, 7)):
            @pl.when(step == when)
            def _():
                if stage == 1:
                    early.wait_load(0)
                early.stage(stage, 0)

        @pl.when(step == n_blk - 1)
        def _():
            early.finish(0, shard_ref, N_COLOR * MLP_CHUNKS * MLP_ROWS)

    for stage, first, count in ((3, 9, MLP_CHUNKS - 1), (2, 7, MLP_CHUNKS), (1, 4, MLP_CHUNKS)):
        @pl.when((step >= first) & (step < first + N_COLOR * count) & (lax.rem(step + 2 * first, N_COLOR) == 0))
        def _():
            red.stage(stage, lax.div(step - first, N_COLOR))

    @pl.when(step < n_blk)
    def _():
        cols = pl.ds(pl.multiple_of(step * FF_BLK, FF_BLK), FF_BLK)
        for row in range(0, seq, 256):
            rows = slice(row, row + 256)
            da = dot_nt(dy_ref[rows, :], w2_ref[0]).astype(jnp.bfloat16).astype(jnp.float32)
            z = z_ref[rows, :].astype(jnp.float32)
            z_sq = z * z
            th = jnp.tanh(z * (GELU_C + (GELU_C * 0.044715) * z_sq))
            cdf = 0.5 + 0.5 * th
            a_ref[rows, :] = (z * cdf).astype(jnp.bfloat16)
            slope = cdf + (0.5 * z) * (1.0 - th * th) * (GELU_C + (3.0 * GELU_C * 0.044715) * z_sq)
            dz_ref[rows, cols] = (slope * da).astype(jnp.bfloat16)
        dw1 = dot_nn(ut_ref[...], dz_ref[:, cols])
        block_ref[0, :, :, 0:48, :] = dw1.reshape(8, 2, 48, UNIT_COLS)
        dw2 = dot_nn(a_ref[...].T, dy_ref[...])
        for part in range(3):
            block_ref[0, :, :, 48 + 16 * part:64 + 16 * part, :] = dw2[:, part * UNIT_COLS:(part + 1) * UNIT_COLS].reshape(8, 2, 16, UNIT_COLS)

    @pl.when(step < N_COLOR * MLP_CHUNKS)
    def _():
        chunk, color = lax.div(step, N_COLOR), lax.rem(step, N_COLOR)

        def body(i, carry):
            red.own[chunk, color, i] = block_ref[0, i, core]
            red.send0[chunk, color, i] = block_ref[0, i, 1 - core].astype(jnp.bfloat16)
            return carry
        lax.fori_loop(0, 8, body, 0)
        red.copy(0, chunk, color).start()

    @pl.when(step >= n_blk)
    def _():
        du_ref[...] = dot_nt(dz_ref[...], w1_ref[0]).astype(jnp.bfloat16)

    @pl.when(step == pl.num_programs(0) - 1)
    def _():
        red.stage(3, MLP_CHUNKS - 1)
        for chunk in range(MLP_CHUNKS):
            red.finish(chunk, shard_ref)


def mlp_backward(dy, u_two, z_lo, w_up, w_down, layer, grads, after, call_id):
    seq, width = dy.shape
    n_blk = w_up.shape[2] // FF_BLK
    n_last = width // 256
    last = n_blk - N_COLOR
    whole = pl.BlockSpec((seq, width), lambda step: (0, 0))
    parts = [qkv_parts(0)] if grads else []
    shard_shape = (N_COLOR * (MLP_CHUNKS * MLP_ROWS + len(parts) * ATTN_ROWS), UNIT_COLS)
    return pl.pallas_call(
        functools.partial(mlp_bwd_kernel, parts, len(grads), len(after)),
        grid=(n_blk + n_last,),
        in_specs=[
            whole, whole,
            pl.BlockSpec((seq, FF_BLK), lambda step: (0, jnp.minimum(step, n_blk - 1))),
            pl.BlockSpec((1, 256, w_up.shape[2]), lambda step: (layer, jnp.maximum(step - n_blk, 0), 0)),
            pl.BlockSpec((1, FF_BLK, width), lambda step: (layer, jnp.minimum(step, n_blk - 1), 0)),
        ] + [pl.BlockSpec(memory_space=pl.ANY)] * (len(grads) + len(after)),
        out_specs=[
            pl.BlockSpec((seq, 256), lambda step: (0, jnp.maximum(step - n_blk, 0))),
            pl.BlockSpec((1, 8, 2, MLP_ROWS, UNIT_COLS), lambda step: (jnp.clip(step - last, 0, N_COLOR - 1), 0, 0, 0, 0)),
            pl.BlockSpec(shard_shape, lambda step: (0, 0)),
        ],
        out_shape=[jax.ShapeDtypeStruct((seq, width), jnp.bfloat16), jax.ShapeDtypeStruct((N_COLOR, 8, 2, MLP_ROWS, UNIT_COLS), jnp.float32), jax.ShapeDtypeStruct(shard_shape, jnp.bfloat16)],
        scratch_shapes=[pltpu.VMEM((width, seq), jnp.bfloat16), pltpu.VMEM((seq, FF_BLK), jnp.bfloat16), pltpu.VMEM((seq, w_up.shape[2]), jnp.bfloat16)] + reducer_scratch(MLP_CHUNKS, MLP_ROWS) + (reducer_scratch(1, ATTN_ROWS) if parts else []),
        compiler_params=pltpu.CompilerParams(dimension_semantics=("arbitrary",), vmem_limit_bytes=VMEM_ALL, collective_id=call_id),
        cost_estimate=cost(30, 30),
        name="mlp_bwd",
    )(dy, u_two, z_lo, w_up, w_down, *grads, *after)


def attn_bwd_kernel(parts, n_grads, n_after, *refs):
    q_ref, k_ref, v_ref, do_ref, lse_ref, u_ref = refs[:6]
    grad_refs = refs[6:6 + n_grads]
    refs = refs[6 + n_grads + n_after:]
    dq_ref, dk_ref, dv_ref, dwq_ref, dwk_ref, dwv_ref, shard_ref, ut_ref, kt_ref, dqt_ref, dk_acc, dv_acc = refs[:12]
    red = Reducer(len(parts), refs[12:], grad_refs, parts)
    n_chunks = red.n_chunks
    pair = pl.program_id(0)
    seq = q_ref.shape[0]
    events = {}
    for chunk in range(n_chunks):
        events.setdefault(1 + chunk, []).append((1, chunk))
        events.setdefault(4 + 2 * chunk, []).append((2, chunk))
        events.setdefault(7 + 2 * chunk, []).append((3, chunk))

    @pl.when(pair == 0)
    def _():
        red.barrier()
        for chunk in range(n_chunks):
            red.load(chunk, 1 - red.bit[0])
        for chunk in range(n_chunks):
            red.convert(chunk)
            red.load(chunk, red.bit[0])
        ut_ref[...] = u_ref[...].T

    kt_ref[...] = k_ref[...].T
    for head in range(LANES // HEAD_DIM):
        for when, todo in events.items():
            if when % 2 == head:
                @pl.when(pair == when // 2)
                def _():
                    for stage, chunk in todo:
                        if stage == 1:
                            red.wait_load(chunk)
                        red.stage(stage, chunk)
        rows = slice(head * HEAD_DIM, (head + 1) * HEAD_DIM)
        for q_start in range(0, seq, Q_BLK):
            q_end = q_start + Q_BLK
            q_m = head_mask(q_ref[q_start:q_end, :], head)
            do_m = head_mask(do_ref[q_start:q_end, :], head)
            s_t = scores_t(k_ref, q_m, q_start)
            p_t = jnp.exp2(s_t * EXP_SCALE - lse_ref[0, head:head + 1, q_start:q_end])
            dp_t = dot_nt(v_ref[:q_end, :], do_m)
            delta = jnp.sum(p_t * dp_t, axis=0, keepdims=True)
            ds_t = (p_t * (dp_t - delta) * HEAD_DIM ** -0.5).astype(jnp.bfloat16)
            dv_part = dot_nn(p_t.astype(jnp.bfloat16), do_m)
            dk_part = dot_nn(ds_t, q_m)
            if head == 0 and q_start == 0:
                dv_acc[...] = jnp.zeros_like(dv_acc)
                dk_acc[...] = jnp.zeros_like(dk_acc)
            dv_acc[:q_end, :] += dv_part
            dk_acc[:q_end, :] += dk_part
            dqt_ref[rows, q_start:q_end] = dot_nn(kt_ref[rows, :q_end], ds_t)
    dq_ref[...] = dqt_ref[...].T.astype(jnp.bfloat16)
    dk_ref[...] = dk_acc[...].astype(jnp.bfloat16)
    dv_ref[...] = dv_acc[...].astype(jnp.bfloat16)
    d_w = dot_nn(ut_ref[...], jnp.concatenate([dq_ref[...], dk_ref[...], dv_ref[...]], axis=1))
    for out_ref, at in ((dwq_ref, 0), (dwk_ref, LANES), (dwv_ref, 2 * LANES)):
        out_ref[...] = d_w[:, at:at + LANES].reshape(out_ref.shape)

    @pl.when(pair == pl.num_programs(0) - 1)
    def _():
        for chunk in range(n_chunks):
            red.finish(chunk, shard_ref)


def tail_kernel(parts, n_grads, n_after, *refs):
    gains_ref = refs[0]
    grad_refs = refs[1:1 + n_grads]
    refs = refs[:1 + n_grads] + refs[1 + n_grads + n_after:]
    shard_ref, gsum_ref, gbuf, gsend_sem, grecv_sem = refs[1 + n_grads:6 + n_grads]
    red = Reducer(len(parts), refs[6 + n_grads:], grad_refs, parts)
    n_dev = gbuf.shape[0]
    for chunk in range(red.n_chunks):
        red.load(chunk, 1 - red.bit[0])
    sem = pltpu.get_barrier_semaphore()
    for shift in range(1, n_dev):
        pl.semaphore_signal(sem, inc=1, device_id=(lax.rem(red.me + shift, n_dev),), device_id_type=MESH)
    pl.semaphore_wait(sem, n_dev - 1)

    def gain_copy(shift):
        dev = lax.rem(red.me + shift, n_dev)
        return pltpu.make_async_remote_copy(src_ref=gains_ref, dst_ref=gbuf.at[shift], send_sem=gsend_sem.at[shift], recv_sem=grecv_sem.at[shift], device_id=(dev,), device_id_type=MESH)
    for shift in range(1, n_dev):
        gain_copy(shift).start()
    gbuf[0] = gains_ref[...]
    for chunk in range(red.n_chunks):
        red.convert(chunk)
        red.load(chunk, red.bit[0])
    for step in range(1, 4):
        for chunk in range(red.n_chunks):
            if step == 1:
                red.wait_load(chunk)
            red.stage(step, chunk)
    for shift in range(1, n_dev):
        gain_copy(shift).wait()
    acc = jnp.zeros(gains_ref.shape, jnp.float32)
    for dev in range(n_dev):
        acc = acc + gbuf[lax.rem(red.me + n_dev - dev, n_dev)]
    gsum_ref[...] = acc
    for chunk in range(red.n_chunks):
        red.finish(chunk, shard_ref)


def attn_specs(seq, n_pairs):
    def col(shift):
        return pl.BlockSpec((seq, LANES), lambda pair: (0, pair + shift))
    lse = pl.BlockSpec((1, 8, seq), lambda pair: (pair, 0, 0))
    return col, lse


def attn_forward(qkv):
    seq, width = qkv.shape[0], qkv.shape[1] // 3
    n_pairs = width // LANES
    col, lse = attn_specs(seq, n_pairs)
    return pl.pallas_call(
        attn_fwd_kernel,
        grid=(n_pairs,),
        in_specs=[col(0), col(n_pairs), col(2 * n_pairs)],
        out_specs=[col(0), lse],
        out_shape=[jax.ShapeDtypeStruct((seq, width), jnp.bfloat16), jax.ShapeDtypeStruct((n_pairs, 8, seq), jnp.float32)],
        scratch_shapes=[pltpu.VMEM((LANES, seq), jnp.bfloat16), pltpu.VMEM((LANES, seq), jnp.float32)],
        compiler_params=pltpu.CompilerParams(dimension_semantics=("arbitrary",), vmem_limit_bytes=48 * MIB),
        cost_estimate=cost(16, 8),
        name="attn_fwd",
    )(qkv, qkv, qkv)


def attn_backward(qkv, d_out, lse_vals, u_one, grads, parts, after, call_id):
    seq, width = qkv.shape[0], qkv.shape[1] // 3
    n_pairs = width // LANES
    col, lse = attn_specs(seq, n_pairs)
    shape = jax.ShapeDtypeStruct((seq, width), jnp.bfloat16)
    shard_shape = (len(parts) * N_COLOR * ATTN_ROWS, UNIT_COLS)
    d_w = pl.BlockSpec((8, 2, width // 16, LANES), lambda pair: (0, 0, 0, pair))
    out = pl.pallas_call(
        functools.partial(attn_bwd_kernel, parts, len(grads), len(after)),
        grid=(n_pairs,),
        in_specs=[col(0), col(n_pairs), col(2 * n_pairs), col(0), lse, pl.BlockSpec((seq, width), lambda pair: (0, 0))] + [pl.BlockSpec(memory_space=pl.ANY)] * (len(grads) + len(after)),
        out_specs=[col(0), col(0), col(0), d_w, d_w, d_w, pl.BlockSpec(shard_shape, lambda pair: (0, 0))],
        out_shape=[shape, shape, shape] + [pltpu.HBM((8, 2, width // 16, width), jnp.float32)] * 3 + [jax.ShapeDtypeStruct(shard_shape, jnp.bfloat16)],
        scratch_shapes=[pltpu.VMEM((width, seq), jnp.bfloat16), pltpu.VMEM((LANES, seq), jnp.bfloat16), pltpu.VMEM((LANES, seq), jnp.float32), pltpu.VMEM((seq, LANES), jnp.float32), pltpu.VMEM((seq, LANES), jnp.float32)] + reducer_scratch(len(parts), ATTN_ROWS),
        compiler_params=pltpu.CompilerParams(dimension_semantics=("arbitrary",), vmem_limit_bytes=VMEM_ALL, collective_id=call_id),
        cost_estimate=cost(40, 14),
        name="attn_bwd",
    )(qkv, qkv, qkv, d_out, lse_vals, u_one, *grads, *after)
    return out[:3], list(out[3:6]), out[6]


def tail_reduce(gains, grads, parts, after, call_id, n_dev):
    n_chunks = len(parts)
    shard_shape = (n_chunks * N_COLOR * ATTN_ROWS, UNIT_COLS)
    return pl.pallas_call(
        functools.partial(tail_kernel, parts, len(grads), len(after)),
        in_specs=[pl.BlockSpec(memory_space=pltpu.VMEM)] + [pl.BlockSpec(memory_space=pl.ANY)] * (len(grads) + len(after)),
        out_specs=[pl.BlockSpec(memory_space=pltpu.VMEM)] * 2,
        out_shape=[jax.ShapeDtypeStruct(shard_shape, jnp.bfloat16), jax.ShapeDtypeStruct(gains.shape, jnp.float32)],
        scratch_shapes=[pltpu.VMEM((n_dev,) + gains.shape, jnp.float32), pltpu.SemaphoreType.DMA((n_dev,)), pltpu.SemaphoreType.DMA((n_dev,))] + reducer_scratch(n_chunks, ATTN_ROWS),
        compiler_params=pltpu.CompilerParams(vmem_limit_bytes=40 * MIB, collective_id=call_id),
        cost_estimate=cost(20, 14),
        name="tail_reduce",
    )(gains, *grads, *after)


def block_forward(x_blk, gain_a, gain_b, w_qkv, w_out, w_up):
    norm_a, norm_a_back = jax.vjp(rms_gain, x_blk.astype(jnp.float32), gain_a)
    u_one = norm_a.astype(jnp.bfloat16)
    qkv = dot_lo(u_one, w_qkv)
    attn_out, lse_vals = attn_forward(qkv)
    hidden = x_blk + dot_lo(attn_out, w_out)
    norm_b, norm_b_back = jax.vjp(rms_gain, hidden.astype(jnp.float32), gain_b)
    u_two = norm_b.astype(jnp.bfloat16)
    pre_lo = dot_lo(u_two, w_up)
    act_lo = gelu_tanh(pre_lo.astype(jnp.float32)).astype(jnp.bfloat16)
    return hidden, act_lo, (norm_a_back, u_one, qkv, lse_vals, attn_out, norm_b_back, u_two, pre_lo)


def block_backward(grad_blk, saved_vals, w_qkv, w_out, w_up, w_down, layer, ready, after):
    (norm_a_back, u_one, qkv, lse_vals, attn_out, norm_b_back, u_two, pre_lo) = saved_vals
    ids = len(ready)
    grad_u_two, block, shard_mlp = mlp_backward(grad_blk, u_two, pre_lo, w_up, w_down, layer, ready, after[:1], ids)
    grad_h_norm, grad_gain_b = norm_b_back(grad_u_two.astype(jnp.float32))
    grad_hidden = (grad_blk.astype(jnp.float32) + grad_h_norm).astype(jnp.bfloat16)
    grad_out_w = dot_tn(attn_out, grad_hidden)
    grad_attn = dot_nt(grad_hidden, w_out).astype(jnp.bfloat16)
    grads = [block, grad_view(grad_out_w)]
    parts = [rest_parts(0, 1)]
    pieces, grad_qkv_w, shard_attn = attn_backward(qkv, grad_attn, lse_vals, u_one, grads, parts, after[1:], ids + 1)
    grad_qkv = jnp.concatenate(pieces, axis=1)
    grad_u_one = dot_nt(grad_qkv, w_qkv).astype(jnp.bfloat16)
    grad_x_norm, grad_gain_a = norm_a_back(grad_u_one.astype(jnp.float32))
    grad_x_blk = (grad_hidden.astype(jnp.float32) + grad_x_norm).astype(jnp.bfloat16)
    return grad_x_blk, grad_gain_a, grad_gain_b, grad_qkv_w, unit_gather(shard_mlp), unit_gather(shard_attn)


def unit_gather(shard):
    return lax.all_gather(shard, 'data', axis=0, tiled=True).reshape((-1,) + shard.shape)


def put_qkv(unit_ref, base, out_ref, scale):
    for color in range(N_COLOR):
        for part in range(3):
            cols = slice((color * 3 + part) * UNIT_COLS, (color * 3 + part + 1) * UNIT_COLS)
            row = base + color * ATTN_ROWS + part * 48
            out_ref[0, :, cols] = unit_ref[0, row:row + 48, :].astype(jnp.float32) * scale


def unpack_kernel(with_qkv, n_dev, n_out, *refs):
    mlp_ref, attn_ref = refs[:2]
    up_ref, down_ref, out_ref = refs[-n_out:][:3]
    scale = 1.0 / n_dev
    n_mlp = N_COLOR * MLP_CHUNKS

    def value(unit):
        return unit.astype(jnp.float32) * scale
    for blk in range(n_mlp + N_COLOR):
        ref, row = (mlp_ref, blk * MLP_ROWS) if blk < n_mlp else (attn_ref, (blk - n_mlp) * ATTN_ROWS)
        up_ref[0, :, blk * FF_BLK:(blk + 1) * FF_BLK] = value(ref[0, row:row + 48, :])
        for part in range(3):
            at = row + 48 + 16 * part
            down_ref[0, blk, 0, :, part * UNIT_COLS:(part + 1) * UNIT_COLS] = value(ref[0, at:at + 16, :])
    for color in range(N_COLOR):
        row = color * ATTN_ROWS + MLP_ROWS
        out_ref[0, :, color * UNIT_COLS:(color + 1) * UNIT_COLS] = value(attn_ref[0, row:row + 48, :])
    if with_qkv:
        put_qkv(mlp_ref, n_mlp * MLP_ROWS, refs[-1], scale)


def unpack(mlp_all, attn_all, with_qkv, layer, width, hidden, into, after):
    n_dev = mlp_all.shape[0]
    def in_spec(arr):
        return pl.BlockSpec((1,) + arr.shape[1:], lambda dev: (dev, 0, 0))
    def rows(shape, at):
        return pl.BlockSpec((1, width // n_dev, shape[2]), lambda dev: (at, dev, 0))
    n_blk = hidden // FF_BLK
    shapes = [(2, width, hidden), (2, n_blk, n_dev, FF_BLK // n_dev, width), (2, width, width)]
    down = pl.BlockSpec((1, n_blk, 1, FF_BLK // n_dev, width), lambda dev: (layer, 0, dev, 0, 0))
    out_specs = [rows(shapes[0], layer), down, rows(shapes[2], layer)]
    if with_qkv:
        shapes.append((2, width, 3 * width))
        out_specs.append(rows(shapes[3], layer + 1))
    return pl.pallas_call(
        functools.partial(unpack_kernel, with_qkv, n_dev, len(shapes)),
        grid=(n_dev,),
        in_specs=[in_spec(mlp_all), in_spec(attn_all)] + [pl.BlockSpec(memory_space=pl.ANY)] * (len(into) + len(after)),
        out_specs=out_specs,
        out_shape=[jax.ShapeDtypeStruct(shape, jnp.float32) for shape in shapes],
        input_output_aliases={2 + i: i for i in range(len(into))},
        compiler_params=pltpu.CompilerParams(dimension_semantics=("arbitrary",), vmem_limit_bytes=VMEM_ALL),
        cost_estimate=cost(10, 40),
        name="unpack",
    )(mlp_all, attn_all, *into, *after)


def unpack_qkv_kernel(n_dev, last_ref, into_ref, out_ref):
    put_qkv(last_ref, 0, out_ref, 1.0 / n_dev)


def unpack_qkv(last_all, into):
    n_dev = last_all.shape[0]
    rows, cols = into.shape[1:]
    return pl.pallas_call(
        functools.partial(unpack_qkv_kernel, n_dev),
        grid=(n_dev,),
        in_specs=[pl.BlockSpec((1,) + last_all.shape[1:], lambda dev: (dev, 0, 0)), pl.BlockSpec(memory_space=pl.ANY)],
        out_specs=pl.BlockSpec((1, rows // n_dev, cols), lambda dev: (0, dev, 0)),
        out_shape=jax.ShapeDtypeStruct(into.shape, jnp.float32),
        input_output_aliases={1: 0},
        compiler_params=pltpu.CompilerParams(dimension_semantics=("arbitrary",), vmem_limit_bytes=VMEM_ALL),
        cost_estimate=cost(4, 20),
        name="unpack_qkv",
    )(last_all, into)


def solution(mesh):
    n_dev = mesh.shape['data']

    def local_step(x_loc, grad_y_loc, gain_one, gain_two, w_qkv, w_out, w_up, w_down):
        n_layers = w_qkv.shape[0]
        hidden_x = x_loc[0]
        saved_all = []
        for layer_idx in range(n_layers):
            hidden, act_lo, saved_vals = block_forward(hidden_x, gain_one[layer_idx], gain_two[layer_idx], w_qkv[layer_idx], w_out[layer_idx], w_up[layer_idx])
            saved_all.append(saved_vals)
            if layer_idx + 1 < n_layers:
                hidden_x = hidden + dot_lo(act_lo, w_down[layer_idx])
        grad_cur = grad_y_loc[0]
        width, hidden = w_up.shape[1:]
        gains = [None] * (2 * n_layers)
        ready, after, gathered = [], [], []
        for layer_idx in reversed(range(n_layers)):
            out = block_backward(grad_cur, saved_all[layer_idx], w_qkv[layer_idx], w_out[layer_idx], w_up, w_down, layer_idx, ready, after)
            grad_cur, gains[layer_idx], gains[n_layers + layer_idx], grad_qkv_w = out[:4]
            ready, after = grad_qkv_w, list(out[4:])
            gathered.append(after)
        (top_mlp, top_attn), (low_mlp, low_attn) = gathered
        gain_rows = jnp.concatenate([jnp.stack(gains), jnp.zeros((8 - 2 * n_layers, width), jnp.float32)])
        shard, gain_sums = tail_reduce(gain_rows, ready, [qkv_parts(0)], [low_mlp], 3 * n_layers, n_dev)
        last = unit_gather(shard)
        partial = unpack(top_mlp, top_attn, False, 1, width, hidden, [], [gain_sums])
        w_u, w_d, w_o, grad_qkv = unpack(low_mlp, low_attn, True, 0, width, hidden, partial, [])
        gain_sums = gain_sums / n_dev
        grad_qkv = unpack_qkv(last, grad_qkv)
        weights = (grad_qkv, w_o, w_u, w_d.reshape(n_layers, hidden, width))
        return (grad_cur[None], gain_sums[:n_layers], gain_sums[n_layers:2 * n_layers]) + weights

    batch_spec = P('data')
    full_spec = P()
    return jax.shard_map(local_step, mesh=mesh, in_specs=(batch_spec, batch_spec) + (full_spec,) * 6, out_specs=(batch_spec,) + (full_spec,) * 6, check_vma=False)
```

```python
import functools

import jax
import jax.numpy as jnp
from jax import lax
from jax.experimental import pallas as pl
from jax.experimental.pallas import tpu as pltpu
from jax.sharding import PartitionSpec as P

NORM_EPS = 1e-6
HEAD_DIM = 64
LANES = 128
Q_BLK = 256
EXP_SCALE = HEAD_DIM ** -0.5 * 1.4426950408889634
NEG = -1e30
MIB = 2 ** 20
VMEM_ALL = 67043328
MESH = pl.DeviceIdType.MESH


def cost(gflops, mbytes):
    return pl.CostEstimate(flops=gflops * 10 ** 9, bytes_accessed=mbytes * MIB, transcendentals=0)


def rms_gain(rows_f, gain_vec):
    return rows_f * lax.rsqrt(jnp.mean(rows_f * rows_f, axis=-1, keepdims=True) + NORM_EPS) * gain_vec


def gelu_tanh(pre_act):
    return jax.nn.gelu(pre_act, approximate=True)


def dot_lo(lhs, rhs):
    return jnp.dot(lhs, rhs, preferred_element_type=jnp.float32).astype(jnp.bfloat16)


def dot_nt(lhs, rhs):
    return lax.dot_general(lhs, rhs, (((1,), (1,)), ((), ())), preferred_element_type=jnp.float32)


def dot_tn(lhs, rhs):
    return lax.dot_general(lhs, rhs, (((0,), (0,)), ((), ())), preferred_element_type=jnp.float32)


def dot_nn(lhs, rhs):
    return jnp.dot(lhs, rhs, preferred_element_type=jnp.float32)


def head_mask(ref_rows, head):
    lane = lax.broadcasted_iota(jnp.int32, ref_rows.shape, 1)
    return jnp.where(lane // HEAD_DIM == head, ref_rows, jnp.zeros_like(ref_rows))


def scores_t(k_ref, q_m, q_start):
    diag = dot_nt(k_ref[q_start:q_start + Q_BLK, :], q_m)
    key_i = lax.broadcasted_iota(jnp.int32, diag.shape, 0)
    query_i = lax.broadcasted_iota(jnp.int32, diag.shape, 1)
    diag = jnp.where(key_i <= query_i, diag, NEG)
    if q_start == 0:
        return diag
    return jnp.concatenate([dot_nt(k_ref[:q_start, :], q_m), diag], axis=0)


def attn_fwd_kernel(q_ref, k_ref, v_ref, o_ref, lse_ref, vt_ref, ot_ref):
    seq = q_ref.shape[0]
    vt_ref[...] = v_ref[...].T
    for head in range(LANES // HEAD_DIM):
        rows = slice(head * HEAD_DIM, (head + 1) * HEAD_DIM)
        for q_start in range(0, seq, Q_BLK):
            q_end = q_start + Q_BLK
            q_m = head_mask(q_ref[q_start:q_end, :], head)
            s_t = scores_t(k_ref, q_m, q_start)
            top = jnp.max(s_t, axis=0, keepdims=True)
            p_t = jnp.exp2((s_t - top) * EXP_SCALE)
            total = jnp.sum(p_t, axis=0, keepdims=True)
            p_lo = (p_t * (1.0 / total)).astype(jnp.bfloat16)
            ot_ref[rows, q_start:q_end] = dot_nn(vt_ref[rows, :q_end], p_lo)
            lse_ref[0, head:head + 1, q_start:q_end] = top * EXP_SCALE + jnp.log2(total)
    o_ref[...] = ot_ref[...].T.astype(jnp.bfloat16)


N_COLOR = 3
UNIT_COLS = 256
FF_BLK = 256
MLP_ROWS = 96
ATTN_ROWS = 144
MLP_CHUNKS = 2
REST_BLKS = 6
REST_ROWS = 240
GELU_C = 0.7978845608028654
AXIS_BITS = (3, 2, 1)


class Reducer:
    def __init__(self, n_chunks, refs, grad_refs=(), parts=()):
        (self.own, self.send0, self.recv0, self.send1, self.recv1, self.send2, self.recv2, self.send3, self.recv3, self.load_sem, self.send_sem, self.recv_sem) = refs
        self.grad_refs, self.parts = grad_refs, parts
        self.n_chunks = n_chunks
        me = lax.axis_index('data')
        self.me = me
        self.bit = [lax.rem(lax.div(me, 1 << b), 2) for b in range(4)]
        self.partner = [me + (1 - 2 * self.bit[b]) * (1 << b) for b in range(4)]

    def barrier(self):
        sem = pltpu.get_barrier_semaphore()
        for dev in self.partner:
            pl.semaphore_signal(sem, inc=1, device_id=(dev,), device_id_type=MESH)
        pl.semaphore_wait(sem, 4)

    def load(self, chunk, half):
        for color in range(N_COLOR):
            for part, (array, kind, col, row, n_rows) in enumerate(self.parts[chunk][color]):
                if kind == 'block':
                    src = self.grad_refs[array].at[col, :, half]
                else:
                    src = self.grad_refs[array].at[:, half, :, pl.ds(col, UNIT_COLS)]
                dst = self.own.at[chunk, color, :, pl.ds(row, n_rows)]
                pltpu.make_async_copy(src, dst, self.load_sem.at[chunk, color, part]).start()

    def wait_load(self, chunk):
        for color in range(N_COLOR):
            for part, (_, _, _, row, n_rows) in enumerate(self.parts[chunk][color]):
                ref = self.own.at[chunk, color, :, pl.ds(row, n_rows)]
                pltpu.make_async_copy(ref, ref, self.load_sem.at[chunk, color, part]).wait()

    def copy(self, stage, chunk, color):
        send = (self.send0, self.send1, self.send2, self.send3)[stage].at[chunk, color]
        recv = (self.recv0, self.recv1, self.recv2, self.recv3)[stage].at[chunk, color]
        dev = self.partner[0] if stage == 0 else self.partner[self.order(color)[stage - 1]]
        return pltpu.make_async_remote_copy(src_ref=send, dst_ref=recv, send_sem=self.send_sem.at[stage, chunk, color], recv_sem=self.recv_sem.at[stage, chunk, color], device_id=(dev,), device_id_type=MESH)

    def order(self, color):
        return [1 + (color + step) % N_COLOR for step in range(N_COLOR)]

    def block(self, values):
        return values[3] * 4 + values[2] * 2 + values[1]

    def convert(self, chunk):
        self.wait_load(chunk)
        for color in range(N_COLOR):
            def body(i, carry):
                self.send0[chunk, color, i] = self.own[chunk, color, i].astype(jnp.bfloat16)
                return carry
            lax.fori_loop(0, 8, body, 0)
            self.copy(0, chunk, color).start()

    def total(self, chunk, color, values, n_recv):
        order = self.order(color)
        index = self.block(values)
        acc = self.own[chunk, color, index] + self.recv0[chunk, color, index].astype(jnp.float32)
        if n_recv >= 2:
            acc = acc + self.recv1[chunk, color, values[order[1]] * 2 + values[order[2]]].astype(jnp.float32)
        if n_recv >= 3:
            acc = acc + self.recv2[chunk, color, values[order[2]]].astype(jnp.float32)
        if n_recv >= 4:
            acc = acc + self.recv3[chunk, color, 0].astype(jnp.float32)
        return acc

    def stage(self, step, chunk):
        send = (None, self.send1, self.send2, self.send3)[step]
        n_free = N_COLOR - step
        for color in range(N_COLOR):
            self.copy(step - 1, chunk, color).wait_recv()
            order = self.order(color)

            def body(i, carry):
                values = [0, 0, 0, 0]
                for done in range(step - 1):
                    values[order[done]] = self.bit[order[done]]
                values[order[step - 1]] = 1 - self.bit[order[step - 1]]
                if n_free == 2:
                    values[order[1]], values[order[2]] = lax.div(i, 2), lax.rem(i, 2)
                elif n_free == 1:
                    values[order[2]] = i
                send[chunk, color, i] = self.total(chunk, color, values, step).astype(jnp.bfloat16)
                return carry
            if n_free:
                lax.fori_loop(0, 1 << n_free, body, 0)
            else:
                body(0, 0)
            self.copy(step, chunk, color).start()

    def finish(self, chunk, out_ref, base=0):
        n_rows = self.own.shape[3]
        for color in range(N_COLOR):
            self.copy(3, chunk, color).wait_recv()
            row = base + (chunk * N_COLOR + color) * n_rows
            out_ref[row:row + n_rows, :] = self.total(chunk, color, self.bit, 4).astype(jnp.bfloat16)
        for stage in range(4):
            for color in range(N_COLOR):
                self.copy(stage, chunk, color).wait_send()


def reducer_scratch(n_chunks, rows):
    def buf(blocks, dtype):
        return pltpu.VMEM((n_chunks, N_COLOR, blocks, rows, UNIT_COLS), dtype)
    lo = jnp.bfloat16
    return [buf(8, jnp.float32), buf(8, lo), buf(8, lo), buf(4, lo), buf(4, lo), buf(2, lo), buf(2, lo), buf(1, lo), buf(1, lo), pltpu.SemaphoreType.DMA((n_chunks, N_COLOR, N_COLOR)), pltpu.SemaphoreType.DMA((4, n_chunks, N_COLOR)), pltpu.SemaphoreType.DMA((4, n_chunks, N_COLOR))]


def grad_view(grad_w):
    rows, cols = grad_w.shape
    return grad_w.reshape(8, 2, rows // 16, cols)


def qkv_parts(array):
    return [[(array + color, 'cols', part * UNIT_COLS, part * 48, 48) for part in range(3)] for color in range(N_COLOR)]


def rest_parts(block_array, out_array):
    n_mlp = REST_BLKS // N_COLOR
    return [[(block_array, 'block', color + N_COLOR * i, i * MLP_ROWS, MLP_ROWS) for i in range(n_mlp)] + [(out_array, 'cols', color * UNIT_COLS, n_mlp * MLP_ROWS, 48)] for color in range(N_COLOR)]


def mlp_bwd_kernel(parts, n_grads, n_after, *refs):
    dy_ref, u_ref, z_ref, w1_ref, w2_ref = refs[:5]
    grad_refs = refs[5:5 + n_grads]
    refs = refs[5 + n_grads + n_after:]
    du_ref, block_ref, shard_ref, ut_ref, a_ref, dz_ref = refs[:6]
    n_red = (len(refs) - 6) // (2 if parts else 1)
    red = Reducer(MLP_CHUNKS, refs[6:6 + n_red])
    early = Reducer(len(parts), refs[6 + n_red:], grad_refs, parts) if parts else None
    step = pl.program_id(0)
    n_blk = dz_ref.shape[1] // FF_BLK
    core = red.bit[0]
    seq = dy_ref.shape[0]

    @pl.when(step == 0)
    def _():
        red.barrier()
        if early:
            early.load(0, 1 - core)
        ut_ref[...] = u_ref[...].T

    if early:
        @pl.when(step == 1)
        def _():
            early.convert(0)
            early.load(0, core)

        for stage, when in ((1, 3), (2, 7), (3, 10)):
            @pl.when(step == when)
            def _():
                if stage == 1:
                    early.wait_load(0)
                early.stage(stage, 0)

        @pl.when(step == n_blk)
        def _():
            early.finish(0, shard_ref, N_COLOR * MLP_CHUNKS * MLP_ROWS)

    second = 9 if early else 8
    for when, stage, chunk in ((4, 1, 0), (second, 2, 0), (7, 1, 1), (12, 3, 0), (second + 3, 2, 1), (14, 3, 1)):
        @pl.when(step == when)
        def _():
            red.stage(stage, chunk)

    @pl.when(step < n_blk)
    def _():
        cols = pl.ds(pl.multiple_of(step * FF_BLK, FF_BLK), FF_BLK)
        for row in range(0, seq, 256):
            rows = slice(row, row + 256)
            da = dot_nt(dy_ref[rows, :], w2_ref[0]).astype(jnp.bfloat16).astype(jnp.float32)
            z = z_ref[rows, :].astype(jnp.float32)
            z_sq = z * z
            th = jnp.tanh(z * (GELU_C + (GELU_C * 0.044715) * z_sq))
            cdf = 0.5 + 0.5 * th
            a_ref[rows, :] = (z * cdf).astype(jnp.bfloat16)
            slope = cdf + (0.5 * z) * (1.0 - th * th) * (GELU_C + (3.0 * GELU_C * 0.044715) * z_sq)
            dz_ref[rows, cols] = (slope * da).astype(jnp.bfloat16)
        dw1 = dot_nn(ut_ref[...], dz_ref[:, cols])
        block_ref[0, :, :, 0:48, :] = dw1.reshape(8, 2, 48, UNIT_COLS)
        dw2 = dot_nn(a_ref[...].T, dy_ref[...])
        for part in range(3):
            block_ref[0, :, :, 48 + 16 * part:64 + 16 * part, :] = dw2[:, part * UNIT_COLS:(part + 1) * UNIT_COLS].reshape(8, 2, 16, UNIT_COLS)

    @pl.when(step < N_COLOR * MLP_CHUNKS)
    def _():
        chunk, color = lax.div(step, N_COLOR), lax.rem(step, N_COLOR)

        def body(i, carry):
            red.own[chunk, color, i] = block_ref[0, i, core]
            red.send0[chunk, color, i] = block_ref[0, i, 1 - core].astype(jnp.bfloat16)
            return carry
        lax.fori_loop(0, 8, body, 0)
        red.copy(0, chunk, color).start()

    @pl.when(step >= n_blk)
    def _():
        du_ref[...] = dot_nt(dz_ref[...], w1_ref[0]).astype(jnp.bfloat16)

    @pl.when(step == pl.num_programs(0) - 1)
    def _():
        for chunk in range(MLP_CHUNKS):
            red.finish(chunk, shard_ref)


def mlp_backward(dy, u_two, z_lo, w_up, w_down, layer, grads, after, call_id):
    seq, width = dy.shape
    n_blk = w_up.shape[2] // FF_BLK
    n_last = width // 256
    last = n_blk - REST_BLKS
    whole = pl.BlockSpec((seq, width), lambda step: (0, 0))
    parts = [qkv_parts(0)] if grads else []
    shard_shape = (N_COLOR * (MLP_CHUNKS * MLP_ROWS + len(parts) * ATTN_ROWS), UNIT_COLS)
    return pl.pallas_call(
        functools.partial(mlp_bwd_kernel, parts, len(grads), len(after)),
        grid=(n_blk + n_last,),
        in_specs=[
            whole, whole,
            pl.BlockSpec((seq, FF_BLK), lambda step: (0, jnp.minimum(step, n_blk - 1))),
            pl.BlockSpec((1, 256, w_up.shape[2]), lambda step: (layer, jnp.maximum(step - n_blk, 0), 0)),
            pl.BlockSpec((1, FF_BLK, width), lambda step: (layer, jnp.minimum(step, n_blk - 1), 0)),
        ] + [pl.BlockSpec(memory_space=pl.ANY)] * (len(grads) + len(after)),
        out_specs=[
            pl.BlockSpec((seq, 256), lambda step: (0, jnp.maximum(step - n_blk, 0))),
            pl.BlockSpec((1, 8, 2, MLP_ROWS, UNIT_COLS), lambda step: (jnp.clip(step - last, 0, REST_BLKS - 1), 0, 0, 0, 0)),
            pl.BlockSpec(shard_shape, lambda step: (0, 0)),
        ],
        out_shape=[jax.ShapeDtypeStruct((seq, width), jnp.bfloat16), jax.ShapeDtypeStruct((REST_BLKS, 8, 2, MLP_ROWS, UNIT_COLS), jnp.float32), jax.ShapeDtypeStruct(shard_shape, jnp.bfloat16)],
        scratch_shapes=[pltpu.VMEM((width, seq), jnp.bfloat16), pltpu.VMEM((seq, FF_BLK), jnp.bfloat16), pltpu.VMEM((seq, w_up.shape[2]), jnp.bfloat16)] + reducer_scratch(MLP_CHUNKS, MLP_ROWS) + (reducer_scratch(1, ATTN_ROWS) if parts else []),
        compiler_params=pltpu.CompilerParams(dimension_semantics=("arbitrary",), vmem_limit_bytes=VMEM_ALL, collective_id=call_id),
        cost_estimate=cost(30, 30),
        name="mlp_bwd",
    )(dy, u_two, z_lo, w_up, w_down, *grads, *after)


def attn_bwd_kernel(parts, n_grads, n_after, *refs):
    q_ref, k_ref, v_ref, do_ref, lse_ref, u_ref = refs[:6]
    grad_refs = refs[6:6 + n_grads]
    refs = refs[6 + n_grads + n_after:]
    dq_ref, dk_ref, dv_ref, dwq_ref, dwk_ref, dwv_ref, shard_ref, ut_ref, kt_ref, dqt_ref, dk_acc, dv_acc = refs[:12]
    red = Reducer(len(parts), refs[12:], grad_refs, parts)
    n_chunks = red.n_chunks
    pair = pl.program_id(0)
    seq = q_ref.shape[0]
    events = {}
    for chunk in range(n_chunks):
        for stage, when in ((1, 2), (2, 6), (3, 9)):
            events[when] = [(stage, chunk)]

    @pl.when(pair == 0)
    def _():
        red.barrier()
        for chunk in range(n_chunks):
            red.load(chunk, 1 - red.bit[0])
        for chunk in range(n_chunks):
            red.convert(chunk)
            red.load(chunk, red.bit[0])
        ut_ref[...] = u_ref[...].T

    kt_ref[...] = k_ref[...].T
    for head in range(LANES // HEAD_DIM):
        for when, todo in events.items():
            if when % 2 == head:
                @pl.when(pair == when // 2)
                def _():
                    for stage, chunk in todo:
                        if stage == 1:
                            red.wait_load(chunk)
                        red.stage(stage, chunk)
        rows = slice(head * HEAD_DIM, (head + 1) * HEAD_DIM)
        for q_start in range(0, seq, Q_BLK):
            q_end = q_start + Q_BLK
            q_m = head_mask(q_ref[q_start:q_end, :], head)
            do_m = head_mask(do_ref[q_start:q_end, :], head)
            s_t = scores_t(k_ref, q_m, q_start)
            p_t = jnp.exp2(s_t * EXP_SCALE - lse_ref[0, head:head + 1, q_start:q_end])
            dp_t = dot_nt(v_ref[:q_end, :], do_m)
            delta = jnp.sum(p_t * dp_t, axis=0, keepdims=True)
            ds_t = (p_t * (dp_t - delta) * HEAD_DIM ** -0.5).astype(jnp.bfloat16)
            dv_part = dot_nn(p_t.astype(jnp.bfloat16), do_m)
            dk_part = dot_nn(ds_t, q_m)
            if head == 0 and q_start == 0:
                dv_acc[...] = jnp.zeros_like(dv_acc)
                dk_acc[...] = jnp.zeros_like(dk_acc)
            dv_acc[:q_end, :] += dv_part
            dk_acc[:q_end, :] += dk_part
            dqt_ref[rows, q_start:q_end] = dot_nn(kt_ref[rows, :q_end], ds_t)
    dq_ref[...] = dqt_ref[...].T.astype(jnp.bfloat16)
    dk_ref[...] = dk_acc[...].astype(jnp.bfloat16)
    dv_ref[...] = dv_acc[...].astype(jnp.bfloat16)
    d_w = dot_nn(ut_ref[...], jnp.concatenate([dq_ref[...], dk_ref[...], dv_ref[...]], axis=1))
    for out_ref, at in ((dwq_ref, 0), (dwk_ref, LANES), (dwv_ref, 2 * LANES)):
        out_ref[...] = d_w[:, at:at + LANES].reshape(out_ref.shape)

    @pl.when(pair == pl.num_programs(0) - 1)
    def _():
        for chunk in range(n_chunks):
            red.finish(chunk, shard_ref)


def tail_kernel(parts, n_grads, n_after, *refs):
    gains_ref = refs[0]
    grad_refs = refs[1:1 + n_grads]
    refs = refs[:1 + n_grads] + refs[1 + n_grads + n_after:]
    shard_ref, gsum_ref, gbuf, gsend_sem, grecv_sem = refs[1 + n_grads:6 + n_grads]
    red = Reducer(len(parts), refs[6 + n_grads:], grad_refs, parts)
    n_dev = gbuf.shape[0]
    for chunk in range(red.n_chunks):
        red.load(chunk, 1 - red.bit[0])
    sem = pltpu.get_barrier_semaphore()
    for shift in range(1, n_dev):
        pl.semaphore_signal(sem, inc=1, device_id=(lax.rem(red.me + shift, n_dev),), device_id_type=MESH)
    pl.semaphore_wait(sem, n_dev - 1)

    def gain_copy(shift):
        dev = lax.rem(red.me + shift, n_dev)
        return pltpu.make_async_remote_copy(src_ref=gains_ref, dst_ref=gbuf.at[shift], send_sem=gsend_sem.at[shift], recv_sem=grecv_sem.at[shift], device_id=(dev,), device_id_type=MESH)
    for shift in range(1, n_dev):
        gain_copy(shift).start()
    gbuf[0] = gains_ref[...]
    for chunk in range(red.n_chunks):
        red.convert(chunk)
        red.load(chunk, red.bit[0])
    for step in range(1, 4):
        for chunk in range(red.n_chunks):
            if step == 1:
                red.wait_load(chunk)
            red.stage(step, chunk)
    for shift in range(1, n_dev):
        gain_copy(shift).wait()
    acc = jnp.zeros(gains_ref.shape, jnp.float32)
    for dev in range(n_dev):
        acc = acc + gbuf[lax.rem(red.me + n_dev - dev, n_dev)]
    gsum_ref[...] = acc
    for chunk in range(red.n_chunks):
        red.finish(chunk, shard_ref)


def attn_specs(seq, n_pairs):
    def col(shift):
        return pl.BlockSpec((seq, LANES), lambda pair: (0, pair + shift))
    lse = pl.BlockSpec((1, 8, seq), lambda pair: (pair, 0, 0))
    return col, lse


def attn_forward(qkv):
    seq, width = qkv.shape[0], qkv.shape[1] // 3
    n_pairs = width // LANES
    col, lse = attn_specs(seq, n_pairs)
    return pl.pallas_call(
        attn_fwd_kernel,
        grid=(n_pairs,),
        in_specs=[col(0), col(n_pairs), col(2 * n_pairs)],
        out_specs=[col(0), lse],
        out_shape=[jax.ShapeDtypeStruct((seq, width), jnp.bfloat16), jax.ShapeDtypeStruct((n_pairs, 8, seq), jnp.float32)],
        scratch_shapes=[pltpu.VMEM((LANES, seq), jnp.bfloat16), pltpu.VMEM((LANES, seq), jnp.float32)],
        compiler_params=pltpu.CompilerParams(dimension_semantics=("arbitrary",), vmem_limit_bytes=48 * MIB),
        cost_estimate=cost(16, 8),
        name="attn_fwd",
    )(qkv, qkv, qkv)


def attn_backward(qkv, d_out, lse_vals, u_one, grads, parts, after, call_id):
    seq, width = qkv.shape[0], qkv.shape[1] // 3
    n_pairs = width // LANES
    col, lse = attn_specs(seq, n_pairs)
    shape = jax.ShapeDtypeStruct((seq, width), jnp.bfloat16)
    shard_shape = (len(parts) * N_COLOR * REST_ROWS, UNIT_COLS)
    d_w = pl.BlockSpec((8, 2, width // 16, LANES), lambda pair: (0, 0, 0, pair))
    out = pl.pallas_call(
        functools.partial(attn_bwd_kernel, parts, len(grads), len(after)),
        grid=(n_pairs,),
        in_specs=[col(0), col(n_pairs), col(2 * n_pairs), col(0), lse, pl.BlockSpec((seq, width), lambda pair: (0, 0))] + [pl.BlockSpec(memory_space=pl.ANY)] * (len(grads) + len(after)),
        out_specs=[col(0), col(0), col(0), d_w, d_w, d_w, pl.BlockSpec(shard_shape, lambda pair: (0, 0))],
        out_shape=[shape, shape, shape] + [pltpu.HBM((8, 2, width // 16, width), jnp.float32)] * 3 + [jax.ShapeDtypeStruct(shard_shape, jnp.bfloat16)],
        scratch_shapes=[pltpu.VMEM((width, seq), jnp.bfloat16), pltpu.VMEM((LANES, seq), jnp.bfloat16), pltpu.VMEM((LANES, seq), jnp.float32), pltpu.VMEM((seq, LANES), jnp.float32), pltpu.VMEM((seq, LANES), jnp.float32)] + reducer_scratch(len(parts), REST_ROWS),
        compiler_params=pltpu.CompilerParams(dimension_semantics=("arbitrary",), vmem_limit_bytes=VMEM_ALL, collective_id=call_id),
        cost_estimate=cost(40, 14),
        name="attn_bwd",
    )(qkv, qkv, qkv, d_out, lse_vals, u_one, *grads, *after)
    return out[:3], list(out[3:6]), out[6]


def tail_reduce(gains, grads, parts, after, call_id, n_dev):
    n_chunks = len(parts)
    shard_shape = (n_chunks * N_COLOR * ATTN_ROWS, UNIT_COLS)
    return pl.pallas_call(
        functools.partial(tail_kernel, parts, len(grads), len(after)),
        in_specs=[pl.BlockSpec(memory_space=pltpu.VMEM)] + [pl.BlockSpec(memory_space=pl.ANY)] * (len(grads) + len(after)),
        out_specs=[pl.BlockSpec(memory_space=pltpu.VMEM)] * 2,
        out_shape=[jax.ShapeDtypeStruct(shard_shape, jnp.bfloat16), jax.ShapeDtypeStruct(gains.shape, jnp.float32)],
        scratch_shapes=[pltpu.VMEM((n_dev,) + gains.shape, jnp.float32), pltpu.SemaphoreType.DMA((n_dev,)), pltpu.SemaphoreType.DMA((n_dev,))] + reducer_scratch(n_chunks, ATTN_ROWS),
        compiler_params=pltpu.CompilerParams(vmem_limit_bytes=40 * MIB, collective_id=call_id),
        cost_estimate=cost(20, 14),
        name="tail_reduce",
    )(gains, *grads, *after)


def block_forward(x_blk, gain_a, gain_b, w_qkv, w_out, w_up):
    norm_a, norm_a_back = jax.vjp(rms_gain, x_blk.astype(jnp.float32), gain_a)
    u_one = norm_a.astype(jnp.bfloat16)
    qkv = dot_lo(u_one, w_qkv)
    attn_out, lse_vals = attn_forward(qkv)
    hidden = x_blk + dot_lo(attn_out, w_out)
    norm_b, norm_b_back = jax.vjp(rms_gain, hidden.astype(jnp.float32), gain_b)
    u_two = norm_b.astype(jnp.bfloat16)
    pre_lo = dot_lo(u_two, w_up)
    act_lo = gelu_tanh(pre_lo.astype(jnp.float32)).astype(jnp.bfloat16)
    return hidden, act_lo, (norm_a_back, u_one, qkv, lse_vals, attn_out, norm_b_back, u_two, pre_lo)


def block_backward(grad_blk, saved_vals, w_qkv, w_out, w_up, w_down, layer, ready, after):
    (norm_a_back, u_one, qkv, lse_vals, attn_out, norm_b_back, u_two, pre_lo) = saved_vals
    ids = len(ready)
    grad_u_two, block, shard_mlp = mlp_backward(grad_blk, u_two, pre_lo, w_up, w_down, layer, ready, after[:1], ids)
    grad_h_norm, grad_gain_b = norm_b_back(grad_u_two.astype(jnp.float32))
    grad_hidden = (grad_blk.astype(jnp.float32) + grad_h_norm).astype(jnp.bfloat16)
    grad_out_w = dot_tn(attn_out, grad_hidden)
    grad_attn = dot_nt(grad_hidden, w_out).astype(jnp.bfloat16)
    grads = [block, grad_view(grad_out_w)]
    parts = [rest_parts(0, 1)]
    pieces, grad_qkv_w, shard_attn = attn_backward(qkv, grad_attn, lse_vals, u_one, grads, parts, after[1:], ids + 1)
    grad_qkv = jnp.concatenate(pieces, axis=1)
    grad_u_one = dot_nt(grad_qkv, w_qkv).astype(jnp.bfloat16)
    grad_x_norm, grad_gain_a = norm_a_back(grad_u_one.astype(jnp.float32))
    grad_x_blk = (grad_hidden.astype(jnp.float32) + grad_x_norm).astype(jnp.bfloat16)
    return grad_x_blk, grad_gain_a, grad_gain_b, grad_qkv_w, unit_gather(shard_mlp), unit_gather(shard_attn)


def unit_gather(shard):
    return lax.all_gather(shard, 'data', axis=0, tiled=True).reshape((-1,) + shard.shape)


def put_qkv(unit_ref, base, out_ref, scale):
    for color in range(N_COLOR):
        for part in range(3):
            cols = slice((color * 3 + part) * UNIT_COLS, (color * 3 + part + 1) * UNIT_COLS)
            row = base + color * ATTN_ROWS + part * 48
            out_ref[0, :, cols] = unit_ref[0, row:row + 48, :].astype(jnp.float32) * scale


def unpack_kernel(with_qkv, n_dev, n_out, *refs):
    mlp_ref, attn_ref = refs[:2]
    up_ref, down_ref, out_ref = refs[-n_out:][:3]
    scale = 1.0 / n_dev
    n_mlp = N_COLOR * MLP_CHUNKS

    def value(unit):
        return unit.astype(jnp.float32) * scale
    for blk in range(n_mlp + REST_BLKS):
        rest, color = (blk - n_mlp) // N_COLOR, (blk - n_mlp) % N_COLOR
        ref, row = (mlp_ref, blk * MLP_ROWS) if blk < n_mlp else (attn_ref, color * REST_ROWS + rest * MLP_ROWS)
        up_ref[0, :, blk * FF_BLK:(blk + 1) * FF_BLK] = value(ref[0, row:row + 48, :])
        for part in range(3):
            at = row + 48 + 16 * part
            down_ref[0, blk, 0, :, part * UNIT_COLS:(part + 1) * UNIT_COLS] = value(ref[0, at:at + 16, :])
    for color in range(N_COLOR):
        row = (color + 1) * REST_ROWS - 48
        out_ref[0, :, color * UNIT_COLS:(color + 1) * UNIT_COLS] = value(attn_ref[0, row:row + 48, :])
    if with_qkv:
        put_qkv(mlp_ref, n_mlp * MLP_ROWS, refs[-1], scale)


def unpack(mlp_all, attn_all, with_qkv, layer, width, hidden, into, after):
    n_dev = mlp_all.shape[0]
    def in_spec(arr):
        return pl.BlockSpec((1,) + arr.shape[1:], lambda dev: (dev, 0, 0))
    def rows(shape, at):
        return pl.BlockSpec((1, width // n_dev, shape[2]), lambda dev: (at, dev, 0))
    n_blk = hidden // FF_BLK
    shapes = [(2, width, hidden), (2, n_blk, n_dev, FF_BLK // n_dev, width), (2, width, width)]
    down = pl.BlockSpec((1, n_blk, 1, FF_BLK // n_dev, width), lambda dev: (layer, 0, dev, 0, 0))
    out_specs = [rows(shapes[0], layer), down, rows(shapes[2], layer)]
    if with_qkv:
        shapes.append((2, width, 3 * width))
        out_specs.append(rows(shapes[3], layer + 1))
    return pl.pallas_call(
        functools.partial(unpack_kernel, with_qkv, n_dev, len(shapes)),
        grid=(n_dev,),
        in_specs=[in_spec(mlp_all), in_spec(attn_all)] + [pl.BlockSpec(memory_space=pl.ANY)] * (len(into) + len(after)),
        out_specs=out_specs,
        out_shape=[jax.ShapeDtypeStruct(shape, jnp.float32) for shape in shapes],
        input_output_aliases={2 + i: i for i in range(len(into))},
        compiler_params=pltpu.CompilerParams(dimension_semantics=("arbitrary",), vmem_limit_bytes=VMEM_ALL),
        cost_estimate=cost(10, 40),
        name="unpack",
    )(mlp_all, attn_all, *into, *after)


def unpack_qkv_kernel(n_dev, last_ref, into_ref, out_ref):
    put_qkv(last_ref, 0, out_ref, 1.0 / n_dev)


def unpack_qkv(last_all, into):
    n_dev = last_all.shape[0]
    rows, cols = into.shape[1:]
    return pl.pallas_call(
        functools.partial(unpack_qkv_kernel, n_dev),
        grid=(n_dev,),
        in_specs=[pl.BlockSpec((1,) + last_all.shape[1:], lambda dev: (dev, 0, 0)), pl.BlockSpec(memory_space=pl.ANY)],
        out_specs=pl.BlockSpec((1, rows // n_dev, cols), lambda dev: (0, dev, 0)),
        out_shape=jax.ShapeDtypeStruct(into.shape, jnp.float32),
        input_output_aliases={1: 0},
        compiler_params=pltpu.CompilerParams(dimension_semantics=("arbitrary",), vmem_limit_bytes=VMEM_ALL),
        cost_estimate=cost(4, 20),
        name="unpack_qkv",
    )(last_all, into)


def solution(mesh):
    n_dev = mesh.shape['data']

    def local_step(x_loc, grad_y_loc, gain_one, gain_two, w_qkv, w_out, w_up, w_down):
        n_layers = w_qkv.shape[0]
        hidden_x = x_loc[0]
        saved_all = []
        for layer_idx in range(n_layers):
            hidden, act_lo, saved_vals = block_forward(hidden_x, gain_one[layer_idx], gain_two[layer_idx], w_qkv[layer_idx], w_out[layer_idx], w_up[layer_idx])
            saved_all.append(saved_vals)
            if layer_idx + 1 < n_layers:
                hidden_x = hidden + dot_lo(act_lo, w_down[layer_idx])
        grad_cur = grad_y_loc[0]
        width, hidden = w_up.shape[1:]
        gains = [None] * (2 * n_layers)
        ready, after, gathered = [], [], []
        for layer_idx in reversed(range(n_layers)):
            out = block_backward(grad_cur, saved_all[layer_idx], w_qkv[layer_idx], w_out[layer_idx], w_up, w_down, layer_idx, ready, after)
            grad_cur, gains[layer_idx], gains[n_layers + layer_idx], grad_qkv_w = out[:4]
            ready, after = grad_qkv_w, list(out[4:])
            gathered.append(after)
        (top_mlp, top_attn), (low_mlp, low_attn) = gathered
        gain_rows = jnp.concatenate([jnp.stack(gains), jnp.zeros((8 - 2 * n_layers, width), jnp.float32)])
        shard, gain_sums = tail_reduce(gain_rows, ready, [qkv_parts(0)], [low_mlp], 3 * n_layers, n_dev)
        last = unit_gather(shard)
        partial = unpack(top_mlp, top_attn, False, 1, width, hidden, [], [gain_sums])
        w_u, w_d, w_o, grad_qkv = unpack(low_mlp, low_attn, True, 0, width, hidden, partial, [])
        gain_sums = gain_sums / n_dev
        grad_qkv = unpack_qkv(last, grad_qkv)
        weights = (grad_qkv, w_o, w_u, w_d.reshape(n_layers, hidden, width))
        return (grad_cur[None], gain_sums[:n_layers], gain_sums[n_layers:2 * n_layers]) + weights

    batch_spec = P('data')
    full_spec = P()
    return jax.shard_map(local_step, mesh=mesh, in_specs=(batch_spec, batch_spec) + (full_spec,) * 6, out_specs=(batch_spec,) + (full_spec,) * 6, check_vma=False)
```

```python
import functools

import jax
import jax.numpy as jnp
from jax import lax
from jax.experimental import pallas as pl
from jax.experimental.pallas import tpu as pltpu
from jax.sharding import PartitionSpec as P

NORM_EPS = 1e-6
HEAD_DIM = 64
LANES = 128
Q_BLK = 256
EXP_SCALE = HEAD_DIM ** -0.5 * 1.4426950408889634
NEG = -1e30
MIB = 2 ** 20
VMEM_ALL = 67043328
MESH = pl.DeviceIdType.MESH


def cost(gflops, mbytes):
    return pl.CostEstimate(flops=gflops * 10 ** 9, bytes_accessed=mbytes * MIB, transcendentals=0)


def rms_gain(rows_f, gain_vec):
    return rows_f * lax.rsqrt(jnp.mean(rows_f * rows_f, axis=-1, keepdims=True) + NORM_EPS) * gain_vec


def gelu_tanh(pre_act):
    return jax.nn.gelu(pre_act, approximate=True)


def dot_lo(lhs, rhs):
    return jnp.dot(lhs, rhs, preferred_element_type=jnp.float32).astype(jnp.bfloat16)


def dot_nt(lhs, rhs):
    return lax.dot_general(lhs, rhs, (((1,), (1,)), ((), ())), preferred_element_type=jnp.float32)


def dot_tn(lhs, rhs):
    return lax.dot_general(lhs, rhs, (((0,), (0,)), ((), ())), preferred_element_type=jnp.float32)


def dot_nn(lhs, rhs):
    return jnp.dot(lhs, rhs, preferred_element_type=jnp.float32)


def head_mask(ref_rows, head):
    lane = lax.broadcasted_iota(jnp.int32, ref_rows.shape, 1)
    return jnp.where(lane // HEAD_DIM == head, ref_rows, jnp.zeros_like(ref_rows))


def scores_t(k_ref, q_m, q_start):
    diag = dot_nt(k_ref[q_start:q_start + Q_BLK, :], q_m)
    key_i = lax.broadcasted_iota(jnp.int32, diag.shape, 0)
    query_i = lax.broadcasted_iota(jnp.int32, diag.shape, 1)
    diag = jnp.where(key_i <= query_i, diag, NEG)
    if q_start == 0:
        return diag
    return jnp.concatenate([dot_nt(k_ref[:q_start, :], q_m), diag], axis=0)


def attn_fwd_kernel(q_ref, k_ref, v_ref, o_ref, lse_ref, vt_ref, ot_ref):
    seq = q_ref.shape[0]
    vt_ref[...] = v_ref[...].T
    for head in range(LANES // HEAD_DIM):
        rows = slice(head * HEAD_DIM, (head + 1) * HEAD_DIM)
        for q_start in range(0, seq, Q_BLK):
            q_end = q_start + Q_BLK
            q_m = head_mask(q_ref[q_start:q_end, :], head)
            s_t = scores_t(k_ref, q_m, q_start)
            top = jnp.max(s_t, axis=0, keepdims=True)
            p_t = jnp.exp2((s_t - top) * EXP_SCALE)
            total = jnp.sum(p_t, axis=0, keepdims=True)
            p_lo = (p_t * (1.0 / total)).astype(jnp.bfloat16)
            ot_ref[rows, q_start:q_end] = dot_nn(vt_ref[rows, :q_end], p_lo)
            lse_ref[0, head:head + 1, q_start:q_end] = top * EXP_SCALE + jnp.log2(total)
    o_ref[...] = ot_ref[...].T.astype(jnp.bfloat16)


N_COLOR = 3
UNIT_COLS = 256
FF_BLK = 256
MLP_ROWS = 96
ATTN_ROWS = 144
MLP_CHUNKS = 3
DEV_BLK = 2
GELU_C = 0.7978845608028654
AXIS_BITS = (3, 2, 1)


class Reducer:
    def __init__(self, n_chunks, refs, grad_refs=(), parts=()):
        (self.own, self.send0, self.recv0, self.send1, self.recv1, self.send2, self.recv2, self.send3, self.recv3, self.load_sem, self.send_sem, self.recv_sem) = refs
        self.grad_refs, self.parts = grad_refs, parts
        self.n_chunks = n_chunks
        me = lax.axis_index('data')
        self.me = me
        self.bit = [lax.rem(lax.div(me, 1 << b), 2) for b in range(4)]
        self.partner = [me + (1 - 2 * self.bit[b]) * (1 << b) for b in range(4)]

    def barrier(self):
        sem = pltpu.get_barrier_semaphore()
        for dev in self.partner:
            pl.semaphore_signal(sem, inc=1, device_id=(dev,), device_id_type=MESH)
        pl.semaphore_wait(sem, 4)

    def load(self, chunk, half):
        for color in range(N_COLOR):
            for part, (array, kind, col, row, n_rows) in enumerate(self.parts[chunk][color]):
                if kind == 'block':
                    src = self.grad_refs[array].at[col, :, half]
                else:
                    src = self.grad_refs[array].at[:, half, :, pl.ds(col, UNIT_COLS)]
                dst = self.own.at[chunk, color, :, pl.ds(row, n_rows)]
                pltpu.make_async_copy(src, dst, self.load_sem.at[chunk, color, part]).start()

    def wait_load(self, chunk):
        for color in range(N_COLOR):
            for part, (_, _, _, row, n_rows) in enumerate(self.parts[chunk][color]):
                ref = self.own.at[chunk, color, :, pl.ds(row, n_rows)]
                pltpu.make_async_copy(ref, ref, self.load_sem.at[chunk, color, part]).wait()

    def copy(self, stage, chunk, color):
        send = (self.send0, self.send1, self.send2, self.send3)[stage].at[chunk, color]
        recv = (self.recv0, self.recv1, self.recv2, self.recv3)[stage].at[chunk, color]
        dev = self.partner[0] if stage == 0 else self.partner[self.order(color)[stage - 1]]
        return pltpu.make_async_remote_copy(src_ref=send, dst_ref=recv, send_sem=self.send_sem.at[stage, chunk, color], recv_sem=self.recv_sem.at[stage, chunk, color], device_id=(dev,), device_id_type=MESH)

    def order(self, color):
        return [1 + (color + step) % N_COLOR for step in range(N_COLOR)]

    def block(self, values):
        return values[3] * 4 + values[2] * 2 + values[1]

    def convert(self, chunk):
        self.wait_load(chunk)
        for color in range(N_COLOR):
            def body(i, carry):
                self.send0[chunk, color, i] = self.own[chunk, color, i].astype(jnp.bfloat16)
                return carry
            lax.fori_loop(0, 8, body, 0)
            self.copy(0, chunk, color).start()

    def total(self, chunk, color, values, n_recv):
        order = self.order(color)
        index = self.block(values)
        acc = self.own[chunk, color, index] + self.recv0[chunk, color, index].astype(jnp.float32)
        if n_recv >= 2:
            acc = acc + self.recv1[chunk, color, values[order[1]] * 2 + values[order[2]]].astype(jnp.float32)
        if n_recv >= 3:
            acc = acc + self.recv2[chunk, color, values[order[2]]].astype(jnp.float32)
        if n_recv >= 4:
            acc = acc + self.recv3[chunk, color, 0].astype(jnp.float32)
        return acc

    def stage(self, step, chunk):
        send = (None, self.send1, self.send2, self.send3)[step]
        n_free = N_COLOR - step
        for color in range(N_COLOR):
            self.copy(step - 1, chunk, color).wait_recv()
            order = self.order(color)

            def body(i, carry):
                values = [0, 0, 0, 0]
                for done in range(step - 1):
                    values[order[done]] = self.bit[order[done]]
                values[order[step - 1]] = 1 - self.bit[order[step - 1]]
                if n_free == 2:
                    values[order[1]], values[order[2]] = lax.div(i, 2), lax.rem(i, 2)
                elif n_free == 1:
                    values[order[2]] = i
                send[chunk, color, i] = self.total(chunk, color, values, step).astype(jnp.bfloat16)
                return carry
            if n_free:
                lax.fori_loop(0, 1 << n_free, body, 0)
            else:
                body(0, 0)
            self.copy(step, chunk, color).start()

    def finish(self, chunk, out_ref, base=0):
        n_rows = self.own.shape[3]
        for color in range(N_COLOR):
            self.copy(3, chunk, color).wait_recv()
            row = base + (chunk * N_COLOR + color) * n_rows
            out_ref[row:row + n_rows, :] = self.total(chunk, color, self.bit, 4).astype(jnp.bfloat16)
        for stage in range(4):
            for color in range(N_COLOR):
                self.copy(stage, chunk, color).wait_send()


def reducer_scratch(n_chunks, rows):
    def buf(blocks, dtype):
        return pltpu.VMEM((n_chunks, N_COLOR, blocks, rows, UNIT_COLS), dtype)
    lo = jnp.bfloat16
    return [buf(8, jnp.float32), buf(8, lo), buf(8, lo), buf(4, lo), buf(4, lo), buf(2, lo), buf(2, lo), buf(1, lo), buf(1, lo), pltpu.SemaphoreType.DMA((n_chunks, N_COLOR, N_COLOR)), pltpu.SemaphoreType.DMA((4, n_chunks, N_COLOR)), pltpu.SemaphoreType.DMA((4, n_chunks, N_COLOR))]


def grad_view(grad_w):
    rows, cols = grad_w.shape
    return grad_w.reshape(8, 2, rows // 16, cols)


def qkv_parts(array):
    return [[(array + color, 'cols', part * UNIT_COLS, part * 48, 48) for part in range(3)] for color in range(N_COLOR)]


def rest_parts(block_array, out_array):
    return [[(block_array, 'block', color, 0, MLP_ROWS), (out_array, 'cols', color * UNIT_COLS, MLP_ROWS, 48)] for color in range(N_COLOR)]


def mlp_bwd_kernel(parts, n_grads, n_after, *refs):
    dy_ref, u_ref, z_ref, w1_ref, w2_ref = refs[:5]
    grad_refs = refs[5:5 + n_grads]
    refs = refs[5 + n_grads + n_after:]
    du_ref, block_ref, shard_ref, ut_ref, a_ref, dz_ref = refs[:6]
    n_red = (len(refs) - 6) // (2 if parts else 1)
    red = Reducer(MLP_CHUNKS, refs[6:6 + n_red])
    early = Reducer(len(parts), refs[6 + n_red:], grad_refs, parts) if parts else None
    step = pl.program_id(0)
    n_blk = dz_ref.shape[1] // FF_BLK
    core = red.bit[0]
    seq = dy_ref.shape[0]

    @pl.when(step == 0)
    def _():
        red.barrier()
        if early:
            early.load(0, 1 - core)
        ut_ref[...] = u_ref[...].T

    if early:
        @pl.when(step == 1)
        def _():
            early.convert(0)
            early.load(0, core)

        for stage, when in ((1, 2), (2, 5), (3, 7)):
            @pl.when(step == when)
            def _():
                if stage == 1:
                    early.wait_load(0)
                early.stage(stage, 0)

        @pl.when(step == n_blk - 1)
        def _():
            early.finish(0, shard_ref, N_COLOR * MLP_CHUNKS * MLP_ROWS)

    for stage, first, count in ((3, 9, MLP_CHUNKS - 1), (2, 7, MLP_CHUNKS), (1, 4, MLP_CHUNKS)):
        @pl.when((step >= first) & (step < first + N_COLOR * count) & (lax.rem(step + 2 * first, N_COLOR) == 0))
        def _():
            red.stage(stage, lax.div(step - first, N_COLOR))

    @pl.when(step < n_blk)
    def _():
        cols = pl.ds(pl.multiple_of(step * FF_BLK, FF_BLK), FF_BLK)
        for row in range(0, seq, 256):
            rows = slice(row, row + 256)
            da = dot_nt(dy_ref[rows, :], w2_ref[0]).astype(jnp.bfloat16).astype(jnp.float32)
            z = z_ref[rows, :].astype(jnp.float32)
            z_sq = z * z
            th = jnp.tanh(z * (GELU_C + (GELU_C * 0.044715) * z_sq))
            cdf = 0.5 + 0.5 * th
            a_ref[rows, :] = (z * cdf).astype(jnp.bfloat16)
            slope = cdf + (0.5 * z) * (1.0 - th * th) * (GELU_C + (3.0 * GELU_C * 0.044715) * z_sq)
            dz_ref[rows, cols] = (slope * da).astype(jnp.bfloat16)
        dw1 = dot_nn(ut_ref[...], dz_ref[:, cols])
        block_ref[0, :, :, 0:48, :] = dw1.reshape(8, 2, 48, UNIT_COLS)
        dw2 = dot_nn(a_ref[...].T, dy_ref[...])
        for part in range(3):
            block_ref[0, :, :, 48 + 16 * part:64 + 16 * part, :] = dw2[:, part * UNIT_COLS:(part + 1) * UNIT_COLS].reshape(8, 2, 16, UNIT_COLS)

    @pl.when(step < N_COLOR * MLP_CHUNKS)
    def _():
        chunk, color = lax.div(step, N_COLOR), lax.rem(step, N_COLOR)

        def body(i, carry):
            red.own[chunk, color, i] = block_ref[0, i, core]
            red.send0[chunk, color, i] = block_ref[0, i, 1 - core].astype(jnp.bfloat16)
            return carry
        lax.fori_loop(0, 8, body, 0)
        red.copy(0, chunk, color).start()

    @pl.when(step >= n_blk)
    def _():
        du_ref[...] = dot_nt(dz_ref[...], w1_ref[0]).astype(jnp.bfloat16)

    @pl.when(step == pl.num_programs(0) - 1)
    def _():
        red.stage(3, MLP_CHUNKS - 1)
        for chunk in range(MLP_CHUNKS):
            red.finish(chunk, shard_ref)


def mlp_backward(dy, u_two, z_lo, w_up, w_down, layer, grads, after, call_id):
    seq, width = dy.shape
    n_blk = w_up.shape[2] // FF_BLK
    n_last = width // 256
    last = n_blk - N_COLOR
    whole = pl.BlockSpec((seq, width), lambda step: (0, 0))
    parts = [qkv_parts(0)] if grads else []
    shard_shape = (N_COLOR * (MLP_CHUNKS * MLP_ROWS + len(parts) * ATTN_ROWS), UNIT_COLS)
    return pl.pallas_call(
        functools.partial(mlp_bwd_kernel, parts, len(grads), len(after)),
        grid=(n_blk + n_last,),
        in_specs=[
            whole, whole,
            pl.BlockSpec((seq, FF_BLK), lambda step: (0, jnp.minimum(step, n_blk - 1))),
            pl.BlockSpec((1, 256, w_up.shape[2]), lambda step: (layer, jnp.maximum(step - n_blk, 0), 0)),
            pl.BlockSpec((1, FF_BLK, width), lambda step: (layer, jnp.minimum(step, n_blk - 1), 0)),
        ] + [pl.BlockSpec(memory_space=pl.ANY)] * (len(grads) + len(after)),
        out_specs=[
            pl.BlockSpec((seq, 256), lambda step: (0, jnp.maximum(step - n_blk, 0))),
            pl.BlockSpec((1, 8, 2, MLP_ROWS, UNIT_COLS), lambda step: (jnp.clip(step - last, 0, N_COLOR - 1), 0, 0, 0, 0)),
            pl.BlockSpec(shard_shape, lambda step: (0, 0)),
        ],
        out_shape=[jax.ShapeDtypeStruct((seq, width), jnp.bfloat16), jax.ShapeDtypeStruct((N_COLOR, 8, 2, MLP_ROWS, UNIT_COLS), jnp.float32), jax.ShapeDtypeStruct(shard_shape, jnp.bfloat16)],
        scratch_shapes=[pltpu.VMEM((width, seq), jnp.bfloat16), pltpu.VMEM((seq, FF_BLK), jnp.bfloat16), pltpu.VMEM((seq, w_up.shape[2]), jnp.bfloat16)] + reducer_scratch(MLP_CHUNKS, MLP_ROWS) + (reducer_scratch(1, ATTN_ROWS) if parts else []),
        compiler_params=pltpu.CompilerParams(dimension_semantics=("arbitrary",), vmem_limit_bytes=VMEM_ALL, collective_id=call_id),
        cost_estimate=cost(30, 30),
        name="mlp_bwd",
    )(dy, u_two, z_lo, w_up, w_down, *grads, *after)


def attn_bwd_kernel(parts, n_grads, n_after, *refs):
    q_ref, k_ref, v_ref, do_ref, lse_ref, u_ref = refs[:6]
    grad_refs = refs[6:6 + n_grads]
    refs = refs[6 + n_grads + n_after:]
    dq_ref, dk_ref, dv_ref, dwq_ref, dwk_ref, dwv_ref, shard_ref, ut_ref, kt_ref, dqt_ref, dk_acc, dv_acc = refs[:12]
    red = Reducer(len(parts), refs[12:], grad_refs, parts)
    n_chunks = red.n_chunks
    pair = pl.program_id(0)
    seq = q_ref.shape[0]
    events = {}
    for chunk in range(n_chunks):
        events.setdefault(1 + chunk, []).append((1, chunk))
        events.setdefault(4 + 2 * chunk, []).append((2, chunk))
        events.setdefault(7 + 2 * chunk, []).append((3, chunk))

    @pl.when(pair == 0)
    def _():
        red.barrier()
        for chunk in range(n_chunks):
            red.load(chunk, 1 - red.bit[0])
        for chunk in range(n_chunks):
            red.convert(chunk)
            red.load(chunk, red.bit[0])
        ut_ref[...] = u_ref[...].T

    kt_ref[...] = k_ref[...].T
    for head in range(LANES // HEAD_DIM):
        for when, todo in events.items():
            if when % 2 == head:
                @pl.when(pair == when // 2)
                def _():
                    for stage, chunk in todo:
                        if stage == 1:
                            red.wait_load(chunk)
                        red.stage(stage, chunk)
        rows = slice(head * HEAD_DIM, (head + 1) * HEAD_DIM)
        for q_start in range(0, seq, Q_BLK):
            q_end = q_start + Q_BLK
            q_m = head_mask(q_ref[q_start:q_end, :], head)
            do_m = head_mask(do_ref[q_start:q_end, :], head)
            s_t = scores_t(k_ref, q_m, q_start)
            p_t = jnp.exp2(s_t * EXP_SCALE - lse_ref[0, head:head + 1, q_start:q_end])
            dp_t = dot_nt(v_ref[:q_end, :], do_m)
            delta = jnp.sum(p_t * dp_t, axis=0, keepdims=True)
            ds_t = (p_t * (dp_t - delta) * HEAD_DIM ** -0.5).astype(jnp.bfloat16)
            dv_part = dot_nn(p_t.astype(jnp.bfloat16), do_m)
            dk_part = dot_nn(ds_t, q_m)
            if head == 0 and q_start == 0:
                dv_acc[...] = jnp.zeros_like(dv_acc)
                dk_acc[...] = jnp.zeros_like(dk_acc)
            dv_acc[:q_end, :] += dv_part
            dk_acc[:q_end, :] += dk_part
            dqt_ref[rows, q_start:q_end] = dot_nn(kt_ref[rows, :q_end], ds_t)
    dq_ref[...] = dqt_ref[...].T.astype(jnp.bfloat16)
    dk_ref[...] = dk_acc[...].astype(jnp.bfloat16)
    dv_ref[...] = dv_acc[...].astype(jnp.bfloat16)
    d_w = dot_nn(ut_ref[...], jnp.concatenate([dq_ref[...], dk_ref[...], dv_ref[...]], axis=1))
    for out_ref, at in ((dwq_ref, 0), (dwk_ref, LANES), (dwv_ref, 2 * LANES)):
        out_ref[...] = d_w[:, at:at + LANES].reshape(out_ref.shape)

    @pl.when(pair == pl.num_programs(0) - 1)
    def _():
        for chunk in range(n_chunks):
            red.finish(chunk, shard_ref)


def tail_kernel(parts, n_grads, n_after, *refs):
    gains_ref = refs[0]
    grad_refs = refs[1:1 + n_grads]
    refs = refs[:1 + n_grads] + refs[1 + n_grads + n_after:]
    shard_ref, gsum_ref, gbuf, gsend_sem, grecv_sem = refs[1 + n_grads:6 + n_grads]
    red = Reducer(len(parts), refs[6 + n_grads:], grad_refs, parts)
    n_dev = gbuf.shape[0]
    for chunk in range(red.n_chunks):
        red.load(chunk, 1 - red.bit[0])
    sem = pltpu.get_barrier_semaphore()
    for shift in range(1, n_dev):
        pl.semaphore_signal(sem, inc=1, device_id=(lax.rem(red.me + shift, n_dev),), device_id_type=MESH)
    pl.semaphore_wait(sem, n_dev - 1)

    def gain_copy(shift):
        dev = lax.rem(red.me + shift, n_dev)
        return pltpu.make_async_remote_copy(src_ref=gains_ref, dst_ref=gbuf.at[shift], send_sem=gsend_sem.at[shift], recv_sem=grecv_sem.at[shift], device_id=(dev,), device_id_type=MESH)
    for shift in range(1, n_dev):
        gain_copy(shift).start()
    gbuf[0] = gains_ref[...]
    for chunk in range(red.n_chunks):
        red.convert(chunk)
        red.load(chunk, red.bit[0])
    for step in range(1, 4):
        for chunk in range(red.n_chunks):
            if step == 1:
                red.wait_load(chunk)
            red.stage(step, chunk)
    for shift in range(1, n_dev):
        gain_copy(shift).wait()
    acc = jnp.zeros(gains_ref.shape, jnp.float32)
    for dev in range(n_dev):
        acc = acc + gbuf[lax.rem(red.me + n_dev - dev, n_dev)]
    gsum_ref[...] = acc
    for chunk in range(red.n_chunks):
        red.finish(chunk, shard_ref)


def attn_specs(seq, n_pairs):
    def col(shift):
        return pl.BlockSpec((seq, LANES), lambda pair: (0, pair + shift))
    lse = pl.BlockSpec((1, 8, seq), lambda pair: (pair, 0, 0))
    return col, lse


def attn_forward(qkv):
    seq, width = qkv.shape[0], qkv.shape[1] // 3
    n_pairs = width // LANES
    col, lse = attn_specs(seq, n_pairs)
    return pl.pallas_call(
        attn_fwd_kernel,
        grid=(n_pairs,),
        in_specs=[col(0), col(n_pairs), col(2 * n_pairs)],
        out_specs=[col(0), lse],
        out_shape=[jax.ShapeDtypeStruct((seq, width), jnp.bfloat16), jax.ShapeDtypeStruct((n_pairs, 8, seq), jnp.float32)],
        scratch_shapes=[pltpu.VMEM((LANES, seq), jnp.bfloat16), pltpu.VMEM((LANES, seq), jnp.float32)],
        compiler_params=pltpu.CompilerParams(dimension_semantics=("arbitrary",), vmem_limit_bytes=24 * MIB),
        cost_estimate=cost(16, 8),
        name="attn_fwd",
    )(qkv, qkv, qkv)


def attn_backward(qkv, d_out, lse_vals, u_one, grads, parts, after, call_id):
    seq, width = qkv.shape[0], qkv.shape[1] // 3
    n_pairs = width // LANES
    col, lse = attn_specs(seq, n_pairs)
    shape = jax.ShapeDtypeStruct((seq, width), jnp.bfloat16)
    shard_shape = (len(parts) * N_COLOR * ATTN_ROWS, UNIT_COLS)
    d_w = pl.BlockSpec((8, 2, width // 16, LANES), lambda pair: (0, 0, 0, pair))
    out = pl.pallas_call(
        functools.partial(attn_bwd_kernel, parts, len(grads), len(after)),
        grid=(n_pairs,),
        in_specs=[col(0), col(n_pairs), col(2 * n_pairs), col(0), lse, pl.BlockSpec((seq, width), lambda pair: (0, 0))] + [pl.BlockSpec(memory_space=pl.ANY)] * (len(grads) + len(after)),
        out_specs=[col(0), col(0), col(0), d_w, d_w, d_w, pl.BlockSpec(shard_shape, lambda pair: (0, 0))],
        out_shape=[shape, shape, shape] + [pltpu.HBM((8, 2, width // 16, width), jnp.float32)] * 3 + [jax.ShapeDtypeStruct(shard_shape, jnp.bfloat16)],
        scratch_shapes=[pltpu.VMEM((width, seq), jnp.bfloat16), pltpu.VMEM((LANES, seq), jnp.bfloat16), pltpu.VMEM((LANES, seq), jnp.float32), pltpu.VMEM((seq, LANES), jnp.float32), pltpu.VMEM((seq, LANES), jnp.float32)] + reducer_scratch(len(parts), ATTN_ROWS),
        compiler_params=pltpu.CompilerParams(dimension_semantics=("arbitrary",), vmem_limit_bytes=VMEM_ALL, collective_id=call_id),
        cost_estimate=cost(40, 14),
        name="attn_bwd",
    )(qkv, qkv, qkv, d_out, lse_vals, u_one, *grads, *after)
    return out[:3], list(out[3:6]), out[6]


def tail_reduce(gains, grads, parts, after, call_id, n_dev):
    n_chunks = len(parts)
    shard_shape = (n_chunks * N_COLOR * ATTN_ROWS, UNIT_COLS)
    return pl.pallas_call(
        functools.partial(tail_kernel, parts, len(grads), len(after)),
        in_specs=[pl.BlockSpec(memory_space=pltpu.VMEM)] + [pl.BlockSpec(memory_space=pl.ANY)] * (len(grads) + len(after)),
        out_specs=[pl.BlockSpec(memory_space=pltpu.VMEM)] * 2,
        out_shape=[jax.ShapeDtypeStruct(shard_shape, jnp.bfloat16), jax.ShapeDtypeStruct(gains.shape, jnp.float32)],
        scratch_shapes=[pltpu.VMEM((n_dev,) + gains.shape, jnp.float32), pltpu.SemaphoreType.DMA((n_dev,)), pltpu.SemaphoreType.DMA((n_dev,))] + reducer_scratch(n_chunks, ATTN_ROWS),
        compiler_params=pltpu.CompilerParams(vmem_limit_bytes=16 * MIB, collective_id=call_id),
        cost_estimate=cost(20, 14),
        name="tail_reduce",
    )(gains, *grads, *after)


def block_forward(x_blk, gain_a, gain_b, w_qkv, w_out, w_up):
    norm_a, norm_a_back = jax.vjp(rms_gain, x_blk.astype(jnp.float32), gain_a)
    u_one = norm_a.astype(jnp.bfloat16)
    qkv = dot_lo(u_one, w_qkv)
    attn_out, lse_vals = attn_forward(qkv)
    hidden = x_blk + dot_lo(attn_out, w_out)
    norm_b, norm_b_back = jax.vjp(rms_gain, hidden.astype(jnp.float32), gain_b)
    u_two = norm_b.astype(jnp.bfloat16)
    pre_lo = dot_lo(u_two, w_up)
    act_lo = gelu_tanh(pre_lo.astype(jnp.float32)).astype(jnp.bfloat16)
    return hidden, act_lo, (norm_a_back, u_one, qkv, lse_vals, attn_out, norm_b_back, u_two, pre_lo)


def block_backward(grad_blk, saved_vals, w_qkv, w_out, w_up, w_down, layer, ready, after):
    (norm_a_back, u_one, qkv, lse_vals, attn_out, norm_b_back, u_two, pre_lo) = saved_vals
    ids = len(ready)
    grad_u_two, block, shard_mlp = mlp_backward(grad_blk, u_two, pre_lo, w_up, w_down, layer, ready, after[:1], ids)
    grad_h_norm, grad_gain_b = norm_b_back(grad_u_two.astype(jnp.float32))
    grad_hidden = (grad_blk.astype(jnp.float32) + grad_h_norm).astype(jnp.bfloat16)
    grad_out_w = dot_tn(attn_out, grad_hidden)
    grad_attn = dot_nt(grad_hidden, w_out).astype(jnp.bfloat16)
    grads = [block, grad_view(grad_out_w)]
    parts = [rest_parts(0, 1)]
    pieces, grad_qkv_w, shard_attn = attn_backward(qkv, grad_attn, lse_vals, u_one, grads, parts, after[1:], ids + 1)
    grad_qkv = jnp.concatenate(pieces, axis=1)
    grad_u_one = dot_nt(grad_qkv, w_qkv).astype(jnp.bfloat16)
    grad_x_norm, grad_gain_a = norm_a_back(grad_u_one.astype(jnp.float32))
    grad_x_blk = (grad_hidden.astype(jnp.float32) + grad_x_norm).astype(jnp.bfloat16)
    return grad_x_blk, grad_gain_a, grad_gain_b, grad_qkv_w, unit_gather(shard_mlp), unit_gather(shard_attn)


def unit_gather(shard):
    return lax.all_gather(shard, 'data', axis=0, tiled=True).reshape((-1,) + shard.shape)


def put_qkv(unit_ref, base, out_ref, scale):
    for dev in range(DEV_BLK):
        for color in range(N_COLOR):
            for part in range(3):
                cols = slice((color * 3 + part) * UNIT_COLS, (color * 3 + part + 1) * UNIT_COLS)
                row = base + color * ATTN_ROWS + part * 48
                out_ref[0, dev * 48:dev * 48 + 48, cols] = unit_ref[dev, row:row + 48, :].astype(jnp.float32) * scale


def unpack_kernel(with_qkv, n_dev, n_out, *refs):
    mlp_ref, attn_ref = refs[:2]
    up_ref, down_ref, out_ref = refs[-n_out:][:3]
    scale = 1.0 / n_dev
    n_mlp = N_COLOR * MLP_CHUNKS

    def value(unit):
        return unit.astype(jnp.float32) * scale
    for dev in range(DEV_BLK):
        rows = slice(dev * 48, dev * 48 + 48)
        for blk in range(n_mlp + N_COLOR):
            ref, row = (mlp_ref, blk * MLP_ROWS) if blk < n_mlp else (attn_ref, (blk - n_mlp) * ATTN_ROWS)
            up_ref[0, rows, blk * FF_BLK:(blk + 1) * FF_BLK] = value(ref[dev, row:row + 48, :])
            for part in range(3):
                at = row + 48 + 16 * part
                down_ref[0, blk, dev, :, part * UNIT_COLS:(part + 1) * UNIT_COLS] = value(ref[dev, at:at + 16, :])
        for color in range(N_COLOR):
            row = color * ATTN_ROWS + MLP_ROWS
            out_ref[0, rows, color * UNIT_COLS:(color + 1) * UNIT_COLS] = value(attn_ref[dev, row:row + 48, :])
    if with_qkv:
        put_qkv(mlp_ref, n_mlp * MLP_ROWS, refs[-1], scale)


def unpack(mlp_all, attn_all, with_qkv, layer, width, hidden, into, after):
    n_dev = mlp_all.shape[0]
    def in_spec(arr):
        return pl.BlockSpec((DEV_BLK,) + arr.shape[1:], lambda dev: (dev, 0, 0))
    def rows(shape, at):
        return pl.BlockSpec((1, DEV_BLK * (width // n_dev), shape[2]), lambda dev: (at, dev, 0))
    n_blk = hidden // FF_BLK
    shapes = [(2, width, hidden), (2, n_blk, n_dev, FF_BLK // n_dev, width), (2, width, width)]
    down = pl.BlockSpec((1, n_blk, DEV_BLK, FF_BLK // n_dev, width), lambda dev: (layer, 0, dev, 0, 0))
    out_specs = [rows(shapes[0], layer), down, rows(shapes[2], layer)]
    if with_qkv:
        shapes.append((2, width, 3 * width))
        out_specs.append(rows(shapes[3], layer + 1))
    return pl.pallas_call(
        functools.partial(unpack_kernel, with_qkv, n_dev, len(shapes)),
        grid=(n_dev // DEV_BLK,),
        in_specs=[in_spec(mlp_all), in_spec(attn_all)] + [pl.BlockSpec(memory_space=pl.ANY)] * (len(into) + len(after)),
        out_specs=out_specs,
        out_shape=[jax.ShapeDtypeStruct(shape, jnp.float32) for shape in shapes],
        input_output_aliases={2 + i: i for i in range(len(into))},
        compiler_params=pltpu.CompilerParams(dimension_semantics=("arbitrary",), vmem_limit_bytes=32 * MIB),
        cost_estimate=cost(10, 40),
        name="unpack",
    )(mlp_all, attn_all, *into, *after)


def unpack_qkv_kernel(n_dev, last_ref, into_ref, out_ref):
    put_qkv(last_ref, 0, out_ref, 1.0 / n_dev)


def unpack_qkv(last_all, into):
    n_dev = last_all.shape[0]
    rows, cols = into.shape[1:]
    return pl.pallas_call(
        functools.partial(unpack_qkv_kernel, n_dev),
        grid=(n_dev // DEV_BLK,),
        in_specs=[pl.BlockSpec((DEV_BLK,) + last_all.shape[1:], lambda dev: (dev, 0, 0)), pl.BlockSpec(memory_space=pl.ANY)],
        out_specs=pl.BlockSpec((1, DEV_BLK * (rows // n_dev), cols), lambda dev: (0, dev, 0)),
        out_shape=jax.ShapeDtypeStruct(into.shape, jnp.float32),
        input_output_aliases={1: 0},
        compiler_params=pltpu.CompilerParams(dimension_semantics=("arbitrary",), vmem_limit_bytes=16 * MIB),
        cost_estimate=cost(4, 20),
        name="unpack_qkv",
    )(last_all, into)


def solution(mesh):
    n_dev = mesh.shape['data']

    def local_step(x_loc, grad_y_loc, gain_one, gain_two, w_qkv, w_out, w_up, w_down):
        n_layers = w_qkv.shape[0]
        hidden_x = x_loc[0]
        saved_all = []
        for layer_idx in range(n_layers):
            hidden, act_lo, saved_vals = block_forward(hidden_x, gain_one[layer_idx], gain_two[layer_idx], w_qkv[layer_idx], w_out[layer_idx], w_up[layer_idx])
            saved_all.append(saved_vals)
            if layer_idx + 1 < n_layers:
                hidden_x = hidden + dot_lo(act_lo, w_down[layer_idx])
        grad_cur = grad_y_loc[0]
        width, hidden = w_up.shape[1:]
        gains = [None] * (2 * n_layers)
        ready, after, gathered = [], [], []
        for layer_idx in reversed(range(n_layers)):
            out = block_backward(grad_cur, saved_all[layer_idx], w_qkv[layer_idx], w_out[layer_idx], w_up, w_down, layer_idx, ready, after)
            grad_cur, gains[layer_idx], gains[n_layers + layer_idx], grad_qkv_w = out[:4]
            ready, after = grad_qkv_w, list(out[4:])
            gathered.append(after)
        (top_mlp, top_attn), (low_mlp, low_attn) = gathered
        gain_rows = jnp.concatenate([jnp.stack(gains), jnp.zeros((8 - 2 * n_layers, width), jnp.float32)])
        shard, gain_sums = tail_reduce(gain_rows, ready, [qkv_parts(0)], [low_mlp], 3 * n_layers, n_dev)
        last = unit_gather(shard)
        partial = unpack(top_mlp, top_attn, False, 1, width, hidden, [], [gain_sums])
        w_u, w_d, w_o, grad_qkv = unpack(low_mlp, low_attn, True, 0, width, hidden, partial, [])
        gain_sums = gain_sums / n_dev
        grad_qkv = unpack_qkv(last, grad_qkv)
        weights = (grad_qkv, w_o, w_u, w_d.reshape(n_layers, hidden, width))
        return (grad_cur[None], gain_sums[:n_layers], gain_sums[n_layers:2 * n_layers]) + weights

    batch_spec = P('data')
    full_spec = P()
    return jax.shard_map(local_step, mesh=mesh, in_specs=(batch_spec, batch_spec) + (full_spec,) * 6, out_specs=(batch_spec,) + (full_spec,) * 6, check_vma=False)
```

```python
import functools

import jax
import jax.numpy as jnp
from jax import lax
from jax.experimental import pallas as pl
from jax.experimental.pallas import tpu as pltpu
from jax.sharding import PartitionSpec as P

NORM_EPS = 1e-6
HEAD_DIM = 64
LANES = 128
Q_BLK = 256
EXP_SCALE = HEAD_DIM ** -0.5 * 1.4426950408889634
NEG = -1e30
MIB = 2 ** 20
VMEM_ALL = 67043328
MESH = pl.DeviceIdType.MESH


def cost(gflops, mbytes):
    return pl.CostEstimate(flops=gflops * 10 ** 9, bytes_accessed=mbytes * MIB, transcendentals=0)


def rms_gain(rows_f, gain_vec):
    return rows_f * lax.rsqrt(jnp.mean(rows_f * rows_f, axis=-1, keepdims=True) + NORM_EPS) * gain_vec


def gelu_tanh(pre_act):
    return jax.nn.gelu(pre_act, approximate=True)


def dot_lo(lhs, rhs):
    return jnp.dot(lhs, rhs, preferred_element_type=jnp.float32).astype(jnp.bfloat16)


def dot_nt(lhs, rhs):
    return lax.dot_general(lhs, rhs, (((1,), (1,)), ((), ())), preferred_element_type=jnp.float32)


def dot_tn(lhs, rhs):
    return lax.dot_general(lhs, rhs, (((0,), (0,)), ((), ())), preferred_element_type=jnp.float32)


def dot_nn(lhs, rhs):
    return jnp.dot(lhs, rhs, preferred_element_type=jnp.float32)


def head_mask(ref_rows, head):
    lane = lax.broadcasted_iota(jnp.int32, ref_rows.shape, 1)
    return jnp.where(lane // HEAD_DIM == head, ref_rows, jnp.zeros_like(ref_rows))


def scores_t(k_ref, q_m, q_start):
    diag = dot_nt(k_ref[q_start:q_start + Q_BLK, :], q_m)
    key_i = lax.broadcasted_iota(jnp.int32, diag.shape, 0)
    query_i = lax.broadcasted_iota(jnp.int32, diag.shape, 1)
    diag = jnp.where(key_i <= query_i, diag, NEG)
    if q_start == 0:
        return diag
    return jnp.concatenate([dot_nt(k_ref[:q_start, :], q_m), diag], axis=0)


def attn_fwd_kernel(q_ref, k_ref, v_ref, o_ref, lse_ref, vt_ref, ot_ref):
    seq = q_ref.shape[0]
    vt_ref[...] = v_ref[...].T
    for head in range(LANES // HEAD_DIM):
        rows = slice(head * HEAD_DIM, (head + 1) * HEAD_DIM)
        for q_start in range(0, seq, Q_BLK):
            q_end = q_start + Q_BLK
            q_m = head_mask(q_ref[q_start:q_end, :], head)
            s_t = scores_t(k_ref, q_m, q_start)
            top = jnp.max(s_t, axis=0, keepdims=True)
            p_t = jnp.exp2((s_t - top) * EXP_SCALE)
            total = jnp.sum(p_t, axis=0, keepdims=True)
            p_lo = (p_t * (1.0 / total)).astype(jnp.bfloat16)
            ot_ref[rows, q_start:q_end] = dot_nn(vt_ref[rows, :q_end], p_lo)
            lse_ref[0, head:head + 1, q_start:q_end] = top * EXP_SCALE + jnp.log2(total)
    o_ref[...] = ot_ref[...].T.astype(jnp.bfloat16)


N_COLOR = 3
UNIT_COLS = 256
FF_BLK = 256
MLP_ROWS = 96
ATTN_ROWS = 144
MLP_CHUNKS = 3
DEV_BLK = 2
GELU_C = 0.7978845608028654
AXIS_BITS = (3, 2, 1)


class Reducer:
    def __init__(self, n_chunks, refs, grad_refs=(), parts=()):
        (self.own, self.send0, self.recv0, self.send1, self.recv1, self.send2, self.recv2, self.send3, self.recv3, self.load_sem, self.send_sem, self.recv_sem) = refs
        self.grad_refs, self.parts = grad_refs, parts
        self.n_chunks = n_chunks
        me = lax.axis_index('data')
        self.me = me
        self.bit = [lax.rem(lax.div(me, 1 << b), 2) for b in range(4)]
        self.partner = [me + (1 - 2 * self.bit[b]) * (1 << b) for b in range(4)]

    def barrier(self):
        sem = pltpu.get_barrier_semaphore()
        for dev in self.partner:
            pl.semaphore_signal(sem, inc=1, device_id=(dev,), device_id_type=MESH)
        pl.semaphore_wait(sem, 4)

    def load(self, chunk, half):
        for color in range(N_COLOR):
            for part, (array, kind, col, row, n_rows) in enumerate(self.parts[chunk][color]):
                if kind == 'block':
                    src = self.grad_refs[array].at[col, :, half]
                else:
                    src = self.grad_refs[array].at[:, half, :, pl.ds(col, UNIT_COLS)]
                dst = self.own.at[chunk, color, :, pl.ds(row, n_rows)]
                pltpu.make_async_copy(src, dst, self.load_sem.at[chunk, color, part]).start()

    def wait_load(self, chunk):
        for color in range(N_COLOR):
            for part, (_, _, _, row, n_rows) in enumerate(self.parts[chunk][color]):
                ref = self.own.at[chunk, color, :, pl.ds(row, n_rows)]
                pltpu.make_async_copy(ref, ref, self.load_sem.at[chunk, color, part]).wait()

    def copy(self, stage, chunk, color):
        send = (self.send0, self.send1, self.send2, self.send3)[stage].at[chunk, color]
        recv = (self.recv0, self.recv1, self.recv2, self.recv3)[stage].at[chunk, color]
        dev = self.partner[0] if stage == 0 else self.partner[self.order(color)[stage - 1]]
        return pltpu.make_async_remote_copy(src_ref=send, dst_ref=recv, send_sem=self.send_sem.at[stage, chunk, color], recv_sem=self.recv_sem.at[stage, chunk, color], device_id=(dev,), device_id_type=MESH)

    def order(self, color):
        return [1 + (color + step) % N_COLOR for step in range(N_COLOR)]

    def block(self, values):
        return values[3] * 4 + values[2] * 2 + values[1]

    def convert(self, chunk):
        self.wait_load(chunk)
        for color in range(N_COLOR):
            def body(i, carry):
                self.send0[chunk, color, i] = self.own[chunk, color, i].astype(jnp.bfloat16)
                return carry
            lax.fori_loop(0, 8, body, 0)
            self.copy(0, chunk, color).start()

    def total(self, chunk, color, values, n_recv):
        order = self.order(color)
        index = self.block(values)
        acc = self.own[chunk, color, index] + self.recv0[chunk, color, index].astype(jnp.float32)
        if n_recv >= 2:
            acc = acc + self.recv1[chunk, color, values[order[1]] * 2 + values[order[2]]].astype(jnp.float32)
        if n_recv >= 3:
            acc = acc + self.recv2[chunk, color, values[order[2]]].astype(jnp.float32)
        if n_recv >= 4:
            acc = acc + self.recv3[chunk, color, 0].astype(jnp.float32)
        return acc

    def stage(self, step, chunk):
        send = (None, self.send1, self.send2, self.send3)[step]
        n_free = N_COLOR - step
        for color in range(N_COLOR):
            self.copy(step - 1, chunk, color).wait_recv()
            order = self.order(color)

            def body(i, carry):
                values = [0, 0, 0, 0]
                for done in range(step - 1):
                    values[order[done]] = self.bit[order[done]]
                values[order[step - 1]] = 1 - self.bit[order[step - 1]]
                if n_free == 2:
                    values[order[1]], values[order[2]] = lax.div(i, 2), lax.rem(i, 2)
                elif n_free == 1:
                    values[order[2]] = i
                send[chunk, color, i] = self.total(chunk, color, values, step).astype(jnp.bfloat16)
                return carry
            if n_free:
                lax.fori_loop(0, 1 << n_free, body, 0)
            else:
                body(0, 0)
            self.copy(step, chunk, color).start()

    def finish(self, chunk, out_ref, base=0):
        n_rows = self.own.shape[3]
        for color in range(N_COLOR):
            self.copy(3, chunk, color).wait_recv()
            row = base + (chunk * N_COLOR + color) * n_rows
            out_ref[row:row + n_rows, :] = self.total(chunk, color, self.bit, 4).astype(jnp.bfloat16)
        for stage in range(4):
            for color in range(N_COLOR):
                self.copy(stage, chunk, color).wait_send()


def reducer_scratch(n_chunks, rows):
    def buf(blocks, dtype):
        return pltpu.VMEM((n_chunks, N_COLOR, blocks, rows, UNIT_COLS), dtype)
    lo = jnp.bfloat16
    return [buf(8, jnp.float32), buf(8, lo), buf(8, lo), buf(4, lo), buf(4, lo), buf(2, lo), buf(2, lo), buf(1, lo), buf(1, lo), pltpu.SemaphoreType.DMA((n_chunks, N_COLOR, N_COLOR)), pltpu.SemaphoreType.DMA((4, n_chunks, N_COLOR)), pltpu.SemaphoreType.DMA((4, n_chunks, N_COLOR))]


def grad_view(grad_w):
    rows, cols = grad_w.shape
    return grad_w.reshape(8, 2, rows // 16, cols)


def qkv_parts(array):
    return [[(array + color, 'cols', part * UNIT_COLS, part * 48, 48) for part in range(3)] for color in range(N_COLOR)]


def rest_parts(block_array, out_array):
    return [[(block_array, 'block', color, 0, MLP_ROWS), (out_array, 'cols', color * UNIT_COLS, MLP_ROWS, 48)] for color in range(N_COLOR)]


def mlp_bwd_kernel(parts, n_grads, n_after, *refs):
    dy_ref, u_ref, z_ref, w1_ref, w2_ref = refs[:5]
    grad_refs = refs[5:5 + n_grads]
    refs = refs[5 + n_grads + n_after:]
    du_ref, block_ref, shard_ref, ut_ref, a_ref, dz_ref = refs[:6]
    n_red = (len(refs) - 6) // (2 if parts else 1)
    red = Reducer(MLP_CHUNKS, refs[6:6 + n_red])
    early = Reducer(len(parts), refs[6 + n_red:], grad_refs, parts) if parts else None
    step = pl.program_id(0)
    n_blk = dz_ref.shape[1] // FF_BLK
    core = red.bit[0]
    seq = dy_ref.shape[0]

    @pl.when(step == 0)
    def _():
        red.barrier()
        if early:
            early.load(0, 1 - core)
        ut_ref[...] = u_ref[...].T

    if early:
        @pl.when(step == 1)
        def _():
            early.convert(0)
            early.load(0, core)

        for stage, when in ((1, 2), (2, 5), (3, 7)):
            @pl.when(step == when)
            def _():
                if stage == 1:
                    early.wait_load(0)
                early.stage(stage, 0)

        @pl.when(step == n_blk - 1)
        def _():
            early.finish(0, shard_ref, N_COLOR * MLP_CHUNKS * MLP_ROWS)

    for stage, first, count in ((3, 9, MLP_CHUNKS - 1), (2, 7, MLP_CHUNKS), (1, 4, MLP_CHUNKS)):
        @pl.when((step >= first) & (step < first + N_COLOR * count) & (lax.rem(step + 2 * first, N_COLOR) == 0))
        def _():
            red.stage(stage, lax.div(step - first, N_COLOR))

    @pl.when(step < n_blk)
    def _():
        cols = pl.ds(pl.multiple_of(step * FF_BLK, FF_BLK), FF_BLK)
        for row in range(0, seq, 256):
            rows = slice(row, row + 256)
            da = dot_nt(dy_ref[rows, :], w2_ref[0]).astype(jnp.bfloat16).astype(jnp.float32)
            z = z_ref[rows, :].astype(jnp.float32)
            z_sq = z * z
            th = jnp.tanh(z * (GELU_C + (GELU_C * 0.044715) * z_sq))
            cdf = 0.5 + 0.5 * th
            a_ref[rows, :] = (z * cdf).astype(jnp.bfloat16)
            slope = cdf + (0.5 * z) * (1.0 - th * th) * (GELU_C + (3.0 * GELU_C * 0.044715) * z_sq)
            dz_ref[rows, cols] = (slope * da).astype(jnp.bfloat16)
        dw1 = dot_nn(ut_ref[...], dz_ref[:, cols])
        block_ref[0, :, :, 0:48, :] = dw1.reshape(8, 2, 48, UNIT_COLS)
        dw2 = dot_nn(a_ref[...].T, dy_ref[...])
        for part in range(3):
            block_ref[0, :, :, 48 + 16 * part:64 + 16 * part, :] = dw2[:, part * UNIT_COLS:(part + 1) * UNIT_COLS].reshape(8, 2, 16, UNIT_COLS)

    @pl.when(step < N_COLOR * MLP_CHUNKS)
    def _():
        chunk, color = lax.div(step, N_COLOR), lax.rem(step, N_COLOR)

        def body(i, carry):
            red.own[chunk, color, i] = block_ref[0, i, core]
            red.send0[chunk, color, i] = block_ref[0, i, 1 - core].astype(jnp.bfloat16)
            return carry
        lax.fori_loop(0, 8, body, 0)
        red.copy(0, chunk, color).start()

    @pl.when(step >= n_blk)
    def _():
        du_ref[...] = dot_nt(dz_ref[...], w1_ref[0]).astype(jnp.bfloat16)

    @pl.when(step == pl.num_programs(0) - 1)
    def _():
        red.stage(3, MLP_CHUNKS - 1)
        for chunk in range(MLP_CHUNKS):
            red.finish(chunk, shard_ref)


def mlp_backward(dy, u_two, z_lo, w_up, w_down, layer, grads, after, call_id):
    seq, width = dy.shape
    n_blk = w_up.shape[2] // FF_BLK
    n_last = width // 256
    last = n_blk - N_COLOR
    whole = pl.BlockSpec((seq, width), lambda step: (0, 0))
    parts = [qkv_parts(0)] if grads else []
    shard_shape = (N_COLOR * (MLP_CHUNKS * MLP_ROWS + len(parts) * ATTN_ROWS), UNIT_COLS)
    return pl.pallas_call(
        functools.partial(mlp_bwd_kernel, parts, len(grads), len(after)),
        grid=(n_blk + n_last,),
        in_specs=[
            whole, whole,
            pl.BlockSpec((seq, FF_BLK), lambda step: (0, jnp.minimum(step, n_blk - 1))),
            pl.BlockSpec((1, 256, w_up.shape[2]), lambda step: (layer, jnp.maximum(step - n_blk, 0), 0)),
            pl.BlockSpec((1, FF_BLK, width), lambda step: (layer, jnp.minimum(step, n_blk - 1), 0)),
        ] + [pl.BlockSpec(memory_space=pl.ANY)] * (len(grads) + len(after)),
        out_specs=[
            pl.BlockSpec((seq, 256), lambda step: (0, jnp.maximum(step - n_blk, 0))),
            pl.BlockSpec((1, 8, 2, MLP_ROWS, UNIT_COLS), lambda step: (jnp.clip(step - last, 0, N_COLOR - 1), 0, 0, 0, 0)),
            pl.BlockSpec(shard_shape, lambda step: (0, 0)),
        ],
        out_shape=[jax.ShapeDtypeStruct((seq, width), jnp.bfloat16), jax.ShapeDtypeStruct((N_COLOR, 8, 2, MLP_ROWS, UNIT_COLS), jnp.float32), jax.ShapeDtypeStruct(shard_shape, jnp.bfloat16)],
        scratch_shapes=[pltpu.VMEM((width, seq), jnp.bfloat16), pltpu.VMEM((seq, FF_BLK), jnp.bfloat16), pltpu.VMEM((seq, w_up.shape[2]), jnp.bfloat16)] + reducer_scratch(MLP_CHUNKS, MLP_ROWS) + (reducer_scratch(1, ATTN_ROWS) if parts else []),
        compiler_params=pltpu.CompilerParams(dimension_semantics=("arbitrary",), vmem_limit_bytes=VMEM_ALL, collective_id=call_id),
        cost_estimate=cost(30, 30),
        name="mlp_bwd",
    )(dy, u_two, z_lo, w_up, w_down, *grads, *after)


def attn_bwd_kernel(parts, n_grads, n_after, *refs):
    q_ref, k_ref, v_ref, do_ref, lse_ref, u_ref = refs[:6]
    grad_refs = refs[6:6 + n_grads]
    refs = refs[6 + n_grads + n_after:]
    dq_ref, dk_ref, dv_ref, dwq_ref, dwk_ref, dwv_ref, shard_ref, ut_ref, kt_ref, dqt_ref, dk_acc, dv_acc = refs[:12]
    red = Reducer(len(parts), refs[12:], grad_refs, parts)
    n_chunks = red.n_chunks
    pair = pl.program_id(0)
    seq = q_ref.shape[0]
    events = {}
    for chunk in range(n_chunks):
        for stage, when in ((1, 2), (2, 6), (3, 9)):
            events[when] = [(stage, chunk)]

    @pl.when(pair == 0)
    def _():
        red.barrier()
        for chunk in range(n_chunks):
            red.load(chunk, 1 - red.bit[0])
        for chunk in range(n_chunks):
            red.convert(chunk)
            red.load(chunk, red.bit[0])
        ut_ref[...] = u_ref[...].T

    kt_ref[...] = k_ref[...].T
    for head in range(LANES // HEAD_DIM):
        for when, todo in events.items():
            if when % 2 == head:
                @pl.when(pair == when // 2)
                def _():
                    for stage, chunk in todo:
                        if stage == 1:
                            red.wait_load(chunk)
                        red.stage(stage, chunk)
        rows = slice(head * HEAD_DIM, (head + 1) * HEAD_DIM)
        for q_start in range(0, seq, Q_BLK):
            q_end = q_start + Q_BLK
            q_m = head_mask(q_ref[q_start:q_end, :], head)
            do_m = head_mask(do_ref[q_start:q_end, :], head)
            s_t = scores_t(k_ref, q_m, q_start)
            p_t = jnp.exp2(s_t * EXP_SCALE - lse_ref[0, head:head + 1, q_start:q_end])
            dp_t = dot_nt(v_ref[:q_end, :], do_m)
            delta = jnp.sum(p_t * dp_t, axis=0, keepdims=True)
            ds_t = (p_t * (dp_t - delta) * HEAD_DIM ** -0.5).astype(jnp.bfloat16)
            dv_part = dot_nn(p_t.astype(jnp.bfloat16), do_m)
            dk_part = dot_nn(ds_t, q_m)
            if head == 0 and q_start == 0:
                dv_acc[...] = jnp.zeros_like(dv_acc)
                dk_acc[...] = jnp.zeros_like(dk_acc)
            dv_acc[:q_end, :] += dv_part
            dk_acc[:q_end, :] += dk_part
            dqt_ref[rows, q_start:q_end] = dot_nn(kt_ref[rows, :q_end], ds_t)
    dq_ref[...] = dqt_ref[...].T.astype(jnp.bfloat16)
    dk_ref[...] = dk_acc[...].astype(jnp.bfloat16)
    dv_ref[...] = dv_acc[...].astype(jnp.bfloat16)
    d_w = dot_nn(ut_ref[...], jnp.concatenate([dq_ref[...], dk_ref[...], dv_ref[...]], axis=1))
    for out_ref, at in ((dwq_ref, 0), (dwk_ref, LANES), (dwv_ref, 2 * LANES)):
        out_ref[...] = d_w[:, at:at + LANES].reshape(out_ref.shape)

    @pl.when(pair == pl.num_programs(0) - 1)
    def _():
        for chunk in range(n_chunks):
            red.finish(chunk, shard_ref)


def tail_kernel(parts, n_grads, n_after, *refs):
    gains_ref = refs[0]
    grad_refs = refs[1:1 + n_grads]
    refs = refs[:1 + n_grads] + refs[1 + n_grads + n_after:]
    shard_ref, gsum_ref, gbuf, gsend_sem, grecv_sem = refs[1 + n_grads:6 + n_grads]
    red = Reducer(len(parts), refs[6 + n_grads:], grad_refs, parts)
    n_dev = gbuf.shape[0]
    for chunk in range(red.n_chunks):
        red.load(chunk, 1 - red.bit[0])
    sem = pltpu.get_barrier_semaphore()
    for shift in range(1, n_dev):
        pl.semaphore_signal(sem, inc=1, device_id=(lax.rem(red.me + shift, n_dev),), device_id_type=MESH)
    pl.semaphore_wait(sem, n_dev - 1)

    def gain_copy(shift):
        dev = lax.rem(red.me + shift, n_dev)
        return pltpu.make_async_remote_copy(src_ref=gains_ref, dst_ref=gbuf.at[shift], send_sem=gsend_sem.at[shift], recv_sem=grecv_sem.at[shift], device_id=(dev,), device_id_type=MESH)
    for shift in range(1, n_dev):
        gain_copy(shift).start()
    gbuf[0] = gains_ref[...]
    for chunk in range(red.n_chunks):
        red.convert(chunk)
        red.load(chunk, red.bit[0])
    for step in range(1, 4):
        for chunk in range(red.n_chunks):
            if step == 1:
                red.wait_load(chunk)
            red.stage(step, chunk)
    for shift in range(1, n_dev):
        gain_copy(shift).wait()
    acc = jnp.zeros(gains_ref.shape, jnp.float32)
    for dev in range(n_dev):
        acc = acc + gbuf[lax.rem(red.me + n_dev - dev, n_dev)]
    gsum_ref[...] = acc
    for chunk in range(red.n_chunks):
        red.finish(chunk, shard_ref)


def attn_specs(seq, n_pairs):
    def col(shift):
        return pl.BlockSpec((seq, LANES), lambda pair: (0, pair + shift))
    lse = pl.BlockSpec((1, 8, seq), lambda pair: (pair, 0, 0))
    return col, lse


def attn_forward(qkv):
    seq, width = qkv.shape[0], qkv.shape[1] // 3
    n_pairs = width // LANES
    col, lse = attn_specs(seq, n_pairs)
    return pl.pallas_call(
        attn_fwd_kernel,
        grid=(n_pairs,),
        in_specs=[col(0), col(n_pairs), col(2 * n_pairs)],
        out_specs=[col(0), lse],
        out_shape=[jax.ShapeDtypeStruct((seq, width), jnp.bfloat16), jax.ShapeDtypeStruct((n_pairs, 8, seq), jnp.float32)],
        scratch_shapes=[pltpu.VMEM((LANES, seq), jnp.bfloat16), pltpu.VMEM((LANES, seq), jnp.float32)],
        compiler_params=pltpu.CompilerParams(dimension_semantics=("arbitrary",), vmem_limit_bytes=24 * MIB),
        cost_estimate=cost(16, 8),
        name="attn_fwd",
    )(qkv, qkv, qkv)


def attn_backward(qkv, d_out, lse_vals, u_one, grads, parts, after, call_id):
    seq, width = qkv.shape[0], qkv.shape[1] // 3
    n_pairs = width // LANES
    col, lse = attn_specs(seq, n_pairs)
    shape = jax.ShapeDtypeStruct((seq, width), jnp.bfloat16)
    shard_shape = (len(parts) * N_COLOR * ATTN_ROWS, UNIT_COLS)
    d_w = pl.BlockSpec((8, 2, width // 16, LANES), lambda pair: (0, 0, 0, pair))
    out = pl.pallas_call(
        functools.partial(attn_bwd_kernel, parts, len(grads), len(after)),
        grid=(n_pairs,),
        in_specs=[col(0), col(n_pairs), col(2 * n_pairs), col(0), lse, pl.BlockSpec((seq, width), lambda pair: (0, 0))] + [pl.BlockSpec(memory_space=pl.ANY)] * (len(grads) + len(after)),
        out_specs=[col(0), col(0), col(0), d_w, d_w, d_w, pl.BlockSpec(shard_shape, lambda pair: (0, 0))],
        out_shape=[shape, shape, shape] + [pltpu.HBM((8, 2, width // 16, width), jnp.float32)] * 3 + [jax.ShapeDtypeStruct(shard_shape, jnp.bfloat16)],
        scratch_shapes=[pltpu.VMEM((width, seq), jnp.bfloat16), pltpu.VMEM((LANES, seq), jnp.bfloat16), pltpu.VMEM((LANES, seq), jnp.float32), pltpu.VMEM((seq, LANES), jnp.float32), pltpu.VMEM((seq, LANES), jnp.float32)] + reducer_scratch(len(parts), ATTN_ROWS),
        compiler_params=pltpu.CompilerParams(dimension_semantics=("arbitrary",), vmem_limit_bytes=VMEM_ALL, collective_id=call_id),
        cost_estimate=cost(40, 14),
        name="attn_bwd",
    )(qkv, qkv, qkv, d_out, lse_vals, u_one, *grads, *after)
    return out[:3], list(out[3:6]), out[6]


def tail_reduce(gains, grads, parts, after, call_id, n_dev):
    n_chunks = len(parts)
    shard_shape = (n_chunks * N_COLOR * ATTN_ROWS, UNIT_COLS)
    return pl.pallas_call(
        functools.partial(tail_kernel, parts, len(grads), len(after)),
        in_specs=[pl.BlockSpec(memory_space=pltpu.VMEM)] + [pl.BlockSpec(memory_space=pl.ANY)] * (len(grads) + len(after)),
        out_specs=[pl.BlockSpec(memory_space=pltpu.VMEM)] * 2,
        out_shape=[jax.ShapeDtypeStruct(shard_shape, jnp.bfloat16), jax.ShapeDtypeStruct(gains.shape, jnp.float32)],
        scratch_shapes=[pltpu.VMEM((n_dev,) + gains.shape, jnp.float32), pltpu.SemaphoreType.DMA((n_dev,)), pltpu.SemaphoreType.DMA((n_dev,))] + reducer_scratch(n_chunks, ATTN_ROWS),
        compiler_params=pltpu.CompilerParams(vmem_limit_bytes=16 * MIB, collective_id=call_id),
        cost_estimate=cost(20, 14),
        name="tail_reduce",
    )(gains, *grads, *after)


def block_forward(x_blk, gain_a, gain_b, w_qkv, w_out, w_up):
    norm_a, norm_a_back = jax.vjp(rms_gain, x_blk.astype(jnp.float32), gain_a)
    u_one = norm_a.astype(jnp.bfloat16)
    qkv = dot_lo(u_one, w_qkv)
    attn_out, lse_vals = attn_forward(qkv)
    hidden = x_blk + dot_lo(attn_out, w_out)
    norm_b, norm_b_back = jax.vjp(rms_gain, hidden.astype(jnp.float32), gain_b)
    u_two = norm_b.astype(jnp.bfloat16)
    pre_lo = dot_lo(u_two, w_up)
    act_lo = gelu_tanh(pre_lo.astype(jnp.float32)).astype(jnp.bfloat16)
    return hidden, act_lo, (norm_a_back, u_one, qkv, lse_vals, attn_out, norm_b_back, u_two, pre_lo)


def block_backward(grad_blk, saved_vals, w_qkv, w_out, w_up, w_down, layer, ready, after):
    (norm_a_back, u_one, qkv, lse_vals, attn_out, norm_b_back, u_two, pre_lo) = saved_vals
    ids = len(ready)
    grad_u_two, block, shard_mlp = mlp_backward(grad_blk, u_two, pre_lo, w_up, w_down, layer, ready, after[:1], ids)
    grad_h_norm, grad_gain_b = norm_b_back(grad_u_two.astype(jnp.float32))
    grad_hidden = (grad_blk.astype(jnp.float32) + grad_h_norm).astype(jnp.bfloat16)
    grad_out_w = dot_tn(attn_out, grad_hidden)
    grad_attn = dot_nt(grad_hidden, w_out).astype(jnp.bfloat16)
    grads = [block, grad_view(grad_out_w)]
    parts = [rest_parts(0, 1)]
    pieces, grad_qkv_w, shard_attn = attn_backward(qkv, grad_attn, lse_vals, u_one, grads, parts, after[1:], ids + 1)
    grad_qkv = jnp.concatenate(pieces, axis=1)
    grad_u_one = dot_nt(grad_qkv, w_qkv).astype(jnp.bfloat16)
    grad_x_norm, grad_gain_a = norm_a_back(grad_u_one.astype(jnp.float32))
    grad_x_blk = (grad_hidden.astype(jnp.float32) + grad_x_norm).astype(jnp.bfloat16)
    return grad_x_blk, grad_gain_a, grad_gain_b, grad_qkv_w, unit_gather(shard_mlp), unit_gather(shard_attn)


def unit_gather(shard):
    return lax.all_gather(shard, 'data', axis=0, tiled=True).reshape((-1,) + shard.shape)


def put_qkv(unit_ref, base, out_ref, scale):
    for dev in range(DEV_BLK):
        for color in range(N_COLOR):
            for part in range(3):
                cols = slice((color * 3 + part) * UNIT_COLS, (color * 3 + part + 1) * UNIT_COLS)
                row = base + color * ATTN_ROWS + part * 48
                out_ref[0, dev * 48:dev * 48 + 48, cols] = unit_ref[dev, row:row + 48, :].astype(jnp.float32) * scale


def unpack_kernel(with_qkv, n_dev, n_out, *refs):
    mlp_ref, attn_ref = refs[:2]
    up_ref, down_ref, out_ref = refs[-n_out:][:3]
    scale = 1.0 / n_dev
    n_mlp = N_COLOR * MLP_CHUNKS

    def value(unit):
        return unit.astype(jnp.float32) * scale
    for dev in range(DEV_BLK):
        rows = slice(dev * 48, dev * 48 + 48)
        for blk in range(n_mlp + N_COLOR):
            ref, row = (mlp_ref, blk * MLP_ROWS) if blk < n_mlp else (attn_ref, (blk - n_mlp) * ATTN_ROWS)
            up_ref[0, rows, blk * FF_BLK:(blk + 1) * FF_BLK] = value(ref[dev, row:row + 48, :])
            for part in range(3):
                at = row + 48 + 16 * part
                down_ref[0, blk, dev, :, part * UNIT_COLS:(part + 1) * UNIT_COLS] = value(ref[dev, at:at + 16, :])
        for color in range(N_COLOR):
            row = color * ATTN_ROWS + MLP_ROWS
            out_ref[0, rows, color * UNIT_COLS:(color + 1) * UNIT_COLS] = value(attn_ref[dev, row:row + 48, :])
    if with_qkv:
        put_qkv(mlp_ref, n_mlp * MLP_ROWS, refs[-1], scale)


def unpack(mlp_all, attn_all, with_qkv, layer, width, hidden, into, after):
    n_dev = mlp_all.shape[0]
    def in_spec(arr):
        return pl.BlockSpec((DEV_BLK,) + arr.shape[1:], lambda dev: (dev, 0, 0))
    def rows(shape, at):
        return pl.BlockSpec((1, DEV_BLK * (width // n_dev), shape[2]), lambda dev: (at, dev, 0))
    n_blk = hidden // FF_BLK
    shapes = [(2, width, hidden), (2, n_blk, n_dev, FF_BLK // n_dev, width), (2, width, width)]
    down = pl.BlockSpec((1, n_blk, DEV_BLK, FF_BLK // n_dev, width), lambda dev: (layer, 0, dev, 0, 0))
    out_specs = [rows(shapes[0], layer), down, rows(shapes[2], layer)]
    if with_qkv:
        shapes.append((2, width, 3 * width))
        out_specs.append(rows(shapes[3], layer + 1))
    return pl.pallas_call(
        functools.partial(unpack_kernel, with_qkv, n_dev, len(shapes)),
        grid=(n_dev // DEV_BLK,),
        in_specs=[in_spec(mlp_all), in_spec(attn_all)] + [pl.BlockSpec(memory_space=pl.ANY)] * (len(into) + len(after)),
        out_specs=out_specs,
        out_shape=[jax.ShapeDtypeStruct(shape, jnp.float32) for shape in shapes],
        input_output_aliases={2 + i: i for i in range(len(into))},
        compiler_params=pltpu.CompilerParams(dimension_semantics=("arbitrary",), vmem_limit_bytes=32 * MIB),
        cost_estimate=cost(10, 40),
        name="unpack",
    )(mlp_all, attn_all, *into, *after)


def unpack_qkv_kernel(n_dev, last_ref, into_ref, out_ref):
    put_qkv(last_ref, 0, out_ref, 1.0 / n_dev)


def unpack_qkv(last_all, into):
    n_dev = last_all.shape[0]
    rows, cols = into.shape[1:]
    return pl.pallas_call(
        functools.partial(unpack_qkv_kernel, n_dev),
        grid=(n_dev // DEV_BLK,),
        in_specs=[pl.BlockSpec((DEV_BLK,) + last_all.shape[1:], lambda dev: (dev, 0, 0)), pl.BlockSpec(memory_space=pl.ANY)],
        out_specs=pl.BlockSpec((1, DEV_BLK * (rows // n_dev), cols), lambda dev: (0, dev, 0)),
        out_shape=jax.ShapeDtypeStruct(into.shape, jnp.float32),
        input_output_aliases={1: 0},
        compiler_params=pltpu.CompilerParams(dimension_semantics=("arbitrary",), vmem_limit_bytes=16 * MIB),
        cost_estimate=cost(4, 20),
        name="unpack_qkv",
    )(last_all, into)


def solution(mesh):
    n_dev = mesh.shape['data']

    def local_step(x_loc, grad_y_loc, gain_one, gain_two, w_qkv, w_out, w_up, w_down):
        n_layers = w_qkv.shape[0]
        hidden_x = x_loc[0]
        saved_all = []
        for layer_idx in range(n_layers):
            hidden, act_lo, saved_vals = block_forward(hidden_x, gain_one[layer_idx], gain_two[layer_idx], w_qkv[layer_idx], w_out[layer_idx], w_up[layer_idx])
            saved_all.append(saved_vals)
            if layer_idx + 1 < n_layers:
                hidden_x = hidden + dot_lo(act_lo, w_down[layer_idx])
        grad_cur = grad_y_loc[0]
        width, hidden = w_up.shape[1:]
        gains = [None] * (2 * n_layers)
        ready, after, gathered = [], [], []
        for layer_idx in reversed(range(n_layers)):
            out = block_backward(grad_cur, saved_all[layer_idx], w_qkv[layer_idx], w_out[layer_idx], w_up, w_down, layer_idx, ready, after)
            grad_cur, gains[layer_idx], gains[n_layers + layer_idx], grad_qkv_w = out[:4]
            ready, after = grad_qkv_w, list(out[4:])
            gathered.append(after)
        (top_mlp, top_attn), (low_mlp, low_attn) = gathered
        gain_rows = jnp.concatenate([jnp.stack(gains), jnp.zeros((8 - 2 * n_layers, width), jnp.float32)])
        shard, gain_sums = tail_reduce(gain_rows, ready, [qkv_parts(0)], [low_mlp[:1, :16]], 3 * n_layers, n_dev)
        last = unit_gather(shard)
        partial = unpack(top_mlp, top_attn, False, 1, width, hidden, [], [gain_sums])
        w_u, w_d, w_o, grad_qkv = unpack(low_mlp, low_attn, True, 0, width, hidden, partial, [])
        gain_sums = gain_sums / n_dev
        grad_qkv = unpack_qkv(last, grad_qkv)
        weights = (grad_qkv, w_o, w_u, w_d.reshape(n_layers, hidden, width))
        return (grad_cur[None], gain_sums[:n_layers], gain_sums[n_layers:2 * n_layers]) + weights

    batch_spec = P('data')
    full_spec = P()
    return jax.shard_map(local_step, mesh=mesh, in_specs=(batch_spec, batch_spec) + (full_spec,) * 6, out_specs=(batch_spec,) + (full_spec,) * 6, check_vma=False)
```

```python
import functools

import jax
import jax.numpy as jnp
from jax import lax
from jax.experimental import pallas as pl
from jax.experimental.pallas import tpu as pltpu
from jax.sharding import PartitionSpec as P

NORM_EPS = 1e-6
HEAD_DIM = 64
LANES = 128
Q_BLK = 256
EXP_SCALE = HEAD_DIM ** -0.5 * 1.4426950408889634
NEG = -1e30
MIB = 2 ** 20
VMEM_ALL = 67043328
MESH = pl.DeviceIdType.MESH


def cost(gflops, mbytes):
    return pl.CostEstimate(flops=gflops * 10 ** 9, bytes_accessed=mbytes * MIB, transcendentals=0)


def rms_gain(rows_f, gain_vec):
    return rows_f * lax.rsqrt(jnp.mean(rows_f * rows_f, axis=-1, keepdims=True) + NORM_EPS) * gain_vec


def gelu_tanh(pre_act):
    return jax.nn.gelu(pre_act, approximate=True)


def dot_lo(lhs, rhs):
    return jnp.dot(lhs, rhs, preferred_element_type=jnp.float32).astype(jnp.bfloat16)


def dot_nt(lhs, rhs):
    return lax.dot_general(lhs, rhs, (((1,), (1,)), ((), ())), preferred_element_type=jnp.float32)


def dot_tn(lhs, rhs):
    return lax.dot_general(lhs, rhs, (((0,), (0,)), ((), ())), preferred_element_type=jnp.float32)


def dot_nn(lhs, rhs):
    return jnp.dot(lhs, rhs, preferred_element_type=jnp.float32)


def head_mask(ref_rows, head):
    lane = lax.broadcasted_iota(jnp.int32, ref_rows.shape, 1)
    return jnp.where(lane // HEAD_DIM == head, ref_rows, jnp.zeros_like(ref_rows))


def scores_t(k_ref, q_m, q_start):
    diag = dot_nt(k_ref[q_start:q_start + Q_BLK, :], q_m)
    key_i = lax.broadcasted_iota(jnp.int32, diag.shape, 0)
    query_i = lax.broadcasted_iota(jnp.int32, diag.shape, 1)
    diag = jnp.where(key_i <= query_i, diag, NEG)
    if q_start == 0:
        return diag
    return jnp.concatenate([dot_nt(k_ref[:q_start, :], q_m), diag], axis=0)


def attn_fwd_kernel(q_ref, k_ref, v_ref, o_ref, lse_ref, vt_ref, ot_ref):
    seq = q_ref.shape[0]
    vt_ref[...] = v_ref[...].T
    for head in range(LANES // HEAD_DIM):
        rows = slice(head * HEAD_DIM, (head + 1) * HEAD_DIM)
        for q_start in range(0, seq, Q_BLK):
            q_end = q_start + Q_BLK
            q_m = head_mask(q_ref[q_start:q_end, :], head)
            s_t = scores_t(k_ref, q_m, q_start)
            top = jnp.max(s_t, axis=0, keepdims=True)
            p_t = jnp.exp2((s_t - top) * EXP_SCALE)
            total = jnp.sum(p_t, axis=0, keepdims=True)
            p_lo = (p_t * (1.0 / total)).astype(jnp.bfloat16)
            ot_ref[rows, q_start:q_end] = dot_nn(vt_ref[rows, :q_end], p_lo)
            lse_ref[0, head:head + 1, q_start:q_end] = top * EXP_SCALE + jnp.log2(total)
    o_ref[...] = ot_ref[...].T.astype(jnp.bfloat16)


N_COLOR = 3
UNIT_COLS = 256
FF_BLK = 256
MLP_ROWS = 96
ATTN_ROWS = 144
MLP_CHUNKS = 3
DEV_BLK = 2
GELU_C = 0.7978845608028654
AXIS_BITS = (3, 2, 1)


class Reducer:
    def __init__(self, n_chunks, refs, grad_refs=(), parts=()):
        (self.own, self.send0, self.recv0, self.send1, self.recv1, self.send2, self.recv2, self.send3, self.recv3, self.load_sem, self.send_sem, self.recv_sem) = refs
        self.grad_refs, self.parts = grad_refs, parts
        self.n_chunks = n_chunks
        me = lax.axis_index('data')
        self.me = me
        self.bit = [lax.rem(lax.div(me, 1 << b), 2) for b in range(4)]
        self.partner = [me + (1 - 2 * self.bit[b]) * (1 << b) for b in range(4)]

    def barrier(self):
        sem = pltpu.get_barrier_semaphore()
        for dev in self.partner:
            pl.semaphore_signal(sem, inc=1, device_id=(dev,), device_id_type=MESH)
        pl.semaphore_wait(sem, 4)

    def load(self, chunk, half):
        for color in range(N_COLOR):
            for part, (array, kind, col, row, n_rows) in enumerate(self.parts[chunk][color]):
                if kind == 'block':
                    src = self.grad_refs[array].at[col, :, half]
                else:
                    src = self.grad_refs[array].at[:, half, :, pl.ds(col, UNIT_COLS)]
                dst = self.own.at[chunk, color, :, pl.ds(row, n_rows)]
                pltpu.make_async_copy(src, dst, self.load_sem.at[chunk, color, part]).start()

    def wait_load(self, chunk):
        for color in range(N_COLOR):
            for part, (_, _, _, row, n_rows) in enumerate(self.parts[chunk][color]):
                ref = self.own.at[chunk, color, :, pl.ds(row, n_rows)]
                pltpu.make_async_copy(ref, ref, self.load_sem.at[chunk, color, part]).wait()

    def copy(self, stage, chunk, color):
        send = (self.send0, self.send1, self.send2, self.send3)[stage].at[chunk, color]
        recv = (self.recv0, self.recv1, self.recv2, self.recv3)[stage].at[chunk, color]
        dev = self.partner[0] if stage == 0 else self.partner[self.order(color)[stage - 1]]
        return pltpu.make_async_remote_copy(src_ref=send, dst_ref=recv, send_sem=self.send_sem.at[stage, chunk, color], recv_sem=self.recv_sem.at[stage, chunk, color], device_id=(dev,), device_id_type=MESH)

    def order(self, color):
        return [1 + (color + step) % N_COLOR for step in range(N_COLOR)]

    def block(self, values):
        return values[3] * 4 + values[2] * 2 + values[1]

    def convert(self, chunk):
        self.wait_load(chunk)
        for color in range(N_COLOR):
            def body(i, carry):
                self.send0[chunk, color, i] = self.own[chunk, color, i].astype(jnp.bfloat16)
                return carry
            lax.fori_loop(0, 8, body, 0)
            self.copy(0, chunk, color).start()

    def total(self, chunk, color, values, n_recv):
        order = self.order(color)
        index = self.block(values)
        acc = self.own[chunk, color, index] + self.recv0[chunk, color, index].astype(jnp.float32)
        if n_recv >= 2:
            acc = acc + self.recv1[chunk, color, values[order[1]] * 2 + values[order[2]]].astype(jnp.float32)
        if n_recv >= 3:
            acc = acc + self.recv2[chunk, color, values[order[2]]].astype(jnp.float32)
        if n_recv >= 4:
            acc = acc + self.recv3[chunk, color, 0].astype(jnp.float32)
        return acc

    def stage(self, step, chunk):
        send = (None, self.send1, self.send2, self.send3)[step]
        n_free = N_COLOR - step
        for color in range(N_COLOR):
            self.copy(step - 1, chunk, color).wait_recv()
            order = self.order(color)

            def body(i, carry):
                values = [0, 0, 0, 0]
                for done in range(step - 1):
                    values[order[done]] = self.bit[order[done]]
                values[order[step - 1]] = 1 - self.bit[order[step - 1]]
                if n_free == 2:
                    values[order[1]], values[order[2]] = lax.div(i, 2), lax.rem(i, 2)
                elif n_free == 1:
                    values[order[2]] = i
                send[chunk, color, i] = self.total(chunk, color, values, step).astype(jnp.bfloat16)
                return carry
            if n_free:
                lax.fori_loop(0, 1 << n_free, body, 0)
            else:
                body(0, 0)
            self.copy(step, chunk, color).start()

    def finish(self, chunk, out_ref, base=0):
        n_rows = self.own.shape[3]
        for color in range(N_COLOR):
            self.copy(3, chunk, color).wait_recv()
            row = base + (chunk * N_COLOR + color) * n_rows
            out_ref[row:row + n_rows, :] = self.total(chunk, color, self.bit, 4).astype(jnp.bfloat16)
        for stage in range(4):
            for color in range(N_COLOR):
                self.copy(stage, chunk, color).wait_send()


def reducer_scratch(n_chunks, rows):
    def buf(blocks, dtype):
        return pltpu.VMEM((n_chunks, N_COLOR, blocks, rows, UNIT_COLS), dtype)
    lo = jnp.bfloat16
    return [buf(8, jnp.float32), buf(8, lo), buf(8, lo), buf(4, lo), buf(4, lo), buf(2, lo), buf(2, lo), buf(1, lo), buf(1, lo), pltpu.SemaphoreType.DMA((n_chunks, N_COLOR, N_COLOR)), pltpu.SemaphoreType.DMA((4, n_chunks, N_COLOR)), pltpu.SemaphoreType.DMA((4, n_chunks, N_COLOR))]


def grad_view(grad_w):
    rows, cols = grad_w.shape
    return grad_w.reshape(8, 2, rows // 16, cols)


def qkv_parts(array):
    return [[(array + color, 'cols', part * UNIT_COLS, part * 48, 48) for part in range(3)] for color in range(N_COLOR)]


def rest_parts(block_array, out_array):
    return [[(block_array, 'block', color, 0, MLP_ROWS), (out_array, 'cols', color * UNIT_COLS, MLP_ROWS, 48)] for color in range(N_COLOR)]


def mlp_bwd_kernel(parts, n_grads, n_after, *refs):
    dy_ref, u_ref, z_ref, w1_ref, w2_ref = refs[:5]
    grad_refs = refs[5:5 + n_grads]
    refs = refs[5 + n_grads + n_after:]
    du_ref, block_ref, shard_ref, ut_ref, a_ref, dz_ref = refs[:6]
    n_red = (len(refs) - 6) // (2 if parts else 1)
    red = Reducer(MLP_CHUNKS, refs[6:6 + n_red])
    early = Reducer(len(parts), refs[6 + n_red:], grad_refs, parts) if parts else None
    step = pl.program_id(0)
    n_blk = dz_ref.shape[1] // FF_BLK
    core = red.bit[0]
    seq = dy_ref.shape[0]

    @pl.when(step == 0)
    def _():
        red.barrier()
        if early:
            early.load(0, 1 - core)
        ut_ref[...] = u_ref[...].T

    if early:
        @pl.when(step == 1)
        def _():
            early.convert(0)
            early.load(0, core)

        for stage, when in ((1, 2), (2, 6), (3, 10)):
            @pl.when(step == when)
            def _():
                if stage == 1:
                    early.wait_load(0)
                early.stage(stage, 0)

        @pl.when(step == n_blk)
        def _():
            early.finish(0, shard_ref, N_COLOR * MLP_CHUNKS * MLP_ROWS)

    for stage, first, count in ((3, 9, MLP_CHUNKS - 1), (2, 7, MLP_CHUNKS), (1, 4, MLP_CHUNKS)):
        @pl.when((step >= first) & (step < first + N_COLOR * count) & (lax.rem(step + 2 * first, N_COLOR) == 0))
        def _():
            red.stage(stage, lax.div(step - first, N_COLOR))

    @pl.when(step < n_blk)
    def _():
        cols = pl.ds(pl.multiple_of(step * FF_BLK, FF_BLK), FF_BLK)
        for row in range(0, seq, 256):
            rows = slice(row, row + 256)
            da = dot_nt(dy_ref[rows, :], w2_ref[0]).astype(jnp.bfloat16).astype(jnp.float32)
            z = z_ref[rows, :].astype(jnp.float32)
            z_sq = z * z
            th = jnp.tanh(z * (GELU_C + (GELU_C * 0.044715) * z_sq))
            cdf = 0.5 + 0.5 * th
            a_ref[rows, :] = (z * cdf).astype(jnp.bfloat16)
            slope = cdf + (0.5 * z) * (1.0 - th * th) * (GELU_C + (3.0 * GELU_C * 0.044715) * z_sq)
            dz_ref[rows, cols] = (slope * da).astype(jnp.bfloat16)
        dw1 = dot_nn(ut_ref[...], dz_ref[:, cols])
        block_ref[0, :, :, 0:48, :] = dw1.reshape(8, 2, 48, UNIT_COLS)
        dw2 = dot_nn(a_ref[...].T, dy_ref[...])
        for part in range(3):
            block_ref[0, :, :, 48 + 16 * part:64 + 16 * part, :] = dw2[:, part * UNIT_COLS:(part + 1) * UNIT_COLS].reshape(8, 2, 16, UNIT_COLS)

    @pl.when(step < N_COLOR * MLP_CHUNKS)
    def _():
        chunk, color = lax.div(step, N_COLOR), lax.rem(step, N_COLOR)

        def body(i, carry):
            red.own[chunk, color, i] = block_ref[0, i, core]
            red.send0[chunk, color, i] = block_ref[0, i, 1 - core].astype(jnp.bfloat16)
            return carry
        lax.fori_loop(0, 8, body, 0)
        red.copy(0, chunk, color).start()

    @pl.when(step >= n_blk)
    def _():
        du_ref[...] = dot_nt(dz_ref[...], w1_ref[0]).astype(jnp.bfloat16)

    @pl.when(step == pl.num_programs(0) - 1)
    def _():
        red.stage(3, MLP_CHUNKS - 1)
        for chunk in range(MLP_CHUNKS):
            red.finish(chunk, shard_ref)


def mlp_backward(dy, u_two, z_lo, w_up, w_down, layer, grads, after, call_id):
    seq, width = dy.shape
    n_blk = w_up.shape[2] // FF_BLK
    n_last = width // 256
    last = n_blk - N_COLOR
    whole = pl.BlockSpec((seq, width), lambda step: (0, 0))
    parts = [qkv_parts(0)] if grads else []
    shard_shape = (N_COLOR * (MLP_CHUNKS * MLP_ROWS + len(parts) * ATTN_ROWS), UNIT_COLS)
    return pl.pallas_call(
        functools.partial(mlp_bwd_kernel, parts, len(grads), len(after)),
        grid=(n_blk + n_last,),
        in_specs=[
            whole, whole,
            pl.BlockSpec((seq, FF_BLK), lambda step: (0, jnp.minimum(step, n_blk - 1))),
            pl.BlockSpec((1, 256, w_up.shape[2]), lambda step: (layer, jnp.maximum(step - n_blk, 0), 0)),
            pl.BlockSpec((1, FF_BLK, width), lambda step: (layer, jnp.minimum(step, n_blk - 1), 0)),
        ] + [pl.BlockSpec(memory_space=pl.ANY)] * (len(grads) + len(after)),
        out_specs=[
            pl.BlockSpec((seq, 256), lambda step: (0, jnp.maximum(step - n_blk, 0))),
            pl.BlockSpec((1, 8, 2, MLP_ROWS, UNIT_COLS), lambda step: (jnp.clip(step - last, 0, N_COLOR - 1), 0, 0, 0, 0)),
            pl.BlockSpec(shard_shape, lambda step: (0, 0)),
        ],
        out_shape=[jax.ShapeDtypeStruct((seq, width), jnp.bfloat16), jax.ShapeDtypeStruct((N_COLOR, 8, 2, MLP_ROWS, UNIT_COLS), jnp.float32), jax.ShapeDtypeStruct(shard_shape, jnp.bfloat16)],
        scratch_shapes=[pltpu.VMEM((width, seq), jnp.bfloat16), pltpu.VMEM((seq, FF_BLK), jnp.bfloat16), pltpu.VMEM((seq, w_up.shape[2]), jnp.bfloat16)] + reducer_scratch(MLP_CHUNKS, MLP_ROWS) + (reducer_scratch(1, ATTN_ROWS) if parts else []),
        compiler_params=pltpu.CompilerParams(dimension_semantics=("arbitrary",), vmem_limit_bytes=VMEM_ALL, collective_id=call_id),
        cost_estimate=cost(30, 30),
        name="mlp_bwd",
    )(dy, u_two, z_lo, w_up, w_down, *grads, *after)


def attn_bwd_kernel(parts, n_grads, n_after, *refs):
    q_ref, k_ref, v_ref, do_ref, lse_ref, u_ref = refs[:6]
    grad_refs = refs[6:6 + n_grads]
    refs = refs[6 + n_grads + n_after:]
    dq_ref, dk_ref, dv_ref, dwq_ref, dwk_ref, dwv_ref, shard_ref, ut_ref, kt_ref, dqt_ref, dk_acc, dv_acc = refs[:12]
    red = Reducer(len(parts), refs[12:], grad_refs, parts)
    n_chunks = red.n_chunks
    pair = pl.program_id(0)
    seq = q_ref.shape[0]
    events = {}
    for chunk in range(n_chunks):
        for stage, when in ((1, 2), (2, 6), (3, 9)):
            events[when] = [(stage, chunk)]

    @pl.when(pair == 0)
    def _():
        red.barrier()
        for chunk in range(n_chunks):
            red.load(chunk, 1 - red.bit[0])
        for chunk in range(n_chunks):
            red.convert(chunk)
            red.load(chunk, red.bit[0])
        ut_ref[...] = u_ref[...].T

    kt_ref[...] = k_ref[...].T
    for head in range(LANES // HEAD_DIM):
        for when, todo in events.items():
            if when % 2 == head:
                @pl.when(pair == when // 2)
                def _():
                    for stage, chunk in todo:
                        if stage == 1:
                            red.wait_load(chunk)
                        red.stage(stage, chunk)
        rows = slice(head * HEAD_DIM, (head + 1) * HEAD_DIM)
        for q_start in range(0, seq, Q_BLK):
            q_end = q_start + Q_BLK
            q_m = head_mask(q_ref[q_start:q_end, :], head)
            do_m = head_mask(do_ref[q_start:q_end, :], head)
            s_t = scores_t(k_ref, q_m, q_start)
            p_t = jnp.exp2(s_t * EXP_SCALE - lse_ref[0, head:head + 1, q_start:q_end])
            dp_t = dot_nt(v_ref[:q_end, :], do_m)
            delta = jnp.sum(p_t * dp_t, axis=0, keepdims=True)
            ds_t = (p_t * (dp_t - delta) * HEAD_DIM ** -0.5).astype(jnp.bfloat16)
            dv_part = dot_nn(p_t.astype(jnp.bfloat16), do_m)
            dk_part = dot_nn(ds_t, q_m)
            if head == 0 and q_start == 0:
                dv_acc[...] = jnp.zeros_like(dv_acc)
                dk_acc[...] = jnp.zeros_like(dk_acc)
            dv_acc[:q_end, :] += dv_part
            dk_acc[:q_end, :] += dk_part
            dqt_ref[rows, q_start:q_end] = dot_nn(kt_ref[rows, :q_end], ds_t)
    dq_ref[...] = dqt_ref[...].T.astype(jnp.bfloat16)
    dk_ref[...] = dk_acc[...].astype(jnp.bfloat16)
    dv_ref[...] = dv_acc[...].astype(jnp.bfloat16)
    d_w = dot_nn(ut_ref[...], jnp.concatenate([dq_ref[...], dk_ref[...], dv_ref[...]], axis=1))
    for out_ref, at in ((dwq_ref, 0), (dwk_ref, LANES), (dwv_ref, 2 * LANES)):
        out_ref[...] = d_w[:, at:at + LANES].reshape(out_ref.shape)

    @pl.when(pair == pl.num_programs(0) - 1)
    def _():
        for chunk in range(n_chunks):
            red.finish(chunk, shard_ref)


def tail_kernel(parts, n_grads, n_after, *refs):
    gains_ref = refs[0]
    grad_refs = refs[1:1 + n_grads]
    refs = refs[:1 + n_grads] + refs[1 + n_grads + n_after:]
    shard_ref, gsum_ref, gbuf, gsend_sem, grecv_sem = refs[1 + n_grads:6 + n_grads]
    red = Reducer(len(parts), refs[6 + n_grads:], grad_refs, parts)
    n_dev = gbuf.shape[0]
    for chunk in range(red.n_chunks):
        red.load(chunk, 1 - red.bit[0])
    sem = pltpu.get_barrier_semaphore()
    for shift in range(1, n_dev):
        pl.semaphore_signal(sem, inc=1, device_id=(lax.rem(red.me + shift, n_dev),), device_id_type=MESH)
    pl.semaphore_wait(sem, n_dev - 1)

    def gain_copy(shift):
        dev = lax.rem(red.me + shift, n_dev)
        return pltpu.make_async_remote_copy(src_ref=gains_ref, dst_ref=gbuf.at[shift], send_sem=gsend_sem.at[shift], recv_sem=grecv_sem.at[shift], device_id=(dev,), device_id_type=MESH)
    for shift in range(1, n_dev):
        gain_copy(shift).start()
    gbuf[0] = gains_ref[...]
    for chunk in range(red.n_chunks):
        red.convert(chunk)
        red.load(chunk, red.bit[0])
    for step in range(1, 4):
        for chunk in range(red.n_chunks):
            if step == 1:
                red.wait_load(chunk)
            red.stage(step, chunk)
    for shift in range(1, n_dev):
        gain_copy(shift).wait()
    acc = jnp.zeros(gains_ref.shape, jnp.float32)
    for dev in range(n_dev):
        acc = acc + gbuf[lax.rem(red.me + n_dev - dev, n_dev)]
    gsum_ref[...] = acc
    for chunk in range(red.n_chunks):
        red.finish(chunk, shard_ref)


def attn_specs(seq, n_pairs):
    def col(shift):
        return pl.BlockSpec((seq, LANES), lambda pair: (0, pair + shift))
    lse = pl.BlockSpec((1, 8, seq), lambda pair: (pair, 0, 0))
    return col, lse


def attn_forward(qkv):
    seq, width = qkv.shape[0], qkv.shape[1] // 3
    n_pairs = width // LANES
    col, lse = attn_specs(seq, n_pairs)
    return pl.pallas_call(
        attn_fwd_kernel,
        grid=(n_pairs,),
        in_specs=[col(0), col(n_pairs), col(2 * n_pairs)],
        out_specs=[col(0), lse],
        out_shape=[jax.ShapeDtypeStruct((seq, width), jnp.bfloat16), jax.ShapeDtypeStruct((n_pairs, 8, seq), jnp.float32)],
        scratch_shapes=[pltpu.VMEM((LANES, seq), jnp.bfloat16), pltpu.VMEM((LANES, seq), jnp.float32)],
        compiler_params=pltpu.CompilerParams(dimension_semantics=("arbitrary",), vmem_limit_bytes=24 * MIB),
        cost_estimate=cost(16, 8),
        name="attn_fwd",
    )(qkv, qkv, qkv)


def attn_backward(qkv, d_out, lse_vals, u_one, grads, parts, after, call_id):
    seq, width = qkv.shape[0], qkv.shape[1] // 3
    n_pairs = width // LANES
    col, lse = attn_specs(seq, n_pairs)
    shape = jax.ShapeDtypeStruct((seq, width), jnp.bfloat16)
    shard_shape = (len(parts) * N_COLOR * ATTN_ROWS, UNIT_COLS)
    d_w = pl.BlockSpec((8, 2, width // 16, LANES), lambda pair: (0, 0, 0, pair))
    out = pl.pallas_call(
        functools.partial(attn_bwd_kernel, parts, len(grads), len(after)),
        grid=(n_pairs,),
        in_specs=[col(0), col(n_pairs), col(2 * n_pairs), col(0), lse, pl.BlockSpec((seq, width), lambda pair: (0, 0))] + [pl.BlockSpec(memory_space=pl.ANY)] * (len(grads) + len(after)),
        out_specs=[col(0), col(0), col(0), d_w, d_w, d_w, pl.BlockSpec(shard_shape, lambda pair: (0, 0))],
        out_shape=[shape, shape, shape] + [pltpu.HBM((8, 2, width // 16, width), jnp.float32)] * 3 + [jax.ShapeDtypeStruct(shard_shape, jnp.bfloat16)],
        scratch_shapes=[pltpu.VMEM((width, seq), jnp.bfloat16), pltpu.VMEM((LANES, seq), jnp.bfloat16), pltpu.VMEM((LANES, seq), jnp.float32), pltpu.VMEM((seq, LANES), jnp.float32), pltpu.VMEM((seq, LANES), jnp.float32)] + reducer_scratch(len(parts), ATTN_ROWS),
        compiler_params=pltpu.CompilerParams(dimension_semantics=("arbitrary",), vmem_limit_bytes=VMEM_ALL, collective_id=call_id),
        cost_estimate=cost(40, 14),
        name="attn_bwd",
    )(qkv, qkv, qkv, d_out, lse_vals, u_one, *grads, *after)
    return out[:3], list(out[3:6]), out[6]


def tail_reduce(gains, grads, parts, after, call_id, n_dev):
    n_chunks = len(parts)
    shard_shape = (n_chunks * N_COLOR * ATTN_ROWS, UNIT_COLS)
    return pl.pallas_call(
        functools.partial(tail_kernel, parts, len(grads), len(after)),
        in_specs=[pl.BlockSpec(memory_space=pltpu.VMEM)] + [pl.BlockSpec(memory_space=pl.ANY)] * (len(grads) + len(after)),
        out_specs=[pl.BlockSpec(memory_space=pltpu.VMEM)] * 2,
        out_shape=[jax.ShapeDtypeStruct(shard_shape, jnp.bfloat16), jax.ShapeDtypeStruct(gains.shape, jnp.float32)],
        scratch_shapes=[pltpu.VMEM((n_dev,) + gains.shape, jnp.float32), pltpu.SemaphoreType.DMA((n_dev,)), pltpu.SemaphoreType.DMA((n_dev,))] + reducer_scratch(n_chunks, ATTN_ROWS),
        compiler_params=pltpu.CompilerParams(vmem_limit_bytes=16 * MIB, collective_id=call_id),
        cost_estimate=cost(20, 14),
        name="tail_reduce",
    )(gains, *grads, *after)


def block_forward(x_blk, gain_a, gain_b, w_qkv, w_out, w_up):
    norm_a, norm_a_back = jax.vjp(rms_gain, x_blk.astype(jnp.float32), gain_a)
    u_one = norm_a.astype(jnp.bfloat16)
    qkv = dot_lo(u_one, w_qkv)
    attn_out, lse_vals = attn_forward(qkv)
    hidden = x_blk + dot_lo(attn_out, w_out)
    norm_b, norm_b_back = jax.vjp(rms_gain, hidden.astype(jnp.float32), gain_b)
    u_two = norm_b.astype(jnp.bfloat16)
    pre_lo = dot_lo(u_two, w_up)
    act_lo = gelu_tanh(pre_lo.astype(jnp.float32)).astype(jnp.bfloat16)
    return hidden, act_lo, (norm_a_back, u_one, qkv, lse_vals, attn_out, norm_b_back, u_two, pre_lo)


def block_backward(grad_blk, saved_vals, w_qkv, w_out, w_up, w_down, layer, ready, after):
    (norm_a_back, u_one, qkv, lse_vals, attn_out, norm_b_back, u_two, pre_lo) = saved_vals
    ids = len(ready)
    grad_u_two, block, shard_mlp = mlp_backward(grad_blk, u_two, pre_lo, w_up, w_down, layer, ready, after[:1], ids)
    grad_h_norm, grad_gain_b = norm_b_back(grad_u_two.astype(jnp.float32))
    grad_hidden = (grad_blk.astype(jnp.float32) + grad_h_norm).astype(jnp.bfloat16)
    grad_out_w = dot_tn(attn_out, grad_hidden)
    grad_attn = dot_nt(grad_hidden, w_out).astype(jnp.bfloat16)
    grads = [block, grad_view(grad_out_w)]
    parts = [rest_parts(0, 1)]
    pieces, grad_qkv_w, shard_attn = attn_backward(qkv, grad_attn, lse_vals, u_one, grads, parts, after[1:], ids + 1)
    grad_qkv = jnp.concatenate(pieces, axis=1)
    grad_u_one = dot_nt(grad_qkv, w_qkv).astype(jnp.bfloat16)
    grad_x_norm, grad_gain_a = norm_a_back(grad_u_one.astype(jnp.float32))
    grad_x_blk = (grad_hidden.astype(jnp.float32) + grad_x_norm).astype(jnp.bfloat16)
    return grad_x_blk, grad_gain_a, grad_gain_b, grad_qkv_w, unit_gather(shard_mlp), unit_gather(shard_attn)


def unit_gather(shard):
    return lax.all_gather(shard, 'data', axis=0, tiled=True).reshape((-1,) + shard.shape)


def put_qkv(unit_ref, base, out_ref, scale):
    for dev in range(DEV_BLK):
        for color in range(N_COLOR):
            for part in range(3):
                cols = slice((color * 3 + part) * UNIT_COLS, (color * 3 + part + 1) * UNIT_COLS)
                row = base + color * ATTN_ROWS + part * 48
                out_ref[0, dev * 48:dev * 48 + 48, cols] = unit_ref[dev, row:row + 48, :].astype(jnp.float32) * scale


def unpack_kernel(with_qkv, n_dev, n_out, *refs):
    mlp_ref, attn_ref = refs[:2]
    up_ref, down_ref, out_ref = refs[-n_out:][:3]
    scale = 1.0 / n_dev
    n_mlp = N_COLOR * MLP_CHUNKS

    def value(unit):
        return unit.astype(jnp.float32) * scale
    for dev in range(DEV_BLK):
        rows = slice(dev * 48, dev * 48 + 48)
        for blk in range(n_mlp + N_COLOR):
            ref, row = (mlp_ref, blk * MLP_ROWS) if blk < n_mlp else (attn_ref, (blk - n_mlp) * ATTN_ROWS)
            up_ref[0, rows, blk * FF_BLK:(blk + 1) * FF_BLK] = value(ref[dev, row:row + 48, :])
            for part in range(3):
                at = row + 48 + 16 * part
                down_ref[0, blk, dev, :, part * UNIT_COLS:(part + 1) * UNIT_COLS] = value(ref[dev, at:at + 16, :])
        for color in range(N_COLOR):
            row = color * ATTN_ROWS + MLP_ROWS
            out_ref[0, rows, color * UNIT_COLS:(color + 1) * UNIT_COLS] = value(attn_ref[dev, row:row + 48, :])
    if with_qkv:
        put_qkv(mlp_ref, n_mlp * MLP_ROWS, refs[-1], scale)


def unpack(mlp_all, attn_all, with_qkv, layer, width, hidden, into, after):
    n_dev = mlp_all.shape[0]
    def in_spec(arr):
        return pl.BlockSpec((DEV_BLK,) + arr.shape[1:], lambda dev: (dev, 0, 0))
    def rows(shape, at):
        return pl.BlockSpec((1, DEV_BLK * (width // n_dev), shape[2]), lambda dev: (at, dev, 0))
    n_blk = hidden // FF_BLK
    shapes = [(2, width, hidden), (2, n_blk, n_dev, FF_BLK // n_dev, width), (2, width, width)]
    down = pl.BlockSpec((1, n_blk, DEV_BLK, FF_BLK // n_dev, width), lambda dev: (layer, 0, dev, 0, 0))
    out_specs = [rows(shapes[0], layer), down, rows(shapes[2], layer)]
    if with_qkv:
        shapes.append((2, width, 3 * width))
        out_specs.append(rows(shapes[3], layer + 1))
    return pl.pallas_call(
        functools.partial(unpack_kernel, with_qkv, n_dev, len(shapes)),
        grid=(n_dev // DEV_BLK,),
        in_specs=[in_spec(mlp_all), in_spec(attn_all)] + [pl.BlockSpec(memory_space=pl.ANY)] * (len(into) + len(after)),
        out_specs=out_specs,
        out_shape=[jax.ShapeDtypeStruct(shape, jnp.float32) for shape in shapes],
        input_output_aliases={2 + i: i for i in range(len(into))},
        compiler_params=pltpu.CompilerParams(dimension_semantics=("arbitrary",), vmem_limit_bytes=32 * MIB),
        cost_estimate=cost(10, 40),
        name="unpack",
    )(mlp_all, attn_all, *into, *after)


def unpack_qkv_kernel(n_dev, last_ref, into_ref, out_ref):
    put_qkv(last_ref, 0, out_ref, 1.0 / n_dev)


def unpack_qkv(last_all, into):
    n_dev = last_all.shape[0]
    rows, cols = into.shape[1:]
    return pl.pallas_call(
        functools.partial(unpack_qkv_kernel, n_dev),
        grid=(n_dev // DEV_BLK,),
        in_specs=[pl.BlockSpec((DEV_BLK,) + last_all.shape[1:], lambda dev: (dev, 0, 0)), pl.BlockSpec(memory_space=pl.ANY)],
        out_specs=pl.BlockSpec((1, DEV_BLK * (rows // n_dev), cols), lambda dev: (0, dev, 0)),
        out_shape=jax.ShapeDtypeStruct(into.shape, jnp.float32),
        input_output_aliases={1: 0},
        compiler_params=pltpu.CompilerParams(dimension_semantics=("arbitrary",), vmem_limit_bytes=16 * MIB),
        cost_estimate=cost(4, 20),
        name="unpack_qkv",
    )(last_all, into)


def solution(mesh):
    n_dev = mesh.shape['data']

    def local_step(x_loc, grad_y_loc, gain_one, gain_two, w_qkv, w_out, w_up, w_down):
        n_layers = w_qkv.shape[0]
        hidden_x = x_loc[0]
        saved_all = []
        for layer_idx in range(n_layers):
            hidden, act_lo, saved_vals = block_forward(hidden_x, gain_one[layer_idx], gain_two[layer_idx], w_qkv[layer_idx], w_out[layer_idx], w_up[layer_idx])
            saved_all.append(saved_vals)
            if layer_idx + 1 < n_layers:
                hidden_x = hidden + dot_lo(act_lo, w_down[layer_idx])
        grad_cur = grad_y_loc[0]
        width, hidden = w_up.shape[1:]
        gains = [None] * (2 * n_layers)
        ready, after, gathered = [], [], []
        for layer_idx in reversed(range(n_layers)):
            out = block_backward(grad_cur, saved_all[layer_idx], w_qkv[layer_idx], w_out[layer_idx], w_up, w_down, layer_idx, ready, after)
            grad_cur, gains[layer_idx], gains[n_layers + layer_idx], grad_qkv_w = out[:4]
            ready, after = grad_qkv_w, list(out[4:])
            gathered.append(after)
        (top_mlp, top_attn), (low_mlp, low_attn) = gathered
        gain_rows = jnp.concatenate([jnp.stack(gains), jnp.zeros((8 - 2 * n_layers, width), jnp.float32)])
        shard, gain_sums = tail_reduce(gain_rows, ready, [qkv_parts(0)], [low_mlp[:1, :16]], 3 * n_layers, n_dev)
        last = unit_gather(shard)
        partial = unpack(top_mlp, top_attn, False, 1, width, hidden, [], [gain_sums])
        w_u, w_d, w_o, grad_qkv = unpack(low_mlp, low_attn, True, 0, width, hidden, partial, [])
        gain_sums = gain_sums / n_dev
        grad_qkv = unpack_qkv(last, grad_qkv)
        weights = (grad_qkv, w_o, w_u, w_d.reshape(n_layers, hidden, width))
        return (grad_cur[None], gain_sums[:n_layers], gain_sums[n_layers:2 * n_layers]) + weights

    batch_spec = P('data')
    full_spec = P()
    return jax.shard_map(local_step, mesh=mesh, in_specs=(batch_spec, batch_spec) + (full_spec,) * 6, out_specs=(batch_spec,) + (full_spec,) * 6, check_vma=False)
```
